128 devices in a mesh: dev: 32 (over y, x, core), ka: 4 (over z).
Axes of the slice: x: 4, y: 4, z: 4, core: 2. Of those that a mesh axis runs over, the one named last changes fastest.
Arguments:
- tile_data: float32 [8192, 128, 128], P(('dev', 'ka')), may hold values from -0.25 to 0.25
- tile_row: int32 [128, 64], P(('dev', 'ka')), may hold values from 0 to 31
- tile_col: int32 [128, 64], P(('dev', 'ka')), may hold values from 0 to 63
- tile_count: int32 [128], P(('dev', 'ka')), may hold values from 10 to 64, as said below
- touched: int32 [128, 64], P(('dev', 'ka')), may hold values from 0 to 511, as said below
- owner_map: int32 [512], replicated, may hold values from 0 to 511, as said below
- observed: float32 [4096, 128, 64], P(('dev', 'ka')), may hold values from -6 to 6
- start_x: float32 [8192, 128, 64], P(('dev', 'ka')), may hold values from -6 to 6
- start_u: float32 [8192, 128, 64], P(('dev', 'ka')), may hold values from -4 to 4
Outputs:
- final_x: float32 [8192, 128, 64], P(('dev', 'ka'))
- final_u: float32 [8192, 128, 64], P(('dev', 'ka'))
- z_keeper_agreed: float32 [512, 128, 64], P(('dev', 'ka'))
- primal_gap: float32 [64], replicated
The draws below stay inside these ranges and needn't reach their ends.
Inputs may be any that keep to these rules, and one draw needn't show every extreme that they name: Shard s uses its first tile_count[s] slots; each count is at least 10 and at most 64, and some shard has exactly 64. `touched`: A shard's 64 entries are distinct column blocks. The owner of block j is shard owner_map[j] // 4; a shard touches at most one block of any one owner, and every shard touches exactly one block of some owner. `owner_map`: A permutation of 0 to 511.
All inputs are finite; a program needn't handle non-finite values.
Results may differ from the reference program's by a relative error of at most 0.0003.
Values sent between devices are 32-bit elements.
A program may use at most 128 MiB of HBM per device.

```python
import math
import jax
import jax.numpy as jnp
import numpy as np
from jax import lax

BLK = 128
TARGETS = 64
TILE_DEV = 64
ROWB_DEV = 32
LOCAL_COLS = 64
COL_DEV = 4
ITERS = 2
CG_STEPS = 4
PIECE_TOTAL = 128
OWNER_LIMIT = 1
COLB = 512
TILES = 8192
ROWBLOCKS = 4096
SLOTS = 8192


def column_plan(key):
    ordering = jax.random.permutation(jax.random.fold_in(key, 11), COLB).astype(jnp.int32)
    inverse = jnp.zeros((COLB,), jnp.int32).at[ordering].set(jnp.arange(COLB, dtype=jnp.int32))
    keeper_demand = jax.random.randint(jax.random.fold_in(key, 12), (PIECE_TOTAL,), 0, 8, dtype=jnp.int32)
    block_heat = jax.random.randint(jax.random.fold_in(key, 13), (PIECE_TOTAL, COL_DEV), 0, 8, dtype=jnp.int32)
    local_noise = jax.random.randint(jax.random.fold_in(key, 14), (PIECE_TOTAL, PIECE_TOTAL, COL_DEV), 0, 1024, dtype=jnp.int32)
    local_score = local_noise * (1 + block_heat * block_heat)[None, :, :] * COL_DEV + jnp.arange(COL_DEV, dtype=jnp.int32)
    local_pick = lax.top_k(local_score, OWNER_LIMIT)[1].astype(jnp.int32)
    couple_jitter = jax.random.randint(jax.random.fold_in(key, 15), (PIECE_TOTAL, PIECE_TOTAL, OWNER_LIMIT), 0, 1024, dtype=jnp.int32)
    preferred_keeper = jax.random.randint(jax.random.fold_in(key, 16), (PIECE_TOTAL,), 0, PIECE_TOTAL, dtype=jnp.int32)
    preference_reward = (jnp.arange(PIECE_TOTAL, dtype=jnp.int32)[None, :] == preferred_keeper[:, None]).astype(jnp.int32) * (1 << 28)
    couple_position = jnp.arange(PIECE_TOTAL * OWNER_LIMIT, dtype=jnp.int32).reshape(PIECE_TOTAL, OWNER_LIMIT)
    couple_rating = couple_jitter * (1 + keeper_demand * keeper_demand)[None, :, None] * (PIECE_TOTAL * OWNER_LIMIT) + couple_position[None, :, :] + preference_reward[:, :, None]
    chosen = lax.top_k(couple_rating.reshape(PIECE_TOTAL, PIECE_TOTAL * OWNER_LIMIT), LOCAL_COLS)[1].astype(jnp.int32)
    owners = chosen // OWNER_LIMIT
    local_ids = jnp.take_along_axis(local_pick.reshape(PIECE_TOTAL, PIECE_TOTAL * OWNER_LIMIT), chosen, axis=1)
    touched_ids = inverse[owners * COL_DEV + local_ids]
    return (ordering, touched_ids.astype(jnp.int32))


def draw_touched(key, part):
    return column_plan(key)[1]


def draw_owner_map(key, part):
    return column_plan(key)[0]


def draw_tile_count(key, part):
    levels = jax.random.randint(jax.random.fold_in(key, 3), (PIECE_TOTAL,), 0, 6, dtype=jnp.int32)
    counts = TILE_DEV // (1 + levels)
    busiest = jax.random.randint(jax.random.fold_in(key, 4), (), 0, PIECE_TOTAL, dtype=jnp.int32)
    return jnp.where(jnp.arange(PIECE_TOTAL, dtype=jnp.int32) == busiest, TILE_DEV, counts).astype(jnp.int32)


def touch_ends(drawn, key, least, largest):
    longest = drawn.shape.index(max(drawn.shape))
    spots = []
    for shift in (0, 1):
        where = [jax.random.randint(jax.random.fold_in(key, axis), (), 0, length) for axis, length in enumerate(drawn.shape)]
        where[longest] = (where[longest] + shift) % drawn.shape[longest]
        spots.append(tuple(where))
    return drawn.at[spots[0]].set(least).at[spots[1]].set(largest)


def block_levels(key, extent, pieces, low, top_value):
    factor_of = 1.0
    for position, shards_of in pieces:
        steps = jax.random.uniform(jax.random.fold_in(jax.random.fold_in(key, 6), position), (shards_of,), jnp.float32, low / len(pieces), top_value / len(pieces))
        factor_of = factor_of * jnp.repeat(jnp.exp(steps), extent[position] // shards_of).reshape((-1,) + (1,) * (len(extent) - 1 - position))
    return factor_of


def cumulative_ranks(number_of, lean):
    loads = [(1 << 20) // math.isqrt(standing ** lean) + 1 for standing in range(1, number_of + 1)]
    width = 1 + sum(loads) // (1 << 30)
    return np.cumsum(np.array([max(1, weight // width) for weight in loads]))


def ranked(own_key, shape, count, slope):
    table = cumulative_ranks(count, slope)
    lot = jax.random.randint(jax.random.fold_in(own_key, 1), shape, 0, int(table[count - 1]))
    rank = jnp.searchsorted(jnp.asarray(table, jnp.int32), lot, side="right")
    return jax.random.permutation(jax.random.fold_in(own_key, 2), count)[rank].astype(jnp.int32)


def normal_values(own_key, shape, scale, most, split=(), kind=jnp.bfloat16):
    level = block_levels(own_key, shape, split, -0.22, 0.18) if split else 1.0
    drawn = jax.random.normal(own_key, shape, jnp.float32) * scale * level
    return jnp.minimum(jnp.maximum(drawn, -most), most).astype(kind)


def setup_inputs(seed: int = 0) -> dict:
    splits = jax.random.split(jax.random.key(seed), 10)
    tile_data = normal_values(splits[0], (TILES, BLK, BLK), (4 * BLK) ** -0.5, 0.25, ((0, 128),), jnp.float32)
    tile_row = touch_ends(jax.random.randint(splits[1], (PIECE_TOTAL, TILE_DEV), 0, ROWB_DEV), jax.random.fold_in(splits[1], 1), 0, ROWB_DEV - 1).astype(jnp.int32)
    tile_col = touch_ends(ranked(splits[2], (PIECE_TOTAL, TILE_DEV), LOCAL_COLS, 2), jax.random.fold_in(splits[2], 3), 0, LOCAL_COLS - 1).astype(jnp.int32)
    tile_count = draw_tile_count(jax.random.fold_in(splits[9], 71), 0)
    touched = draw_touched(jax.random.fold_in(splits[9], 71), 0)
    owner_map = draw_owner_map(jax.random.fold_in(splits[9], 71), 0)
    observed = normal_values(splits[6], (ROWBLOCKS, BLK, TARGETS), 1.0, 6.0, ((0, 128),), jnp.float32)
    start_x = normal_values(splits[7], (SLOTS, BLK, TARGETS), 1.0, 6.0, ((0, 128),), jnp.float32)
    start_u = normal_values(splits[8], (SLOTS, BLK, TARGETS), 0.5, 4.0, ((0, 128),), jnp.float32)
    return dict(tile_data=tile_data, tile_row=tile_row, tile_col=tile_col, tile_count=tile_count, touched=touched, owner_map=owner_map, observed=observed, start_x=start_x, start_u=start_u)


EXACTNESS = lax.Precision.HIGHEST
PENALTY = 1.0
COUPLING = 1.0

def shrink(amount, cutoff):
    return amount - jnp.clip(amount, -cutoff, cutoff)

def forward(tile_set, row_ids, col_ids, in_use, vector):
    product = jnp.einsum('tij,tjr->tir', tile_set, vector[col_ids], precision=EXACTNESS) * in_use[:, None, None]
    return jax.ops.segment_sum(product, row_ids, ROWB_DEV)

def backward(tile_set, row_ids, col_ids, in_use, vector):
    product = jnp.einsum('tji,tjr->tir', tile_set, vector[row_ids], precision=EXACTNESS) * in_use[:, None, None]
    return jax.ops.segment_sum(product, col_ids, LOCAL_COLS)

def pull_one(packed):
    tile_set, row_ids, col_ids, in_use, observed_set = packed
    return backward(tile_set, row_ids, col_ids, in_use, observed_set)

def conjugate(packed):
    tile_set, row_ids, col_ids, in_use, rhs_side, begin = packed

    def operate(vector):
        image_rows = forward(tile_set, row_ids, col_ids, in_use, vector)
        return backward(tile_set, row_ids, col_ids, in_use, image_rows) + COUPLING * vector
    iterate = begin
    residual = rhs_side - operate(begin)
    direction = residual
    norm_now = lax.optimization_barrier(jnp.sum(residual * residual, axis=(0, 1)))
    for cg_step in range(CG_STEPS):
        mapped = operate(direction)
        step_size = norm_now / lax.optimization_barrier(jnp.sum(direction * mapped, axis=(0, 1)))
        iterate = iterate + step_size * direction
        residual = residual - step_size * mapped
        norm_next = lax.optimization_barrier(jnp.sum(residual * residual, axis=(0, 1)))
        direction = residual + norm_next / norm_now * direction
        norm_now = norm_next
    return iterate

def reference(tile_data, tile_row, tile_col, tile_count, touched, owner_map, observed, start_x, start_u):
    tile_sets = tile_data.reshape(PIECE_TOTAL, TILE_DEV, BLK, BLK)
    observed_sets = observed.reshape(PIECE_TOTAL, ROWB_DEV, BLK, TARGETS)
    current_x = start_x.reshape(PIECE_TOTAL, LOCAL_COLS, BLK, TARGETS)
    current_u = start_u.reshape(PIECE_TOTAL, LOCAL_COLS, BLK, TARGETS)
    in_use = (jnp.arange(TILE_DEV, dtype=jnp.int32)[None, :] < tile_count[:, None]).astype(jnp.float32)
    pulled = lax.map(pull_one, (tile_sets, tile_row, tile_col, in_use, observed_sets))
    flat_ids = touched.reshape(-1)
    counts = jax.ops.segment_sum(jnp.ones(flat_ids.shape, jnp.float32), flat_ids, COLB)
    share = jnp.maximum(counts, 1.0)[:, None, None]
    consensus = jnp.zeros((COLB, BLK, TARGETS), jnp.float32)
    difference = jnp.zeros_like(current_x)
    for outer_step in range(ITERS):
        merged = (current_x + current_u).reshape(SLOTS, BLK, TARGETS)
        summed = jax.ops.segment_sum(merged, flat_ids, COLB)
        consensus = shrink(summed / share, PENALTY / (COUPLING * share))
        z_local = consensus[touched]
        difference = current_x - z_local
        current_u = current_u + difference
        rhs_side = pulled + COUPLING * (z_local - current_u)
        current_x = lax.map(conjugate, (tile_sets, tile_row, tile_col, in_use, rhs_side, current_x))
    primal_gap = jnp.sqrt(lax.optimization_barrier(jnp.sum(difference * difference, axis=(0, 1, 2))) / (PIECE_TOTAL * LOCAL_COLS * BLK))
    z_keeper_agreed = jnp.zeros_like(consensus).at[owner_map].set(consensus)
    return (current_x.reshape(SLOTS, BLK, TARGETS), current_u.reshape(SLOTS, BLK, TARGETS), z_keeper_agreed, primal_gap)
```

```python
import functools

import jax
import jax.numpy as jnp
from jax import lax
from jax.experimental import pallas as pl
from jax.experimental.pallas import tpu as pltpu
from jax.sharding import PartitionSpec as P

ITERS = 2
CG_STEPS = 4
GROUP = 8
AXES = ("dev", "ka")
F32 = jnp.float32
BF16 = jnp.bfloat16


def split_store(ref, index, value):
    rows = value.shape[0]
    high = value.astype(BF16)
    low = (value - high.astype(F32)).astype(BF16)
    ref[index, :rows, :] = high
    ref[index, rows:, :] = low


def join(wide, rows, cols):
    return (wide[:rows, :cols] + wide[:rows, cols:]) + wide[rows:, :cols]


def tile_plan(rows, cols, count):
    tiles = rows.shape[0]
    place = jnp.arange(tiles, dtype=jnp.int32)
    used = place < count

    def order(key):
        code = jnp.where(used, key, tiles) * tiles + place
        rank = jnp.sum((code[None, :] < code[:, None]).astype(jnp.int32), axis=1)
        pick = rank[None, :] == place[:, None]
        return rank, pick

    def take(pick, values):
        return jnp.sum(jnp.where(pick, values[None, :], 0), axis=1)

    row_key = jnp.where(used, rows, tiles)
    col_key = jnp.where(used, cols, tiles)
    rank_f, pick_f = order(rows)
    rank_b, pick_b = order(cols)
    row_sorted = take(pick_f, row_key)
    col_sorted = take(pick_b, col_key)
    before = lambda s: jnp.concatenate([jnp.full((1,), -1, jnp.int32), s[:-1]])
    after = lambda s: jnp.concatenate([s[1:], jnp.full((1,), -1, jnp.int32)])
    keep_f = (row_sorted == before(row_sorted)).astype(jnp.int32)
    keep_b = (col_sorted == before(col_sorted)).astype(jnp.int32)
    ends_f = ((row_sorted != after(row_sorted)) & (row_sorted < tiles)).astype(jnp.int32)
    last_of_row = jnp.max(jnp.where(row_key[:, None] == row_key[None, :], rank_f[None, :], 0), axis=1)
    column = jnp.arange(tiles, dtype=jnp.int32)
    last_of_col = jnp.max(jnp.where(col_key[None, :] == column[:, None], rank_b[None, :] + 1, 0), axis=1)
    last_of_col = jnp.where(last_of_col == 0, tiles, last_of_col - 1)
    return jnp.stack([
        take(pick_f, place), take(pick_f, cols), keep_f, ends_f, jnp.minimum(row_sorted, 31),
        take(pick_b, place), take(pick_b, last_of_row), keep_b, last_of_col,
    ])


def make_passes(plan, tiles_hl, image_hl, back, slots, targets, blk):
    count = slots

    def forward(source_hl, observed=None, square=False):
        def group(g, carry):
            acc, total = carry
            for n in range(GROUP):
                k = g * GROUP + n
                tile = plan[0, k]
                wide = lax.dot_general(
                    source_hl[plan[1, k]], tiles_hl[tile], (((1,), (1,)), ((), ())),
                    preferred_element_type=F32)
                acc = jnp.where(plan[2, k] > 0, acc, 0.0) + join(wide, targets, blk)
                if square:
                    total = total + jnp.where(plan[3, k] > 0, acc * acc, 0.0)
                elif observed is not None:
                    split_store(image_hl, k, observed[plan[4, k]] - acc)
                else:
                    split_store(image_hl, k, acc)
            return acc, total

        zero = jnp.zeros((targets, blk), F32)
        return lax.fori_loop(0, count // GROUP, group, (zero, zero))[1]

    def backward():
        def group(g, acc):
            for n in range(GROUP):
                k = g * GROUP + n
                both = tiles_hl[plan[5, k]]
                weights = jnp.concatenate([both[:blk], both[blk:]], axis=1)
                wide = jnp.dot(image_hl[plan[6, k]], weights, preferred_element_type=F32)
                acc = jnp.where(plan[7, k] > 0, acc, 0.0) + join(wide, targets, blk)
                back[k] = acc
            return acc

        lax.fori_loop(0, count // GROUP, group, jnp.zeros((targets, blk), F32))

    return forward, backward


def over_slots(slots, body, *init):
    step = 4

    def group(g, carry):
        for n in range(step):
            carry = body(g * step + n, *carry)
        return carry

    return lax.fori_loop(0, slots // step, group, init)


def total_of(value):
    return jnp.sum(value, axis=1, keepdims=True)


def solve_kernel(first, *refs):
    if first:
        (plan, tiles, observed, x, u, z, x_out, r_out, u_out, gap_out,
         tiles_hl, p, p_hl, image_hl, back) = refs
    else:
        (plan, tiles, x, u, z, z_before, r_in, x_out, u_out, gap_out,
         r_out, tiles_hl, p, p_hl, image_hl, back) = refs
    slots, targets, blk = x.shape
    zero = jnp.zeros((targets, blk), F32)
    back[slots] = zero

    def split_tile(t, _):
        split_store(tiles_hl, t, tiles[t])
        return _

    lax.fori_loop(0, slots, split_tile, 0)
    forward, backward = make_passes(plan, tiles_hl, image_hl, back, slots, targets, blk)

    if first:
        def load_x(c, _):
            split_store(p_hl, c, x[c])
            return (_,)

        over_slots(slots, load_x, 0)
        forward(p_hl, observed=observed)
        backward()

    def begin(c, rr, gap):
        diff = x[c] - z[c]
        u_new = u[c] + diff
        u_out[c] = u_new
        if first:
            r = back[plan[8, c]] + (z[c] - u_new) - x[c]
        else:
            r = r_in[c] + ((z[c] - u_new) - (z_before[c] - u[c]))
        r_out[c] = r
        p[c] = r
        split_store(p_hl, c, r)
        x_out[c] = x[c]
        return rr + r * r, gap + diff * diff

    rr, gap = over_slots(slots, begin, zero, zero)
    gap_out[...] = gap
    rr = total_of(rr)

    def advance(a, update_p, rr):
        def move(c, nn):
            r = r_out[c] - a * (back[plan[8, c]] + p[c])
            r_out[c] = r
            x_out[c] = x_out[c] + a * p[c]
            return (nn + r * r,)

        (nn,) = over_slots(slots, move, zero)
        nn = total_of(nn)
        if update_p:
            ratio = nn / rr

            def turn(c, _):
                value = r_out[c] + ratio * p[c]
                p[c] = value
                split_store(p_hl, c, value)
                return (_,)

            over_slots(slots, turn, 0)
        return nn

    def length(c, pq):
        value = p[c]
        return (pq + value * (back[plan[8, c]] + value),)

    def step(_, rr):
        forward(p_hl)
        backward()
        (pq,) = over_slots(slots, length, zero)
        return advance(rr / total_of(pq), True, rr)

    rr = lax.fori_loop(0, CG_STEPS - 1, step, rr)
    if first:
        forward(p_hl)
        backward()
        (pq,) = over_slots(slots, length, zero)
        advance(rr / total_of(pq), False, rr)
    else:
        square = forward(p_hl, square=True)

        def own(c, total):
            return (total + p[c] * p[c],)

        (pp,) = over_slots(slots, own, square)
        a = rr / total_of(pp)

        def finish(c, _):
            x_out[c] = x_out[c] + a * p[c]
            return (_,)

        over_slots(slots, finish, 0)


def solve(first, plan, *arrays):
    tiles = arrays[0]
    x = arrays[2] if first else arrays[1]
    slots, targets, blk = x.shape
    like = jax.ShapeDtypeStruct(x.shape, F32)
    gap = jax.ShapeDtypeStruct((targets, blk), F32)
    work = [
        pltpu.VMEM((tiles.shape[0], 2 * blk, blk), BF16),
        pltpu.VMEM(x.shape, F32),
        pltpu.VMEM((slots, 2 * targets, blk), BF16),
        pltpu.VMEM((slots, 2 * targets, blk), BF16),
        pltpu.VMEM((slots + 1, targets, blk), F32),
    ]
    if first:
        outs = (like, like, like, gap)
    else:
        outs = (like, like, gap)
        work = [pltpu.VMEM(x.shape, F32)] + work
    whole = pl.BlockSpec(memory_space=pltpu.VMEM)
    return pl.pallas_call(
        functools.partial(solve_kernel, first),
        out_shape=outs,
        in_specs=[pl.BlockSpec(memory_space=pltpu.SMEM)] + [whole] * len(arrays),
        out_specs=tuple(whole for _ in outs),
        scratch_shapes=work,
        compiler_params=pltpu.CompilerParams(vmem_limit_bytes=60 * 1024 * 1024),
        name="solve_first" if first else "solve_next",
    )(plan, *arrays)


def shrink(amount, cutoff):
    return amount - jnp.clip(amount, -cutoff, cutoff)


def on_device(tile_data, tile_row, tile_col, tile_count, touched, owner_map, observed, start_x, start_u):
    shards = lax.axis_size(AXES)
    local_cols = touched.shape[1]
    col_blocks = owner_map.shape[0]
    col_dev = col_blocks // shards
    plan = tile_plan(tile_row[0], tile_col[0], tile_count[0])
    wanted = touched[0]
    matches = (wanted[:, None] == jnp.arange(col_blocks, dtype=jnp.int32)[None, :]).astype(jnp.int32)
    position = jnp.sum(matches * owner_map[None, :], axis=1)
    owner = position // col_dev
    local_slot = position - owner * col_dev
    tags = jnp.full((shards,), -1, jnp.int32).at[owner].set(local_slot)
    arrived = lax.all_to_all(tags.reshape(shards, 1), AXES, split_axis=0, concat_axis=0, tiled=True).reshape(-1)
    delivery = (arrived[None, :] == jnp.arange(col_dev, dtype=jnp.int32)[:, None]).astype(F32)
    share = jnp.maximum(jnp.sum(delivery, axis=1), 1.0)[:, None, None]
    flip = lambda a: jnp.swapaxes(a, 1, 2)
    x, u, b = flip(start_x), flip(start_u), flip(observed)
    block = x.shape[1:]

    def consensus(merged):
        outbox = jnp.zeros((shards,) + block, F32).at[owner].set(merged)
        inbox = lax.all_to_all(outbox, AXES, split_axis=0, concat_axis=0, tiled=True)
        summed = jnp.einsum("dy,ysh->dsh", delivery, inbox, precision=lax.Precision.HIGHEST)
        z = shrink(summed / share, 1.0 / share)
        back = jnp.einsum("pu,pxa->uxa", delivery, z, precision=lax.Precision.HIGHEST)
        returned = lax.all_to_all(back, AXES, split_axis=0, concat_axis=0, tiled=True)
        return z, returned[owner]

    z, z_local = consensus(x + u)
    x1, r1, u1, _ = solve(True, plan, tile_data, b, x, u, z_local)
    z, z_next = consensus(x1 + u1)
    x2, u2, gap = solve(False, plan, tile_data, x1, u1, z_next, z_local, r1)
    total = lax.psum(jnp.sum(gap, axis=1), AXES)
    primal_gap = jnp.sqrt(total / (shards * local_cols * start_x.shape[1]))
    return flip(x2), flip(u2), flip(z), primal_gap


def solution(mesh):
    split = P(AXES)
    return jax.shard_map(
        on_device, mesh=mesh,
        in_specs=(split, split, split, split, split, P(), split, split, split),
        out_specs=(split, split, split, P()),
        check_vma=False,
    )
```

```python
import functools

import jax
import jax.numpy as jnp
from jax import lax
from jax.experimental import pallas as pl
from jax.experimental.pallas import tpu as pltpu
from jax.sharding import PartitionSpec as P

ITERS = 2
CG_STEPS = 4
GROUP = 8
AXES = ("dev", "ka")
F32 = jnp.float32
BF16 = jnp.bfloat16


def split_store(ref, index, value):
    rows = value.shape[0]
    high = value.astype(BF16)
    low = (value - high.astype(F32)).astype(BF16)
    ref[index, :rows, :] = high
    ref[index, rows:, :] = low


def join(wide, rows, cols):
    return (wide[:rows, :cols] + wide[:rows, cols:]) + wide[rows:, :cols]


def tile_plan(rows, cols, count):
    tiles = rows.shape[0]
    place = jnp.arange(tiles, dtype=jnp.int32)
    used = place < count

    def order(key):
        code = jnp.where(used, key, tiles) * tiles + place
        rank = jnp.sum((code[None, :] < code[:, None]).astype(jnp.int32), axis=1)
        pick = rank[None, :] == place[:, None]
        return rank, pick

    def take(pick, values):
        return jnp.sum(jnp.where(pick, values[None, :], 0), axis=1)

    row_key = jnp.where(used, rows, tiles)
    col_key = jnp.where(used, cols, tiles)
    rank_f, pick_f = order(rows)
    rank_b, pick_b = order(cols)
    row_sorted = take(pick_f, row_key)
    col_sorted = take(pick_b, col_key)
    before = lambda s: jnp.concatenate([jnp.full((1,), -1, jnp.int32), s[:-1]])
    after = lambda s: jnp.concatenate([s[1:], jnp.full((1,), -1, jnp.int32)])
    keep_f = (row_sorted == before(row_sorted)).astype(jnp.int32)
    keep_b = (col_sorted == before(col_sorted)).astype(jnp.int32)
    ends_f = ((row_sorted != after(row_sorted)) & (row_sorted < tiles)).astype(jnp.int32)
    last_of_row = jnp.max(jnp.where(row_key[:, None] == row_key[None, :], rank_f[None, :], 0), axis=1)
    column = jnp.arange(tiles, dtype=jnp.int32)
    last_of_col = jnp.max(jnp.where(col_key[None, :] == column[:, None], rank_b[None, :] + 1, 0), axis=1)
    last_of_col = jnp.where(last_of_col == 0, tiles, last_of_col - 1)
    return jnp.stack([
        take(pick_f, place), take(pick_f, cols), keep_f, ends_f, jnp.minimum(row_sorted, 31),
        take(pick_b, place), take(pick_b, last_of_row), keep_b, last_of_col,
    ])


def make_passes(plan, tiles_hl, image_hl, back, slots, targets, blk):
    count = slots

    def forward(source_hl, observed=None, square=False):
        def group(g, carry):
            acc, total = carry
            for n in range(GROUP):
                k = g * GROUP + n
                tile = plan[0, k]
                wide = lax.dot_general(
                    source_hl[plan[1, k]], tiles_hl[tile], (((1,), (1,)), ((), ())),
                    preferred_element_type=F32)
                acc = jnp.where(plan[2, k] > 0, acc, 0.0) + join(wide, targets, blk)
                if square:
                    total = total + jnp.where(plan[3, k] > 0, acc * acc, 0.0)
                elif observed is not None:
                    split_store(image_hl, k, observed[plan[4, k]] - acc)
                else:
                    split_store(image_hl, k, acc)
            return acc, total

        zero = jnp.zeros((targets, blk), F32)
        return lax.fori_loop(0, count // GROUP, group, (zero, zero))[1]

    def backward():
        def group(g, acc):
            for n in range(GROUP):
                k = g * GROUP + n
                both = tiles_hl[plan[5, k]]
                weights = jnp.concatenate([both[:blk], both[blk:]], axis=1)
                wide = jnp.dot(image_hl[plan[6, k]], weights, preferred_element_type=F32)
                acc = jnp.where(plan[7, k] > 0, acc, 0.0) + join(wide, targets, blk)
                back[k] = acc
            return acc

        lax.fori_loop(0, count // GROUP, group, jnp.zeros((targets, blk), F32))

    return forward, backward


def over_slots(slots, body, *init):
    step = 4

    def group(g, carry):
        for n in range(step):
            carry = body(g * step + n, *carry)
        return carry

    return lax.fori_loop(0, slots // step, group, init)


def total_of(value):
    return jnp.sum(value, axis=1, keepdims=True)


def solve_kernel(first, *refs):
    if first:
        (plan, tiles, observed, x, u, z, x_out, r_out, u_out, gap_out,
         tiles_hl, p, p_hl, image_hl, back) = refs
    else:
        (plan, tiles, x, u, z, z_before, r_in, x_out, u_out, gap_out,
         r_out, tiles_hl, p, p_hl, image_hl, back) = refs
    slots, targets, blk = x.shape
    zero = jnp.zeros((targets, blk), F32)
    back[slots] = zero

    def split_tile(t, _):
        split_store(tiles_hl, t, tiles[t])
        return _

    lax.fori_loop(0, slots, split_tile, 0)
    forward, backward = make_passes(plan, tiles_hl, image_hl, back, slots, targets, blk)

    if first:
        def load_x(c, _):
            split_store(p_hl, c, x[c])
            return (_,)

        over_slots(slots, load_x, 0)
        forward(p_hl, observed=observed)
        backward()

    def begin(c, rr, gap):
        diff = x[c] - z[c]
        u_new = u[c] + diff
        u_out[c] = u_new
        if first:
            r = back[plan[8, c]] + (z[c] - u_new) - x[c]
        else:
            r = r_in[c] + ((z[c] - u_new) - (z_before[c] - u[c]))
        r_out[c] = r
        p[c] = r
        split_store(p_hl, c, r)
        x_out[c] = x[c]
        return rr + r * r, gap + diff * diff

    rr, gap = over_slots(slots, begin, zero, zero)
    gap_out[...] = gap
    rr = total_of(rr)

    def advance(a, update_p, rr):
        def move(c, nn):
            r = r_out[c] - a * (back[plan[8, c]] + p[c])
            r_out[c] = r
            x_out[c] = x_out[c] + a * p[c]
            return (nn + r * r,)

        (nn,) = over_slots(slots, move, zero)
        nn = total_of(nn)
        if update_p:
            ratio = nn / rr

            def turn(c, _):
                value = r_out[c] + ratio * p[c]
                p[c] = value
                split_store(p_hl, c, value)
                return (_,)

            over_slots(slots, turn, 0)
        return nn

    def length(c, pq):
        value = p[c]
        return (pq + value * (back[plan[8, c]] + value),)

    def step(_, rr):
        forward(p_hl)
        backward()
        (pq,) = over_slots(slots, length, zero)
        return advance(rr / total_of(pq), True, rr)

    rr = lax.fori_loop(0, CG_STEPS - 1, step, rr)
    if first:
        forward(p_hl)
        backward()
        (pq,) = over_slots(slots, length, zero)
        advance(rr / total_of(pq), False, rr)
    else:
        square = forward(p_hl, square=True)

        def own(c, total):
            return (total + p[c] * p[c],)

        (pp,) = over_slots(slots, own, square)
        a = rr / total_of(pp)

        def finish(c, _):
            x_out[c] = x_out[c] + a * p[c]
            return (_,)

        over_slots(slots, finish, 0)


def solve(first, plan, *arrays):
    tiles = arrays[0]
    x = arrays[2] if first else arrays[1]
    slots, targets, blk = x.shape
    like = jax.ShapeDtypeStruct(x.shape, F32)
    gap = jax.ShapeDtypeStruct((targets, blk), F32)
    work = [
        pltpu.VMEM((tiles.shape[0], 2 * blk, blk), BF16),
        pltpu.VMEM(x.shape, F32),
        pltpu.VMEM((slots, 2 * targets, blk), BF16),
        pltpu.VMEM((slots, 2 * targets, blk), BF16),
        pltpu.VMEM((slots + 1, targets, blk), F32),
    ]
    if first:
        outs = (like, like, like, gap)
    else:
        outs = (like, like, gap)
        work = [pltpu.VMEM(x.shape, F32)] + work
    whole = pl.BlockSpec(memory_space=pltpu.VMEM)
    return pl.pallas_call(
        functools.partial(solve_kernel, first),
        out_shape=outs,
        in_specs=[pl.BlockSpec(memory_space=pltpu.SMEM)] + [whole] * len(arrays),
        out_specs=tuple(whole for _ in outs),
        scratch_shapes=work,
        compiler_params=pltpu.CompilerParams(vmem_limit_bytes=60 * 1024 * 1024),
        name="solve_first" if first else "solve_next",
    )(plan, *arrays)

SIDE = 4
ORDERS = (("x", "y", "z"), ("y", "z", "x"), ("z", "x", "y"))
PART_TILES = (3, 3, 2)
SUB = 8
PER = 4
S1, S1F, S2F, S2S, S2D, S3, T3, T2O, T2F, T2D, T1, T1F, SEMS = 0, 8, 9, 10, 11, 12, 16, 20, 21, 22, 23, 31, 32


def exchange_plan(owner, slot_tag, shards):
    y, x, core, z = owner // 32, (owner // 8) % 4, (owner // 4) % 2, owner % 4
    place = {"x": x, "y": y, "z": z}
    index = jnp.stack([place[a] * 32 + core * 16 + place[b] * 4 + place[c] for a, b, c in ORDERS])
    match = index[:, :, None] == jnp.arange(shards, dtype=jnp.int32)[None, None, :]
    number = jnp.arange(owner.shape[0], dtype=jnp.int32)
    slot = jnp.sum(jnp.where(match, number[None, :, None], 0), axis=1)
    tag = jnp.sum(jnp.where(match, slot_tag[None, :, None] + 1, 0), axis=1) - 1
    index = jnp.pad(index, ((0, 0), (0, shards - owner.shape[0])))
    return jnp.concatenate([slot, tag, index])


def exchange_kernel(table, x_in, u_in, z_local, z_own, *scratch):
    parts = len(ORDERS)
    boxes = [scratch[n * parts:(n + 1) * parts] for n in range(12)]
    mail, in1, fwd1, part2, fwd2, in2, part3, in3, zb2, inbox, sel, zrel = boxes
    send_sem, recv_sem = scratch[12 * parts:]
    slots, targets, blk = x_in.shape
    dev, z = lax.axis_index("dev"), lax.axis_index("ka")
    core = lax.rem(dev, 2)
    me = {"x": lax.rem(dev // 2, SIDE), "y": dev // 8, "z": z}
    way = 1 - 2 * core

    def near(axis, delta, to_core):
        at = dict(me)
        at[axis] = lax.rem(me[axis] + delta + SIDE, SIDE)
        return ((at["y"] * SIDE + at["x"]) * 2 + to_core, at["z"])

    barrier = pltpu.get_barrier_semaphore()
    friends = [near("x", 0, 1 - core)]
    for axis in ("x", "y", "z"):
        friends += [near(axis, 2, core)]
        friends += [near(axis, delta, c) for delta in (1, -1) for c in (0, 1)]
    for friend in friends:
        pl.semaphore_signal(barrier, inc=1, device_id=friend, device_id_type=pl.DeviceIdType.MESH)

    def pack(p):
        tiles = PART_TILES[p]
        base = sum(PART_TILES[:p]) * SUB
        rows = tiles * SUB

        def record(q, _):
            for i in range(16):
                slot = table[p, q * 16 + i]
                tag = table[parts + p, q * 16 + i]
                where = pl.ds(base, rows)
                mail[p][q, i * rows:(i + 1) * rows, :] = x_in[slot, where, :] + u_in[slot, where, :]
                mail[p][q, 16 * rows + i:16 * rows + i + 1, :] = jnp.full((1, blk), tag, jnp.int32).astype(F32)
            return _

        lax.fori_loop(0, 8, record, 0)

    sends = []

    def copy(p, src, dst, send, recv, device):
        return pltpu.make_async_remote_copy(
            src_ref=src, dst_ref=dst, send_sem=send_sem.at[p, send], recv_sem=recv_sem.at[p, recv],
            device_id=device, device_id_type=pl.DeviceIdType.MESH)

    def go(p, src, dst, send, recv, device):
        moving = copy(p, src, dst, send, recv, device)
        moving.start()
        sends.append(moving)

    def arrive(p, dst, recv):
        copy(p, dst, dst, 0, recv, near("x", 0, 1 - core)).wait_recv()

    ring = lambda a, delta: lax.rem(me[a] + delta + SIDE, SIDE)

    def scatter_start(p, box, into, relay, base, base_f):
        a = ORDERS[p][0]
        go(p, box(ring(a, 2), None), relay, base_f, base_f, near(a, way, core))
        for delta in (1, 3):
            for c in (0, 1):
                go(p, box(ring(a, delta), c), into(delta), base + delta * 2 + c, base + delta * 2 + core, near(a, delta, c))
        go(p, box(me[a], 1 - core), into(0), base, base + core, near(a, 0, 1 - core))

    def scatter_relay(p, relay, into, base, base_f):
        a = ORDERS[p][0]
        arrive(p, relay(None), base_f)
        for c in (0, 1):
            go(p, relay(c), into, base + 4 + c, base + 4 + core, near(a, way, c))

    def mail_box(p):
        return lambda at, c: mail[p].at[pl.ds(at * 2, 2)] if c is None else mail[p].at[at * 2 + c]

    for p in range(parts):
        pack(p)
        if p == 0:
            pl.semaphore_wait(barrier, len(friends))
        scatter_start(p, mail_box(p), lambda delta: in1[p].at[delta * 2 + core], fwd1[p], S1, S1F)
    for p in range(parts):
        relay = lambda c: fwd1[p] if c is None else fwd1[p].at[c]
        scatter_relay(p, relay, in1[p].at[4 + core], S1, S1F)

    def sources(p):
        a = ORDERS[p][0]
        own = lambda rows: mail[p][me[a] * 2 + core, rows, :]
        found = [(0, core, own)]
        for delta, c in ((0, 1 - core), (1, 0), (1, 1), (2, 0), (2, 1), (3, 0), (3, 1)):
            found.append((delta, c, lambda rows, n=delta * 2 + c: in1[p][n, rows, :]))
        return found

    def combine(p):
        tiles = PART_TILES[p]
        rows = tiles * SUB
        width = PER * rows + SUB
        found = sources(p)

        def some(a2, _):
            for a3 in range(SIDE):
                i = a2 * SIDE + a3
                tags = [jnp.broadcast_to(read(pl.ds(16 * rows + i, 1)), (SUB, blk)) for _, _, read in found]
                hits = [[tag == float(k) for tag in tags] for k in range(PER)]
                for j in range(tiles):
                    at = pl.multiple_of(i * rows + j * SUB, SUB)
                    data = [read(pl.ds(at, SUB)) for _, _, read in found]
                    for k in range(PER):
                        acc = functools.reduce(
                            lambda s, n: s + n, [jnp.where(h, v, 0.0) for h, v in zip(hits[k], data)])
                        start = a3 * width + k * rows + j * SUB
                        part2[p][a2, start:start + SUB, :] = acc
                for k in range(PER):
                    number = functools.reduce(lambda s, n: s + n, [jnp.where(h, 1.0, 0.0) for h in hits[k]])
                    start = a3 * width + PER * rows + k
                    part2[p][a2, start:start + 1, :] = number[:1]
                start = a3 * width + PER * rows + PER
                part2[p][a2, start:start + SUB - PER, :] = jnp.zeros((SUB - PER, blk), F32)
            return _

        lax.fori_loop(0, SIDE, some, 0)

    for p in range(parts):
        for delta, c in ((1, 0), (1, 1), (3, 0), (3, 1), (2, 0), (2, 1), (0, 1 - core)):
            arrive(p, in1[p].at[delta * 2 + c], S1 + delta * 2 + c)
        combine(p)
        b = ORDERS[p][1]
        go(p, part2[p].at[ring(b, 2)], fwd2[p], S2F, S2F, near(b, way, core))
        go(p, part2[p].at[ring(b, -way)], in2[p].at[1], S2D, S2D, near(b, -way, core))
    for p in range(parts):
        b = ORDERS[p][1]
        arrive(p, fwd2[p], S2F)
        at = ring(b, way)
        part2[p][at] = part2[p][at] + fwd2[p][...]
        go(p, part2[p].at[at], in2[p].at[0], S2S, S2S, near(b, way, core))
    for p in range(parts):
        b, c3 = ORDERS[p][1], ORDERS[p][2]
        width = PER * PART_TILES[p] * SUB + SUB
        arrive(p, in2[p].at[1], S2D)
        arrive(p, in2[p].at[0], S2S)
        whole = part2[p][me[b]] + in2[p][0] + in2[p][1]
        for a3 in range(SIDE):
            part3[p][a3] = whole[a3 * width:(a3 + 1) * width]
        for delta in (1, 2, 3):
            go(p, part3[p].at[ring(c3, delta)], in3[p].at[delta - 1], S3 + delta, S3 + delta, near(c3, delta, core))
    for p in range(parts):
        b, c3 = ORDERS[p][1], ORDERS[p][2]
        rows = PART_TILES[p] * SUB
        base = sum(PART_TILES[:p]) * SUB
        for delta in (1, 2, 3):
            arrive(p, in3[p].at[delta - 1], S3 + delta)
        whole = ((part3[p][me[c3]] + in3[p][0]) + in3[p][1]) + in3[p][2]
        for k in range(PER):
            number = whole[PER * rows + k:PER * rows + k + 1]
            share = jnp.maximum(number, 1.0)
            value = whole[k * rows:(k + 1) * rows] / share
            cut = jnp.broadcast_to(1.0 / share, value.shape)
            value = value - jnp.minimum(jnp.maximum(value, -cut), cut)
            z_own[k, base:base + rows, :] = value
            zb2[p][me[b], me[c3], k * rows:(k + 1) * rows, :] = value
        own = zb2[p].at[me[b], me[c3]]
        for delta in (1, 2, 3):
            go(p, own, own, T3 + delta, T3 + delta, near(c3, delta, core))
    for p in range(parts):
        b, c3 = ORDERS[p][1], ORDERS[p][2]
        for delta in (1, 2, 3):
            arrive(p, zb2[p].at[me[b], ring(c3, -delta)], T3 + delta)
        own = zb2[p].at[me[b]]
        go(p, own, own, T2O, T2O, near(b, way, core))
        go(p, own, own, T2D, T2D, near(b, -way, core))
    for p in range(parts):
        b = ORDERS[p][1]
        passing = zb2[p].at[ring(b, -way)]
        arrive(p, passing, T2O)
        go(p, passing, passing, T2F, T2F, near(b, way, core))

    def select(p):
        tiles = PART_TILES[p]
        rows = tiles * SUB
        a = ORDERS[p][0]
        found = sources(p)

        def some(a2, _):
            for a3 in range(SIDE):
                i = a2 * SIDE + a3
                blocks = [zb2[p][a2, a3, n * SUB:(n + 1) * SUB, :] for n in range(PER * tiles)]
                for number, (delta, c, read) in enumerate(found):
                    tag = jnp.broadcast_to(read(pl.ds(16 * rows + i, 1)), (SUB, blk))
                    hit = [tag == float(k) for k in range(PER - 1)]
                    for j in range(tiles):
                        value = blocks[(PER - 1) * tiles + j]
                        for k in range(PER - 1):
                            value = jnp.where(hit[k], blocks[k * tiles + j], value)
                        if number == 0:
                            inbox[p][(me[a] * 2 + core) * 16 + i, j * SUB:(j + 1) * SUB, :] = value
                        else:
                            sel[p][(ring(a, -delta) * 2 + c) * 16 + i, j * SUB:(j + 1) * SUB, :] = value
            return _

        lax.fori_loop(0, SIDE, some, 0)

    for p in range(parts):
        a, b = ORDERS[p][0], ORDERS[p][1]
        arrive(p, zb2[p].at[ring(b, way)], T2D)
        arrive(p, zb2[p].at[ring(b, 2)], T2F)
        select(p)
        box = lambda at, c: sel[p].at[pl.ds(at * 32, 32)] if c is None else sel[p].at[pl.ds((at * 2 + c) * 16, 16)]
        mine = inbox[p].at[pl.ds((me[a] * 2 + core) * 16, 16)]
        scatter_start(p, box, lambda delta: mine, zrel[p], T1, T1F)
    for p in range(parts):
        a = ORDERS[p][0]
        relay = lambda c: zrel[p] if c is None else zrel[p].at[pl.ds(c * 16, 16)]
        scatter_relay(p, relay, inbox[p].at[pl.ds((ring(a, -way) * 2 + core) * 16, 16)], T1, T1F)

    def unpack(p):
        rows = PART_TILES[p] * SUB
        base = sum(PART_TILES[:p]) * SUB

        def group(g, _):
            for n in range(8):
                c = g * 8 + n
                z_local[c, base:base + rows, :] = inbox[p][table[2 * parts + p, c]]
            return _

        lax.fori_loop(0, slots // 8, group, 0)

    for p in range(parts):
        a = ORDERS[p][0]
        for delta, c in ((1, 0), (1, 1), (3, 0), (3, 1), (2, 0), (2, 1), (0, 1 - core)):
            arrive(p, inbox[p].at[pl.ds((ring(a, -delta) * 2 + c) * 16, 16)], T1 + delta * 2 + c)
        unpack(p)
    for moving in sends:
        moving.wait_send()


def exchange(number, table, x, u):
    slots, targets, blk = x.shape
    each = lambda shape: [pltpu.VMEM(shape(t * SUB), F32) for t in PART_TILES]
    scratch = (
        each(lambda r: (8, 16 * r + 16, blk)) + each(lambda r: (8, 16 * r + 16, blk))
        + each(lambda r: (2, 16 * r + 16, blk)) + each(lambda r: (SIDE, SIDE * (PER * r + SUB), blk))
        + each(lambda r: (SIDE * (PER * r + SUB), blk)) + each(lambda r: (2, SIDE * (PER * r + SUB), blk))
        + each(lambda r: (SIDE, PER * r + SUB, blk)) + each(lambda r: (3, PER * r + SUB, blk))
        + each(lambda r: (SIDE, SIDE, PER * r, blk)) + each(lambda r: (128, r, blk))
        + each(lambda r: (128, r, blk)) + each(lambda r: (32, r, blk))
        + [pltpu.SemaphoreType.DMA((len(ORDERS), SEMS)), pltpu.SemaphoreType.DMA((len(ORDERS), SEMS))]
    )
    whole = pl.BlockSpec(memory_space=pltpu.VMEM)
    return pl.pallas_call(
        exchange_kernel,
        out_shape=(jax.ShapeDtypeStruct(x.shape, F32), jax.ShapeDtypeStruct((PER, targets, blk), F32)),
        in_specs=[pl.BlockSpec(memory_space=pltpu.SMEM), whole, whole],
        out_specs=(whole, whole),
        scratch_shapes=scratch,
        compiler_params=pltpu.CompilerParams(
            collective_id=number, has_side_effects=True, vmem_limit_bytes=60 * 1024 * 1024),
        name="exchange",
    )(table, x, u)


def on_device(tile_data, tile_row, tile_col, tile_count, touched, owner_map, observed, start_x, start_u):
    shards = lax.axis_size(AXES)
    local_cols = touched.shape[1]
    col_blocks = owner_map.shape[0]
    col_dev = col_blocks // shards
    plan = tile_plan(tile_row[0], tile_col[0], tile_count[0])
    wanted = touched[0]
    matches = (wanted[:, None] == jnp.arange(col_blocks, dtype=jnp.int32)[None, :]).astype(jnp.int32)
    position = jnp.sum(matches * owner_map[None, :], axis=1)
    owner = position // col_dev
    local_slot = position - owner * col_dev
    table = exchange_plan(owner, local_slot, shards)
    flip = lambda a: jnp.swapaxes(a, 1, 2)
    x, u, b = flip(start_x), flip(start_u), flip(observed)
    z_local, z = exchange(0, table, x, u)
    x1, r1, u1, _ = solve(True, plan, tile_data, b, x, u, z_local)
    z_next, z = exchange(1, table, x1, u1)
    x2, u2, gap = solve(False, plan, tile_data, x1, u1, z_next, z_local, r1)
    total = lax.psum(jnp.sum(gap, axis=1), AXES)
    primal_gap = jnp.sqrt(total / (shards * local_cols * start_x.shape[1]))
    return flip(x2), flip(u2), flip(z), primal_gap


def solution(mesh):
    split = P(AXES)
    return jax.shard_map(
        on_device, mesh=mesh,
        in_specs=(split, split, split, split, split, P(), split, split, split),
        out_specs=(split, split, split, P()),
        check_vma=False,
    )
```

```python
import functools

import jax
import jax.numpy as jnp
from jax import lax
from jax.experimental import pallas as pl
from jax.experimental.pallas import tpu as pltpu
from jax.sharding import PartitionSpec as P

ITERS = 2
CG_STEPS = 4
GROUP = 16
AXES = ("dev", "ka")
F32 = jnp.float32
BF16 = jnp.bfloat16
MESH = pl.DeviceIdType.MESH

SIDE = 4
SUB = 8
PER = 4
ORDERS = (("x", "y", "z"), ("y", "z", "x"), ("z", "x", "y"))
SETS = ((3, 3, 2),)
S1, S1F, S2F, S2S, S2D, S3, T3, T2O, T2F, T2D, T1, T1F, SEMS = 0, 8, 9, 10, 11, 12, 16, 20, 21, 22, 23, 31, 32
BOXES = 12


def fold(values):
    return functools.reduce(lambda s, n: s + n, values)


def split_store(ref, index, value):
    rows = value.shape[0]
    high = value.astype(BF16)
    low = (value - high.astype(F32)).astype(BF16)
    ref[index, :rows, :] = high
    ref[index, rows:, :] = low


def join(wide, rows, cols):
    return (wide[:rows, :cols] + wide[:rows, cols:]) + wide[rows:, :cols]


def total_of(value):
    return jnp.sum(value, axis=1, keepdims=True)


def tile_plan(rows, cols, count):
    tiles = rows.shape[0]
    place = jnp.arange(tiles, dtype=jnp.int32)
    used = place < count

    def order(key):
        code = jnp.where(used, key, tiles) * tiles + place
        rank = jnp.sum((code[None, :] < code[:, None]).astype(jnp.int32), axis=1)
        pick = rank[None, :] == place[:, None]
        return rank, pick

    def take(pick, values):
        return jnp.sum(jnp.where(pick, values[None, :], 0), axis=1)

    row_key = jnp.where(used, rows, tiles)
    col_key = jnp.where(used, cols, tiles)
    rank_f, pick_f = order(rows)
    rank_b, pick_b = order(cols)
    row_sorted = take(pick_f, row_key)
    col_sorted = take(pick_b, col_key)
    before = lambda s: jnp.concatenate([jnp.full((1,), -1, jnp.int32), s[:-1]])
    after = lambda s: jnp.concatenate([s[1:], jnp.full((1,), -1, jnp.int32)])
    keep_f = (row_sorted == before(row_sorted)).astype(jnp.int32)
    keep_b = (col_sorted == before(col_sorted)).astype(jnp.int32)
    ends_f = ((row_sorted != after(row_sorted)) & (row_sorted < tiles)).astype(jnp.int32)
    last_of_row = jnp.max(jnp.where(row_key[:, None] == row_key[None, :], rank_f[None, :], 0), axis=1)
    column = jnp.arange(tiles, dtype=jnp.int32)
    last_of_col = jnp.max(jnp.where(col_key[None, :] == column[:, None], rank_b[None, :] + 1, 0), axis=1)
    last_of_col = jnp.where(last_of_col == 0, tiles, last_of_col - 1)
    return jnp.stack([
        take(pick_f, place), take(pick_f, cols), keep_f, ends_f, jnp.minimum(row_sorted, 31),
        take(pick_b, place), take(pick_b, last_of_row), keep_b, last_of_col,
    ])

def exchange_plan(owner, slot_tag, shards):
    y, x, core, z = owner // 32, (owner // 8) % 4, (owner // 4) % 2, owner % 4
    place = {"x": x, "y": y, "z": z}
    index = jnp.stack([place[a] * 32 + core * 16 + place[b] * 4 + place[c] for a, b, c in ORDERS])
    match = index[:, :, None] == jnp.arange(shards, dtype=jnp.int32)[None, None, :]
    number = jnp.arange(owner.shape[0], dtype=jnp.int32)
    slot = jnp.sum(jnp.where(match, number[None, :, None], 0), axis=1)
    tag = jnp.sum(jnp.where(match, slot_tag[None, :, None] + 1, 0), axis=1) - 1
    index = jnp.pad(index, ((0, 0), (0, shards - owner.shape[0])))
    return jnp.concatenate([slot, tag, index])


def loop(count, step, body, *init):
    def group(g, carry):
        for n in range(step):
            carry = body(g * step + n, *carry)
        return carry

    return lax.fori_loop(0, count // step, group, init)


def near_device(me, axis, delta, to_core):
    at = dict(me)
    at[axis] = lax.rem(me[axis] + delta + SIDE, SIDE)
    return ((at["y"] * SIDE + at["x"]) * 2 + to_core, at["z"])


class Place:
    def __init__(self):
        dev, z = lax.axis_index("dev"), lax.axis_index("ka")
        self.core = lax.rem(dev, 2)
        self.me = {"x": lax.rem(dev // 2, SIDE), "y": dev // 8, "z": z}
        self.way = 1 - 2 * self.core
        self.partner = (dev + 1 - 2 * self.core, z)

    def near(self, axis, delta, to_core=None):
        return near_device(self.me, axis, delta, self.core if to_core is None else to_core)

    def ring(self, axis, delta):
        return lax.rem(self.me[axis] + delta + SIDE, SIDE)


class Exchange:
    def __init__(self, at, table, tiles, base, boxes, send_sem, recv_sem):
        self.at, self.table, self.tiles = at, table, tiles
        self.base = [(base + sum(tiles[:p])) * SUB for p in range(len(tiles))]
        (self.mail, self.in1, self.fwd1, self.part2, self.fwd2, self.in2, self.part3, self.in3,
         self.zb2, self.inbox, self.sel, self.zrel) = boxes
        self.send_sem, self.recv_sem = send_sem, recv_sem
        self.sends = []
        self.parts = range(len(tiles))

    def copy(self, p, src, dst, send, recv, device):
        return pltpu.make_async_remote_copy(
            src_ref=src, dst_ref=dst, send_sem=self.send_sem.at[p, send], recv_sem=self.recv_sem.at[p, recv],
            device_id=device, device_id_type=MESH)

    def go(self, p, src, dst, send, recv, device):
        moving = self.copy(p, src, dst, send, recv, device)
        moving.start()
        self.sends.append(moving)

    def arrive(self, p, dst, recv):
        self.copy(p, dst, dst, 0, recv, self.at.partner).wait_recv()

    def sent(self):
        for moving in self.sends:
            moving.wait_send()
        self.sends = []

    def pack(self, p, x, u):
        rows = self.tiles[p] * SUB
        where = pl.ds(self.base[p], rows)
        table, parts, mail = self.table, len(ORDERS), self.mail[p]

        def record(q, _):
            for i in range(16):
                slot = table[p, q * 16 + i]
                tag = table[parts + p, q * 16 + i]
                mail[q, i * rows:(i + 1) * rows, :] = x[slot, where, :] + u[slot, where, :]
                mail[q, 16 * rows + i:16 * rows + i + 1, :] = jnp.full((1, x.shape[2]), tag, jnp.int32).astype(F32)
            return (_,)

        loop(8, 1, record, 0)

    def scatter(self, p, box, into, relay, base, base_f):
        at, a, core = self.at, ORDERS[p][0], self.at.core
        self.go(p, box(at.ring(a, 2), None), relay, base_f, base_f, at.near(a, at.way))
        for delta in (1, 3):
            for c in (0, 1):
                self.go(p, box(at.ring(a, delta), c), into(delta), base + delta * 2 + c,
                        base + delta * 2 + core, at.near(a, delta, c))
        self.go(p, box(at.me[a], 1 - core), into(0), base, base + core, at.partner)

    def relay(self, p, relay, into, base, base_f):
        at, a = self.at, ORDERS[p][0]
        self.arrive(p, relay(None), base_f)
        for c in (0, 1):
            self.go(p, relay(c), into, base + 4 + c, base + 4 + at.core, at.near(a, at.way, c))

    def start(self, p, x, u):
        self.pack(p, x, u)

        def box(place, c):
            return self.mail[p].at[pl.ds(place * 2, 2)] if c is None else self.mail[p].at[place * 2 + c]

        return lambda: self.scatter(
            p, box, lambda delta: self.in1[p].at[delta * 2 + self.at.core], self.fwd1[p], S1, S1F)

    def pass_on(self):
        for p in self.parts:
            fwd = self.fwd1[p]
            self.relay(p, lambda c: fwd if c is None else fwd.at[c], self.in1[p].at[4 + self.at.core], S1, S1F)

    def sources(self, p):
        at, a = self.at, ORDERS[p][0]
        mail, in1 = self.mail[p], self.in1[p]
        found = [(0, at.core, lambda rows: mail[at.me[a] * 2 + at.core, rows, :])]
        for delta, c in ((0, 1 - at.core), (1, 0), (1, 1), (2, 0), (2, 1), (3, 0), (3, 1)):
            found.append((delta, c, lambda rows, n=delta * 2 + c: in1[n, rows, :]))
        return found

    def others(self):
        return ((1, 0), (1, 1), (3, 0), (3, 1), (0, 1 - self.at.core), (2, 0), (2, 1))

    def combine(self, p):
        tiles = self.tiles[p]
        rows = tiles * SUB
        width = PER * rows + SUB
        found = self.sources(p)
        part2 = self.part2[p]
        blk = part2.shape[2]

        def some(a2, _):
            for a3 in range(SIDE):
                i = a2 * SIDE + a3
                tags = [jnp.broadcast_to(read(pl.ds(16 * rows + i, 1)), (SUB, blk)) for _, _, read in found]
                hits = [[tag == float(k) for tag in tags] for k in range(PER)]
                for j in range(tiles):
                    place = pl.multiple_of(i * rows + j * SUB, SUB)
                    data = [read(pl.ds(place, SUB)) for _, _, read in found]
                    for k in range(PER):
                        start = a3 * width + k * rows + j * SUB
                        part2[a2, start:start + SUB, :] = fold(
                            [jnp.where(h, v, 0.0) for h, v in zip(hits[k], data)])
                for k in range(PER):
                    start = a3 * width + PER * rows + k
                    part2[a2, start:start + 1, :] = fold([jnp.where(h, 1.0, 0.0) for h in hits[k]])[:1]
                start = a3 * width + PER * rows + PER
                part2[a2, start:start + SUB - PER, :] = jnp.zeros((SUB - PER, blk), F32)
            return (_,)

        loop(SIDE, 1, some, 0)

    def reduce_first(self):
        at = self.at
        for p in self.parts:
            b = ORDERS[p][1]
            for delta, c in self.others():
                self.arrive(p, self.in1[p].at[delta * 2 + c], S1 + delta * 2 + c)
            self.combine(p)
            self.go(p, self.part2[p].at[at.ring(b, 2)], self.fwd2[p], S2F, S2F, at.near(b, at.way))
            self.go(p, self.part2[p].at[at.ring(b, -at.way)], self.in2[p].at[1], S2D, S2D, at.near(b, -at.way))

    def reduce_second(self):
        at = self.at
        for p in self.parts:
            b = ORDERS[p][1]
            self.arrive(p, self.fwd2[p], S2F)
            to = at.ring(b, at.way)
            self.part2[p][to] = self.part2[p][to] + self.fwd2[p][...]
            self.go(p, self.part2[p].at[to], self.in2[p].at[0], S2S, S2S, at.near(b, at.way))

    def reduce_third(self):
        at = self.at
        for p in self.parts:
            b, d = ORDERS[p][1], ORDERS[p][2]
            width = PER * self.tiles[p] * SUB + SUB
            self.arrive(p, self.in2[p].at[1], S2D)
            self.arrive(p, self.in2[p].at[0], S2S)
            whole = self.part2[p][at.me[b]] + self.in2[p][0] + self.in2[p][1]
            for a3 in range(SIDE):
                self.part3[p][a3] = whole[a3 * width:(a3 + 1) * width]
            for delta in (2, 1, 3):
                self.go(p, self.part3[p].at[at.ring(d, delta)], self.in3[p].at[delta - 1],
                        S3 + delta, S3 + delta, at.near(d, delta))

    def agree(self, z_own):
        at = self.at
        for p in self.parts:
            b, d = ORDERS[p][1], ORDERS[p][2]
            rows, base = self.tiles[p] * SUB, self.base[p]
            for delta in (1, 3, 2):
                self.arrive(p, self.in3[p].at[delta - 1], S3 + delta)
            whole = ((self.part3[p][at.me[d]] + self.in3[p][0]) + self.in3[p][1]) + self.in3[p][2]
            for k in range(PER):
                number = whole[PER * rows + k:PER * rows + k + 1]
                share = jnp.maximum(number, 1.0)
                value = whole[k * rows:(k + 1) * rows] / share
                cut = jnp.broadcast_to(1.0 / share, value.shape)
                value = value - jnp.minimum(jnp.maximum(value, -cut), cut)
                z_own[k, base:base + rows, :] = value
                self.zb2[p][at.me[b], at.me[d], k * rows:(k + 1) * rows, :] = value
            own = self.zb2[p].at[at.me[b], at.me[d]]
            for delta in (2, 1, 3):
                self.go(p, own, own, T3 + delta, T3 + delta, at.near(d, delta))

    def spread_first(self):
        at = self.at
        for p in self.parts:
            b, d = ORDERS[p][1], ORDERS[p][2]
            for delta in (1, 3, 2):
                self.arrive(p, self.zb2[p].at[at.me[b], at.ring(d, -delta)], T3 + delta)
            own = self.zb2[p].at[at.me[b]]
            self.go(p, own, own, T2O, T2O, at.near(b, at.way))
            self.go(p, own, own, T2D, T2D, at.near(b, -at.way))

    def spread_second(self):
        at = self.at
        for p in self.parts:
            b = ORDERS[p][1]
            passing = self.zb2[p].at[at.ring(b, -at.way)]
            self.arrive(p, passing, T2O)
            self.go(p, passing, passing, T2F, T2F, at.near(b, at.way))

    def select(self, p):
        at = self.at
        tiles = self.tiles[p]
        rows = tiles * SUB
        a = ORDERS[p][0]
        found = self.sources(p)
        zb2, inbox, sel = self.zb2[p], self.inbox[p], self.sel[p]

        def some(a2, _):
            for a3 in range(SIDE):
                i = a2 * SIDE + a3
                blocks = [zb2[a2, a3, n * SUB:(n + 1) * SUB, :] for n in range(PER * tiles)]
                for number, (delta, c, read) in enumerate(found):
                    tag = jnp.broadcast_to(read(pl.ds(16 * rows + i, 1)), blocks[0].shape)
                    hit = [tag == float(k) for k in range(PER - 1)]
                    for j in range(tiles):
                        value = blocks[(PER - 1) * tiles + j]
                        for k in range(PER - 1):
                            value = jnp.where(hit[k], blocks[k * tiles + j], value)
                        place = (at.ring(a, -delta) * 2 + c) * 16 + i
                        (sel if number else inbox)[place, j * SUB:(j + 1) * SUB, :] = value
            return (_,)

        loop(SIDE, 1, some, 0)

    def give_back(self):
        at = self.at
        self.sent()
        for p in self.parts:
            a, b = ORDERS[p][0], ORDERS[p][1]
            self.arrive(p, self.zb2[p].at[at.ring(b, at.way)], T2D)
            self.arrive(p, self.zb2[p].at[at.ring(b, 2)], T2F)
            self.select(p)
            sel = self.sel[p]

            def box(place, c):
                return sel.at[pl.ds(place * 32, 32)] if c is None else sel.at[pl.ds((place * 2 + c) * 16, 16)]

            mine = self.inbox[p].at[pl.ds((at.me[a] * 2 + at.core) * 16, 16)]
            self.scatter(p, box, lambda delta: mine, self.zrel[p], T1, T1F)

    def give_on(self):
        at = self.at
        for p in self.parts:
            zrel, a = self.zrel[p], ORDERS[p][0]
            self.relay(p, lambda c: zrel if c is None else zrel.at[pl.ds(c * 16, 16)],
                       self.inbox[p].at[pl.ds((at.ring(a, -at.way) * 2 + at.core) * 16, 16)], T1, T1F)

    def finish(self):
        at = self.at
        for p in self.parts:
            a = ORDERS[p][0]
            for delta, c in self.others():
                self.arrive(p, self.inbox[p].at[pl.ds((at.ring(a, -delta) * 2 + c) * 16, 16)], T1 + delta * 2 + c)
        self.sent()

    def read(self, c):
        found = [self.inbox[p][self.table[2 * len(ORDERS) + p, c]] for p in self.parts]
        return jnp.concatenate(found, axis=0)


class Solver:
    def __init__(self, plan, tiles_hl, x, u, r, p, p_hl, image_hl, back, z_before):
        self.plan, self.tiles_hl = plan, tiles_hl
        self.x, self.u, self.r, self.p = x, u, r, p
        self.p_hl, self.image_hl, self.back, self.z_before = p_hl, image_hl, back, z_before
        self.slots, self.blk = p_hl.shape[0], p_hl.shape[2]
        self.targets = p_hl.shape[1] // 2
        self.zero = jnp.zeros((self.targets, self.blk), F32)

    def forward(self, observed=None, square=False):
        plan, targets, blk = self.plan, self.targets, self.blk

        def tile_step(k, acc, total):
            wide = lax.dot_general(
                self.p_hl[plan[1, k]], self.tiles_hl[plan[0, k]], (((1,), (1,)), ((), ())),
                preferred_element_type=F32)
            acc = jnp.where(plan[2, k] > 0, acc, 0.0) + join(wide, targets, blk)
            if square:
                total = total + jnp.where(plan[3, k] > 0, acc * acc, 0.0)
            elif observed is not None:
                split_store(self.image_hl, k, observed[plan[4, k]] - acc)
            else:
                split_store(self.image_hl, k, acc)
            return acc, total

        return loop(self.slots, GROUP, tile_step, self.zero, self.zero)[1]

    def backward(self):
        plan, targets, blk = self.plan, self.targets, self.blk

        def tile_step(k, acc):
            both = self.tiles_hl[plan[5, k]]
            weights = jnp.concatenate([both[:blk], both[blk:]], axis=1)
            wide = jnp.dot(self.image_hl[plan[6, k]], weights, preferred_element_type=F32)
            acc = jnp.where(plan[7, k] > 0, acc, 0.0) + join(wide, targets, blk)
            self.back[k] = acc
            return (acc,)

        loop(self.slots, GROUP, tile_step, self.zero)

    def load_x(self):
        def one(c, _):
            split_store(self.p_hl, c, self.x[c])
            return (_,)

        loop(self.slots, 4, one, 0)

    def begin(self, first, z_of):
        def one(c, rr, gap):
            z, x, u = z_of(c), self.x[c], self.u[c]
            diff = x - z
            u_new = u + diff
            self.u[c] = u_new
            if first:
                r = self.back[self.plan[8, c]] + (z - u_new) - x
                self.z_before[c] = z
            else:
                r = self.r[c] + ((z - u_new) - (self.z_before[c] - u))
            self.r[c] = r
            self.p[c] = r
            split_store(self.p_hl, c, r)
            return rr + r * r, gap + diff * diff

        rr, gap = loop(self.slots, 4, one, self.zero, self.zero)
        self.rr = total_of(rr)
        return gap

    def step(self, last):
        p, r, x, back, plan = self.p, self.r, self.x, self.back, self.plan
        self.forward()
        self.backward()

        def length(c, pq):
            value = p[c]
            return (pq + value * (back[plan[8, c]] + value),)

        (pq,) = loop(self.slots, 4, length, self.zero)
        a = self.rr / total_of(pq)

        def move(c, nn):
            value = p[c]
            new = r[c] - a * (back[plan[8, c]] + value)
            r[c] = new
            if last:
                x[c] = x[c] + a * value
            return (nn + new * new,)

        (nn,) = loop(self.slots, 4, move, self.zero)
        nn = total_of(nn)
        if last:
            return
        ratio = nn / self.rr

        def turn(c, _):
            value = p[c]
            x[c] = x[c] + a * value
            value = r[c] + ratio * value
            p[c] = value
            split_store(self.p_hl, c, value)
            return (_,)

        loop(self.slots, 4, turn, 0)
        self.rr = nn

    def end(self):
        square = self.forward(square=True)

        def own(c, total):
            return (total + self.p[c] * self.p[c],)

        (pp,) = loop(self.slots, 4, own, square)
        a = self.rr / total_of(pp)

        def move(c, _):
            self.x[c] = self.x[c] + a * self.p[c]
            return (_,)

        loop(self.slots, 4, move, 0)


def fused_kernel(plan, table, tiles_in, observed_in, x_in, u_in, x, u, z_own, gap_out, *scratch):
    (tiles, observed, tiles_hl, r, p, p_hl, image_hl, back, z_before, gap_box, local_sem, gap_send, gap_recv,
     send_sem, recv_sem) = scratch[BOXES * len(ORDERS):]
    boxes = [scratch[n * len(ORDERS):(n + 1) * len(ORDERS)] for n in range(BOXES)]
    loads = [pltpu.make_async_copy(src, dst, local_sem.at[n]) for n, (src, dst) in enumerate(
        ((x_in, x), (u_in, u), (tiles_in, tiles), (observed_in, observed)))]
    for load in loads:
        load.start()
    at = Place()
    barrier = pltpu.get_barrier_semaphore()
    friends = [at.partner]
    for axis in ("x", "y", "z"):
        friends += [at.near(axis, 2)] + [at.near(axis, delta, c) for delta in (1, -1) for c in (0, 1)]
    for friend in friends:
        pl.semaphore_signal(barrier, inc=1, device_id=friend, device_id_type=MESH)
    exchange = Exchange(at, table, SETS[0], 0, boxes, send_sem, recv_sem)
    solver = Solver(plan, tiles_hl, x, u, r, p, p_hl, image_hl, back, z_before)
    loads[0].wait()
    loads[1].wait()
    for part in exchange.parts:
        launch = exchange.start(part, x, u)
        if part == 0:
            pl.semaphore_wait(barrier, len(friends))
        launch()
    loads[2].wait()

    def split_tile(t, _):
        split_store(tiles_hl, t, tiles[t])
        return (_,)

    loop(tiles.shape[0], 2, split_tile, 0)
    back[back.shape[0] - 1] = solver.zero
    loads[3].wait()
    solver.load_x()
    exchange.pass_on()
    solver.forward(observed=observed)
    solver.backward()

    def rest():
        exchange.reduce_first()
        exchange.reduce_second()
        exchange.reduce_third()
        exchange.agree(z_own)
        exchange.spread_first()
        exchange.spread_second()
        exchange.give_back()
        exchange.give_on()
        exchange.finish()

    rest()
    solver.begin(True, exchange.read)
    for number in range(CG_STEPS):
        solver.step(number == CG_STEPS - 1)
    for part in exchange.parts:
        exchange.start(part, x, u)()
    exchange.pass_on()
    rest()
    gap = solver.begin(False, exchange.read)

    gap_moves = []

    def gap_copy(n, device):
        return pltpu.make_async_remote_copy(
            src_ref=gap_box.at[10 + n // 3], dst_ref=gap_box.at[n], send_sem=gap_send.at[n],
            recv_sem=gap_recv.at[n], device_id=device, device_id_type=MESH)

    def gap_stage(stage, value):
        gap_box[10 + stage] = value
        peers = [at.near("xyz"[stage], delta) for delta in (1, 2, 3)] if stage < 3 else [at.partner]
        for n, peer in enumerate(peers):
            moving = gap_copy(3 * stage + n, peer)
            moving.start()
            gap_moves.append(moving)

    def gap_sum(stage):
        value = gap_box[10 + stage]
        for n in range(3 if stage < 3 else 1):
            gap_copy(3 * stage + n, at.partner).wait_recv()
            value = value + gap_box[3 * stage + n]
        return value

    gap_stage(0, gap)
    for number in range(CG_STEPS - 1):
        solver.step(False)
        gap_stage(number + 1, gap_sum(number))
    solver.end()
    gap_out[...] = gap_sum(3)
    for moving in gap_moves:
        moving.wait_send()


def fused(plan, table, tiles, observed, x, u):
    slots, targets, blk = x.shape
    count = tiles.shape[0]
    each = lambda shape: [pltpu.VMEM(shape(t * SUB), F32) for t in SETS[0]]
    scratch = (
        each(lambda r: (8, 16 * r + 16, blk)) + each(lambda r: (8, 16 * r + 16, blk))
        + each(lambda r: (2, 16 * r + 16, blk)) + each(lambda r: (SIDE, SIDE * (PER * r + SUB), blk))
        + each(lambda r: (SIDE * (PER * r + SUB), blk)) + each(lambda r: (2, SIDE * (PER * r + SUB), blk))
        + each(lambda r: (SIDE, PER * r + SUB, blk)) + each(lambda r: (3, PER * r + SUB, blk))
        + each(lambda r: (SIDE, SIDE, PER * r, blk)) + each(lambda r: (128, r, blk))
        + each(lambda r: (128, r, blk)) + each(lambda r: (32, r, blk))
        + [
            pltpu.VMEM(tiles.shape, F32), pltpu.VMEM(observed.shape, F32),
            pltpu.VMEM((count, 2 * blk, blk), BF16), pltpu.VMEM(x.shape, F32), pltpu.VMEM(x.shape, F32),
            pltpu.VMEM((slots, 2 * targets, blk), BF16), pltpu.VMEM((count, 2 * targets, blk), BF16),
            pltpu.VMEM((count + 1, targets, blk), F32), pltpu.VMEM(x.shape, F32),
            pltpu.VMEM((14, targets, blk), F32),
            pltpu.SemaphoreType.DMA((4,)), pltpu.SemaphoreType.DMA((10,)), pltpu.SemaphoreType.DMA((10,)),
            pltpu.SemaphoreType.DMA((len(ORDERS), SEMS)), pltpu.SemaphoreType.DMA((len(ORDERS), SEMS)),
        ]
    )
    whole = pl.BlockSpec(memory_space=pltpu.VMEM)
    scalars = pl.BlockSpec(memory_space=pltpu.SMEM)
    like = jax.ShapeDtypeStruct(x.shape, F32)
    return pl.pallas_call(
        fused_kernel,
        out_shape=(like, like, jax.ShapeDtypeStruct((PER, targets, blk), F32),
                   jax.ShapeDtypeStruct((targets, blk), F32)),
        in_specs=[scalars, scalars] + [pl.BlockSpec(memory_space=pl.ANY)] * 4,
        out_specs=(whole,) * 4,
        scratch_shapes=scratch,
        compiler_params=pltpu.CompilerParams(
            collective_id=0, has_side_effects=True, vmem_limit_bytes=67043328),
        name="consensus",
    )(plan, table, tiles, observed, x, u)


def on_device(tile_data, tile_row, tile_col, tile_count, touched, owner_map, observed, start_x, start_u):
    shards = lax.axis_size(AXES)
    local_cols = touched.shape[1]
    col_blocks = owner_map.shape[0]
    col_dev = col_blocks // shards
    plan = tile_plan(tile_row[0], tile_col[0], tile_count[0])
    wanted = touched[0]
    matches = (wanted[:, None] == jnp.arange(col_blocks, dtype=jnp.int32)[None, :]).astype(jnp.int32)
    position = jnp.sum(matches * owner_map[None, :], axis=1)
    owner = position // col_dev
    table = exchange_plan(owner, position - owner * col_dev, shards)
    flip = lambda a: jnp.swapaxes(a, 1, 2)
    x, u, z, gap = fused(plan, table, tile_data, flip(observed), flip(start_x), flip(start_u))
    primal_gap = jnp.sqrt(jnp.sum(gap, axis=1) / (shards * local_cols * start_x.shape[1]))
    return flip(x), flip(u), flip(z), primal_gap


def solution(mesh):
    split = P(AXES)
    return jax.shard_map(
        on_device, mesh=mesh,
        in_specs=(split, split, split, split, split, P(), split, split, split),
        out_specs=(split, split, split, P()),
        check_vma=False,
    )
```

```python
import functools

import jax
import jax.numpy as jnp
from jax import lax
from jax.experimental import pallas as pl
from jax.experimental.pallas import tpu as pltpu
from jax.sharding import PartitionSpec as P

ITERS = 2
CG_STEPS = 4
GROUP = 32
AXES = ("dev", "ka")
F32 = jnp.float32
BF16 = jnp.bfloat16
MESH = pl.DeviceIdType.MESH

SIDE = 4
SUB = 8
PER = 4
ORDERS = (("x", "y", "z"), ("y", "z", "x"), ("z", "x", "y"))
SETS = ((3, 3, 2),)
S1, S1F, S2F, S2S, S2D, S3, T3, T2O, T2F, T2D, T1, T1F, SEMS = 0, 8, 9, 13, 17, 21, 25, 29, 33, 37, 41, 49, 50
THERE, BACK = (2, 1, 3, 0), (0, 1, 3, 2)
BOXES = 13


def fold(values):
    return functools.reduce(lambda s, n: s + n, values)


def split_tile(ref, index, value):
    rows = value.shape[0]
    high = value.astype(BF16)
    low = (value - high.astype(F32)).astype(BF16)
    ref[index, :rows, :] = high
    ref[index, rows:, :] = low


def split_store(ref, index, value):
    for n in range(0, value.shape[0], SUB):
        part = value[n:n + SUB]
        high = part.astype(BF16).astype(F32)
        ref[index, 2 * n:2 * n + 2 * SUB, :] = jnp.concatenate([high, part - high], axis=0).astype(BF16)


def join(wide, rows, cols):
    pieces = []
    for n in range(0, 2 * rows, 2 * SUB):
        high, low = wide[n:n + SUB], wide[n + SUB:n + 2 * SUB]
        pieces.append((high[:, :cols] + high[:, cols:]) + low[:, :cols])
    return jnp.concatenate(pieces, axis=0)


def total_of(value):
    return jnp.sum(value, axis=1, keepdims=True)


def tile_plan(rows, cols, count):
    tiles = rows.shape[0]
    place = jnp.arange(tiles, dtype=jnp.int32)
    used = place < count

    def order(key):
        code = jnp.where(used, key, tiles) * tiles + place
        rank = jnp.sum((code[None, :] < code[:, None]).astype(jnp.int32), axis=1)
        pick = rank[None, :] == place[:, None]
        return rank, pick

    def take(pick, values):
        return jnp.sum(jnp.where(pick, values[None, :], 0), axis=1)

    row_key = jnp.where(used, rows, tiles)
    col_key = jnp.where(used, cols, tiles)
    rank_f, pick_f = order(rows)
    rank_b, pick_b = order(cols)
    row_sorted = take(pick_f, row_key)
    col_sorted = take(pick_b, col_key)
    before = lambda s: jnp.concatenate([jnp.full((1,), -1, jnp.int32), s[:-1]])
    after = lambda s: jnp.concatenate([s[1:], jnp.full((1,), -1, jnp.int32)])
    keep_f = (row_sorted == before(row_sorted)).astype(jnp.int32)
    keep_b = (col_sorted == before(col_sorted)).astype(jnp.int32)
    ends_f = ((row_sorted != after(row_sorted)) & (row_sorted < tiles)).astype(jnp.int32)
    last_of_row = jnp.max(jnp.where(row_key[:, None] == row_key[None, :], rank_f[None, :], 0), axis=1)
    column = jnp.arange(tiles, dtype=jnp.int32)
    last_of_col = jnp.max(jnp.where(col_key[None, :] == column[:, None], rank_b[None, :] + 1, 0), axis=1)
    last_of_col = jnp.where(last_of_col == 0, tiles, last_of_col - 1)
    return jnp.stack([
        take(pick_f, place), take(pick_f, cols), keep_f, ends_f, jnp.minimum(row_sorted, 31),
        take(pick_b, place), take(pick_b, last_of_row), keep_b, last_of_col,
    ])

def exchange_plan(owner, slot_tag, shards):
    y, x, core, z = owner // 32, (owner // 8) % 4, (owner // 4) % 2, owner % 4
    place = {"x": x, "y": y, "z": z}
    index = jnp.stack([place[a] * 32 + core * 16 + place[b] * 4 + place[c] for a, b, c in ORDERS])
    match = index[:, :, None] == jnp.arange(shards, dtype=jnp.int32)[None, None, :]
    number = jnp.arange(owner.shape[0], dtype=jnp.int32)
    slot = jnp.sum(jnp.where(match, number[None, :, None], 0), axis=1)
    tag = jnp.sum(jnp.where(match, slot_tag[None, :, None] + 1, 0), axis=1) - 1
    index = jnp.pad(index, ((0, 0), (0, shards - owner.shape[0])))
    return jnp.concatenate([slot, tag, index])


def loop(count, step, body, *init):
    def group(g, carry):
        for n in range(step):
            carry = body(g * step + n, *carry)
        return carry

    return lax.fori_loop(0, count // step, group, init)


def near_device(me, axis, delta, to_core):
    at = dict(me)
    at[axis] = lax.rem(me[axis] + delta + SIDE, SIDE)
    return ((at["y"] * SIDE + at["x"]) * 2 + to_core, at["z"])


class Place:
    def __init__(self):
        dev, z = lax.axis_index("dev"), lax.axis_index("ka")
        self.core = lax.rem(dev, 2)
        self.me = {"x": lax.rem(dev // 2, SIDE), "y": dev // 8, "z": z}
        self.way = 1 - 2 * self.core
        self.partner = (dev + 1 - 2 * self.core, z)

    def near(self, axis, delta, to_core=None):
        return near_device(self.me, axis, delta, self.core if to_core is None else to_core)

    def ring(self, axis, delta):
        return lax.rem(self.me[axis] + delta + SIDE, SIDE)


class Exchange:
    def __init__(self, at, table, tiles, base, boxes, send_sem, recv_sem):
        self.at, self.table, self.tiles = at, table, tiles
        self.base = [(base + sum(tiles[:p])) * SUB for p in range(len(tiles))]
        (self.mail, self.in1, self.fwd1, self.part2, self.fwd2, self.in2, self.part3, self.in3,
         self.zb2, self.inbox, self.sel, self.zrel, self.share) = boxes
        self.first = True
        self.send_sem, self.recv_sem = send_sem, recv_sem
        self.sends = []
        self.parts = range(len(tiles))

    def copy(self, p, src, dst, send, recv, device):
        return pltpu.make_async_remote_copy(
            src_ref=src, dst_ref=dst, send_sem=self.send_sem.at[p, send], recv_sem=self.recv_sem.at[p, recv],
            device_id=device, device_id_type=MESH)

    def go(self, p, src, dst, send, recv, device):
        moving = self.copy(p, src, dst, send, recv, device)
        moving.start()
        self.sends.append(moving)

    def arrive(self, p, dst, recv):
        self.copy(p, dst, dst, 0, recv, self.at.partner).wait_recv()

    def sent(self):
        for moving in self.sends:
            moving.wait_send()
        self.sends = []

    def pack(self, p, x, u):
        rows = self.tiles[p] * SUB
        where = pl.ds(self.base[p], rows)
        table, parts, mail = self.table, len(ORDERS), self.mail[p]

        def record(q, _):
            for i in range(16):
                slot = table[p, q * 16 + i]
                mail[q, i * rows:(i + 1) * rows, :] = x[slot, where, :] + u[slot, where, :]
                if self.first:
                    tag = table[parts + p, q * 16 + i]
                    mail[q, 16 * rows + i:16 * rows + i + 1, :] = jnp.full((1, x.shape[2]), tag, jnp.int32).astype(F32)
            return (_,)

        loop(8, 1, record, 0)

    def sent_rows(self, p, count, extra):
        return pl.ds(0, count * self.tiles[p] * SUB + (extra if self.first else 0))

    def scatter(self, p, box, into, relay, base, base_f):
        at, a, core = self.at, ORDERS[p][0], self.at.core
        self.go(p, box(at.ring(a, 2), None), relay, base_f, base_f, at.near(a, at.way))
        for delta in (1, 3):
            for c in (0, 1):
                self.go(p, box(at.ring(a, delta), c), into(delta), base + delta * 2 + c,
                        base + delta * 2 + core, at.near(a, delta, c))
        self.go(p, box(at.me[a], 1 - core), into(0), base, base + core, at.partner)

    def relay(self, p, relay, into, base, base_f):
        at, a = self.at, ORDERS[p][0]
        self.arrive(p, relay(None), base_f)
        for c in (0, 1):
            self.go(p, relay(c), into, base + 4 + c, base + 4 + at.core, at.near(a, at.way, c))

    def start(self, p, x, u):
        self.pack(p, x, u)

        rows = self.sent_rows(p, 16, 16)

        def box(place, c):
            return self.mail[p].at[pl.ds(place * 2, 2) if c is None else place * 2 + c, rows]

        return lambda: self.scatter(
            p, box, lambda delta: self.in1[p].at[delta * 2 + self.at.core, rows], self.fwd1[p].at[:, rows], S1, S1F)

    def pass_on(self):
        for p in self.parts:
            fwd, rows = self.fwd1[p], self.sent_rows(p, 16, 16)
            self.relay(p, lambda c: fwd.at[:, rows] if c is None else fwd.at[c, rows],
                       self.in1[p].at[4 + self.at.core, rows], S1, S1F)

    def sources(self, p):
        at, a = self.at, ORDERS[p][0]
        mail, in1 = self.mail[p], self.in1[p]
        found = [(0, at.core, lambda rows: mail[at.me[a] * 2 + at.core, rows, :])]
        for delta, c in ((0, 1 - at.core), (1, 0), (1, 1), (2, 0), (2, 1), (3, 0), (3, 1)):
            found.append((delta, c, lambda rows, n=delta * 2 + c: in1[n, rows, :]))
        return found

    def others(self):
        return ((1, 0), (1, 1), (3, 0), (3, 1), (0, 1 - self.at.core), (2, 0), (2, 1))

    def combine(self, p):
        tiles = self.tiles[p]
        rows = tiles * SUB
        found = self.sources(p)
        part2 = self.part2[p]
        blk = part2.shape[3]

        def some(a2, _):
            for a3 in range(SIDE):
                i = a2 * SIDE + a3
                tags = [jnp.broadcast_to(read(pl.ds(16 * rows + i, 1)), (SUB, blk)) for _, _, read in found]
                hits = [[tag == float(k) for tag in tags] for k in range(PER)]
                for j in range(tiles):
                    place = pl.multiple_of(i * rows + j * SUB, SUB)
                    data = [read(pl.ds(place, SUB)) for _, _, read in found]
                    for k in range(PER):
                        start = k * rows + j * SUB
                        part2[a2, a3, start:start + SUB, :] = fold(
                            [jnp.where(h, v, 0.0) for h, v in zip(hits[k], data)])
                if self.first:
                    counts = [fold([jnp.where(h, 1.0, 0.0) for h in hits[k]])[:1] for k in range(PER)]
                    counts.append(jnp.zeros((SUB - PER, blk), F32))
                    part2[a2, a3, PER * rows:PER * rows + SUB, :] = jnp.concatenate(counts, axis=0)
            return (_,)

        loop(SIDE, 1, some, 0)

    def reduce_first(self):
        at = self.at
        for p in self.parts:
            b, d = ORDERS[p][1], ORDERS[p][2]
            every = self.sent_rows(p, 16, 16)
            rows = self.sent_rows(p, PER, SUB)
            for delta, c in self.others():
                self.arrive(p, self.in1[p].at[delta * 2 + c, every], S1 + delta * 2 + c)
            self.combine(p)
            for n, delta in enumerate(THERE):
                piece = at.ring(d, delta)
                self.go(p, self.part2[p].at[at.ring(b, 2), piece, rows], self.fwd2[p].at[piece, rows],
                        S2F + n, S2F + n, at.near(b, at.way))
            for n, delta in enumerate(THERE):
                piece = at.ring(d, delta)
                self.go(p, self.part2[p].at[at.ring(b, -at.way), piece, rows], self.in2[p].at[1, piece, rows],
                        S2D + n, S2D + n, at.near(b, -at.way))

    def reduce_second(self):
        at = self.at
        for n, delta in enumerate(THERE):
            for p in self.parts:
                b, piece = ORDERS[p][1], at.ring(ORDERS[p][2], delta)
                rows = self.sent_rows(p, PER, SUB)
                self.arrive(p, self.fwd2[p].at[piece, rows], S2F + n)
                to = at.ring(b, at.way)
                self.part2[p][to, piece, rows, :] = self.part2[p][to, piece, rows, :] + self.fwd2[p][piece, rows, :]
                self.go(p, self.part2[p].at[to, piece, rows], self.in2[p].at[0, piece, rows],
                        S2S + n, S2S + n, at.near(b, at.way))

    def reduce_third(self):
        at = self.at
        for n, delta in enumerate(THERE):
            for p in self.parts:
                b, d = ORDERS[p][1], ORDERS[p][2]
                piece = at.ring(d, delta)
                rows = self.sent_rows(p, PER, SUB)
                self.arrive(p, self.in2[p].at[1, piece, rows], S2D + n)
                self.arrive(p, self.in2[p].at[0, piece, rows], S2S + n)
                self.part3[p][piece, rows, :] = (
                    self.part2[p][at.me[b], piece, rows, :] + self.in2[p][0, piece, rows, :]
                    + self.in2[p][1, piece, rows, :])
                if delta:
                    self.go(p, self.part3[p].at[piece, rows], self.in3[p].at[delta - 1, rows],
                            S3 + delta, S3 + delta, at.near(d, delta))

    def agree(self, z_own):
        at = self.at
        for p in self.parts:
            b, d = ORDERS[p][1], ORDERS[p][2]
            rows, base = self.tiles[p] * SUB, self.base[p]
            every = self.sent_rows(p, PER, SUB)
            for delta in (1, 3, 2):
                self.arrive(p, self.in3[p].at[delta - 1, every], S3 + delta)
            whole = fold([self.part3[p][at.me[d], every, :]] + [self.in3[p][n, every, :] for n in range(3)])
            if self.first:
                self.share[p][...] = jnp.maximum(whole[PER * rows:], 1.0)
            for k in range(PER):
                share = self.share[p][k:k + 1, :]
                value = whole[k * rows:(k + 1) * rows] / share
                cut = jnp.broadcast_to(1.0 / share, value.shape)
                value = value - jnp.minimum(jnp.maximum(value, -cut), cut)
                z_own[k, base:base + rows, :] = value
                self.zb2[p][at.me[b], at.me[d], k * rows:(k + 1) * rows, :] = value
            own = self.zb2[p].at[at.me[b], at.me[d]]
            for delta in (2, 1, 3):
                self.go(p, own, own, T3 + delta, T3 + delta, at.near(d, delta))
            self.spread(p, 0)

    def spread(self, p, n):
        at, b = self.at, ORDERS[p][1]
        own = self.zb2[p].at[at.me[b], at.ring(ORDERS[p][2], -BACK[n])]
        if n:
            self.arrive(p, own, T3 + BACK[n])
        self.go(p, own, own, T2O + n, T2O + n, at.near(b, at.way))
        self.go(p, own, own, T2D + n, T2D + n, at.near(b, -at.way))

    def spread_on(self, p, n):
        at, b = self.at, ORDERS[p][1]
        passing = self.zb2[p].at[at.ring(b, -at.way), at.ring(ORDERS[p][2], -BACK[n])]
        self.arrive(p, passing, T2O + n)
        self.go(p, passing, passing, T2F + n, T2F + n, at.near(b, at.way))

    def spread_all(self):
        for act, n in ((self.spread, 1), (self.spread, 2), (self.spread_on, 0), (self.spread, 3),
                       (self.spread_on, 1), (self.spread_on, 2), (self.spread_on, 3)):
            for p in self.parts:
                act(p, n)

    def select(self, p):
        at = self.at
        tiles = self.tiles[p]
        rows = tiles * SUB
        a = ORDERS[p][0]
        found = self.sources(p)
        zb2, inbox, sel = self.zb2[p], self.inbox[p], self.sel[p]

        def some(a2, _):
            for a3 in range(SIDE):
                i = a2 * SIDE + a3
                blocks = [zb2[a2, a3, n * SUB:(n + 1) * SUB, :] for n in range(PER * tiles)]
                for number, (delta, c, read) in enumerate(found):
                    tag = jnp.broadcast_to(read(pl.ds(16 * rows + i, 1)), blocks[0].shape)
                    hit = [tag == float(k) for k in range(PER - 1)]
                    for j in range(tiles):
                        value = blocks[(PER - 1) * tiles + j]
                        for k in range(PER - 1):
                            value = jnp.where(hit[k], blocks[k * tiles + j], value)
                        place = (at.ring(a, -delta) * 2 + c) * 16 + i
                        (sel if number else inbox)[place, j * SUB:(j + 1) * SUB, :] = value
            return (_,)

        loop(SIDE, 1, some, 0)

    def give_back(self):
        at = self.at
        self.sent()
        for p in self.parts:
            a, b = ORDERS[p][0], ORDERS[p][1]
            for n, delta in enumerate(BACK):
                piece = at.ring(ORDERS[p][2], -delta)
                self.arrive(p, self.zb2[p].at[at.ring(b, at.way), piece], T2D + n)
                self.arrive(p, self.zb2[p].at[at.ring(b, 2), piece], T2F + n)
            self.select(p)
            sel = self.sel[p]

            def box(place, c):
                return sel.at[pl.ds(place * 32, 32)] if c is None else sel.at[pl.ds((place * 2 + c) * 16, 16)]

            mine = self.inbox[p].at[pl.ds((at.me[a] * 2 + at.core) * 16, 16)]
            self.scatter(p, box, lambda delta: mine, self.zrel[p], T1, T1F)

    def give_on(self):
        at = self.at
        for p in self.parts:
            zrel, a = self.zrel[p], ORDERS[p][0]
            self.relay(p, lambda c: zrel if c is None else zrel.at[pl.ds(c * 16, 16)],
                       self.inbox[p].at[pl.ds((at.ring(a, -at.way) * 2 + at.core) * 16, 16)], T1, T1F)

    def finish(self):
        at = self.at
        for p in self.parts:
            a = ORDERS[p][0]
            for delta, c in self.others():
                self.arrive(p, self.inbox[p].at[pl.ds((at.ring(a, -delta) * 2 + c) * 16, 16)], T1 + delta * 2 + c)
        self.sent()

    def read(self, c):
        found = [self.inbox[p][self.table[2 * len(ORDERS) + p, c]] for p in self.parts]
        return jnp.concatenate(found, axis=0)


class Solver:
    def __init__(self, plan, tiles_hl, x, u, r, p, p_hl, image_hl, back, z_before):
        self.plan, self.tiles_hl = plan, tiles_hl
        self.x, self.u, self.r, self.p = x, u, r, p
        self.p_hl, self.image_hl, self.back, self.z_before = p_hl, image_hl, back, z_before
        self.slots, self.blk = p_hl.shape[0], p_hl.shape[2]
        self.targets = p_hl.shape[1] // 2
        self.zero = jnp.zeros((self.targets, self.blk), F32)

    def forward(self, observed=None):
        plan, targets, blk = self.plan, self.targets, self.blk

        def tile_step(k, acc, total):
            wide = lax.dot_general(
                self.p_hl[plan[1, k]], self.tiles_hl[plan[0, k]], (((1,), (1,)), ((), ())),
                preferred_element_type=F32)
            acc = jnp.where(plan[2, k] > 0, acc, 0.0) + join(wide, targets, blk)
            if observed is not None:
                split_store(self.image_hl, k, observed[plan[4, k]] - acc)
            else:
                split_store(self.image_hl, k, acc)
                total = total + jnp.where(plan[3, k] > 0, acc * acc, 0.0)
            return acc, total

        return loop(self.slots, GROUP, tile_step, self.zero, self.zero)[1]

    def backward(self):
        plan, targets, blk = self.plan, self.targets, self.blk

        def tile_step(k, acc):
            both = self.tiles_hl[plan[5, k]]
            weights = jnp.concatenate([both[:blk], both[blk:]], axis=1)
            wide = jnp.dot(self.image_hl[plan[6, k]], weights, preferred_element_type=F32)
            acc = jnp.where(plan[7, k] > 0, acc, 0.0) + join(wide, targets, blk)
            self.back[k] = acc
            return (acc,)

        loop(self.slots, GROUP, tile_step, self.zero)

    def load_x(self):
        def one(c, _):
            split_store(self.p_hl, c, self.x[c])
            return (_,)

        loop(self.slots, 4, one, 0)

    def begin(self, first, z_of):
        def one(c, rr, gap):
            z, x, u = z_of(c), self.x[c], self.u[c]
            diff = x - z
            u_new = u + diff
            self.u[c] = u_new
            if first:
                r = self.back[self.plan[8, c]] + (z - u_new) - x
                self.z_before[c] = z
            else:
                r = self.r[c] + ((z - u_new) - (self.z_before[c] - u))
            self.r[c] = r
            self.p[c] = r
            split_store(self.p_hl, c, r)
            return rr + r * r, gap + diff * diff

        rr, gap = loop(self.slots, 4, one, self.zero, self.zero)
        self.own = rr
        self.rr = total_of(rr)
        return gap

    def length(self):
        self.a = self.rr / total_of(self.forward() + self.own)

    def move_x(self):
        p, x, a = self.p, self.x, self.a

        def move(c, _):
            x[c] = x[c] + a * p[c]
            return (_,)

        loop(self.slots, 4, move, 0)

    def move_r(self):
        p, r, back, plan, a = self.p, self.r, self.back, self.plan, self.a
        self.backward()

        def move(c, nn):
            new = r[c] - a * (back[plan[8, c]] + p[c])
            r[c] = new
            return (nn + new * new,)

        return loop(self.slots, 4, move, self.zero)[0]

    def step(self):
        p, r, x = self.p, self.r, self.x
        self.length()
        a = self.a
        nn = total_of(self.move_r())
        ratio = nn / self.rr

        def turn(c, own):
            value = p[c]
            x[c] = x[c] + a * value
            value = r[c] + ratio * value
            p[c] = value
            split_store(self.p_hl, c, value)
            return (own + value * value,)

        self.own = loop(self.slots, 4, turn, self.zero)[0]
        self.rr = nn


def fused_kernel(plan, table, tiles_in, observed_in, x_in, u_in, x, u, z_own, gap_out, *scratch):
    (tiles, observed, tiles_hl, r, p, p_hl, image_hl, back, z_before, gap_box, local_sem, gap_send, gap_recv,
     send_sem, recv_sem) = scratch[BOXES * len(ORDERS):]
    boxes = [scratch[n * len(ORDERS):(n + 1) * len(ORDERS)] for n in range(BOXES)]
    loads = [pltpu.make_async_copy(src, dst, local_sem.at[n]) for n, (src, dst) in enumerate(
        ((x_in, x), (u_in, u), (tiles_in, tiles), (observed_in, observed)))]
    for load in loads:
        load.start()
    at = Place()
    barrier = pltpu.get_barrier_semaphore()
    friends = [at.partner]
    for axis in ("x", "y", "z"):
        friends += [at.near(axis, 2)] + [at.near(axis, delta, c) for delta in (1, -1) for c in (0, 1)]
    for friend in friends:
        pl.semaphore_signal(barrier, inc=1, device_id=friend, device_id_type=MESH)
    exchange = Exchange(at, table, SETS[0], 0, boxes, send_sem, recv_sem)
    solver = Solver(plan, tiles_hl, x, u, r, p, p_hl, image_hl, back, z_before)
    loads[0].wait()
    loads[1].wait()
    for part in exchange.parts:
        launch = exchange.start(part, x, u)
        if part == 0:
            pl.semaphore_wait(barrier, len(friends))
        launch()
    loads[2].wait()

    def one_tile(t, _):
        split_tile(tiles_hl, t, tiles[t])
        return (_,)

    loop(tiles.shape[0], 2, one_tile, 0)
    back[back.shape[0] - 1] = solver.zero
    loads[3].wait()
    solver.load_x()
    exchange.pass_on()
    solver.forward(observed=observed)
    solver.backward()

    def rest():
        exchange.reduce_first()
        exchange.reduce_second()
        exchange.reduce_third()
        exchange.agree(z_own)
        exchange.spread_all()
        exchange.give_back()
        exchange.give_on()
        exchange.finish()

    rest()
    solver.begin(True, exchange.read)
    for number in range(CG_STEPS - 1):
        solver.step()
    solver.length()
    solver.move_x()
    exchange.first = False
    for part in exchange.parts:
        exchange.start(part, x, u)()
    solver.move_r()
    exchange.pass_on()
    rest()
    gap = solver.begin(False, exchange.read)

    gap_moves = []

    def gap_copy(n, device):
        return pltpu.make_async_remote_copy(
            src_ref=gap_box.at[10 + n // 3], dst_ref=gap_box.at[n], send_sem=gap_send.at[n],
            recv_sem=gap_recv.at[n], device_id=device, device_id_type=MESH)

    def gap_stage(stage, value):
        gap_box[10 + stage] = value
        peers = [at.near("xyz"[stage], delta) for delta in (1, 2, 3)] if stage < 3 else [at.partner]
        for n, peer in enumerate(peers):
            moving = gap_copy(3 * stage + n, peer)
            moving.start()
            gap_moves.append(moving)

    def gap_sum(stage):
        value = gap_box[10 + stage]
        for n in range(3 if stage < 3 else 1):
            gap_copy(3 * stage + n, at.partner).wait_recv()
            value = value + gap_box[3 * stage + n]
        return value

    gap_stage(0, gap)
    for number in range(CG_STEPS - 1):
        solver.step()
        gap_stage(number + 1, gap_sum(number))
    solver.length()
    solver.move_x()
    gap_out[...] = gap_sum(3)
    for moving in gap_moves:
        moving.wait_send()


def fused(plan, table, tiles, observed, x, u):
    slots, targets, blk = x.shape
    count = tiles.shape[0]
    each = lambda shape: [pltpu.VMEM(shape(t * SUB), F32) for t in SETS[0]]
    scratch = (
        each(lambda r: (8, 16 * r + 16, blk)) + each(lambda r: (8, 16 * r + 16, blk))
        + each(lambda r: (2, 16 * r + 16, blk)) + each(lambda r: (SIDE, SIDE, PER * r + SUB, blk))
        + each(lambda r: (SIDE, PER * r + SUB, blk)) + each(lambda r: (2, SIDE, PER * r + SUB, blk))
        + each(lambda r: (SIDE, PER * r + SUB, blk)) + each(lambda r: (3, PER * r + SUB, blk))
        + each(lambda r: (SIDE, SIDE, PER * r, blk)) + each(lambda r: (128, r, blk))
        + each(lambda r: (128, r, blk)) + each(lambda r: (32, r, blk)) + each(lambda r: (SUB, blk))
        + [
            pltpu.VMEM(tiles.shape, F32), pltpu.VMEM(observed.shape, F32),
            pltpu.VMEM((count, 2 * blk, blk), BF16), pltpu.VMEM(x.shape, F32), pltpu.VMEM(x.shape, F32),
            pltpu.VMEM((slots, 2 * targets, blk), BF16), pltpu.VMEM((count, 2 * targets, blk), BF16),
            pltpu.VMEM((count + 1, targets, blk), F32), pltpu.VMEM(x.shape, F32),
            pltpu.VMEM((14, targets, blk), F32),
            pltpu.SemaphoreType.DMA((4,)), pltpu.SemaphoreType.DMA((10,)), pltpu.SemaphoreType.DMA((10,)),
            pltpu.SemaphoreType.DMA((len(ORDERS), SEMS)), pltpu.SemaphoreType.DMA((len(ORDERS), SEMS)),
        ]
    )
    whole = pl.BlockSpec(memory_space=pltpu.VMEM)
    scalars = pl.BlockSpec(memory_space=pltpu.SMEM)
    like = jax.ShapeDtypeStruct(x.shape, F32)
    return pl.pallas_call(
        fused_kernel,
        out_shape=(like, like, jax.ShapeDtypeStruct((PER, targets, blk), F32),
                   jax.ShapeDtypeStruct((targets, blk), F32)),
        in_specs=[scalars, scalars] + [pl.BlockSpec(memory_space=pl.ANY)] * 4,
        out_specs=(whole,) * 4,
        scratch_shapes=scratch,
        compiler_params=pltpu.CompilerParams(
            collective_id=0, has_side_effects=True, vmem_limit_bytes=67043328),
        name="consensus",
    )(plan, table, tiles, observed, x, u)


def on_device(tile_data, tile_row, tile_col, tile_count, touched, owner_map, observed, start_x, start_u):
    shards = lax.axis_size(AXES)
    local_cols = touched.shape[1]
    col_blocks = owner_map.shape[0]
    col_dev = col_blocks // shards
    plan = tile_plan(tile_row[0], tile_col[0], tile_count[0])
    wanted = touched[0]
    matches = (wanted[:, None] == jnp.arange(col_blocks, dtype=jnp.int32)[None, :]).astype(jnp.int32)
    position = jnp.sum(matches * owner_map[None, :], axis=1)
    owner = position // col_dev
    table = exchange_plan(owner, position - owner * col_dev, shards)
    flip = lambda a: jnp.swapaxes(a, 1, 2)
    x, u, z, gap = fused(plan, table, tile_data, flip(observed), flip(start_x), flip(start_u))
    primal_gap = jnp.sqrt(jnp.sum(gap, axis=1) / (shards * local_cols * start_x.shape[1]))
    return flip(x), flip(u), flip(z), primal_gap


def solution(mesh):
    split = P(AXES)
    return jax.shard_map(
        on_device, mesh=mesh,
        in_specs=(split, split, split, split, split, P(), split, split, split),
        out_specs=(split, split, split, P()),
        check_vma=False,
    )
```

```python
import functools

import jax
import jax.numpy as jnp
from jax import lax
from jax.experimental import pallas as pl
from jax.experimental.pallas import tpu as pltpu
from jax.sharding import PartitionSpec as P

ITERS = 2
CG_STEPS = 4
GROUP = 32
AXES = ("dev", "ka")
F32 = jnp.float32
BF16 = jnp.bfloat16
MESH = pl.DeviceIdType.MESH

SIDE = 4
SUB = 8
PER = 4
ORDERS = (("x", "y", "z"), ("y", "z", "x"), ("z", "x", "y"))
ROWS = (22, 22, 20)
DEEP = 24
S1, S1F, S2F, S2S, S2D, S3, T3, T2O, T2F, T2D, T1, T1F, SEMS = 0, 8, 9, 13, 17, 21, 25, 29, 33, 37, 41, 49, 50
THERE, BACK = (2, 1, 3, 0), (0, 1, 3, 2)
BOXES = 13


def fold(values):
    return functools.reduce(lambda s, n: s + n, values)


def split_tile(ref, index, value):
    rows = value.shape[0]
    high = value.astype(BF16)
    low = (value - high.astype(F32)).astype(BF16)
    ref[index, :rows, :] = high
    ref[index, rows:, :] = low


def split_store(ref, index, value):
    for n in range(0, value.shape[0], SUB):
        part = value[n:n + SUB]
        high = part.astype(BF16).astype(F32)
        ref[index, 2 * n:2 * n + 2 * SUB, :] = jnp.concatenate([high, part - high], axis=0).astype(BF16)


def join(wide, rows, cols):
    pieces = []
    for n in range(0, 2 * rows, 2 * SUB):
        high, low = wide[n:n + SUB], wide[n + SUB:n + 2 * SUB]
        pieces.append((high[:, :cols] + high[:, cols:]) + low[:, :cols])
    return jnp.concatenate(pieces, axis=0)


def total_of(value):
    return jnp.sum(value, axis=1, keepdims=True)


def tables_kernel(rows, cols, touched, owner_map, count, out):
    tiles, lanes = rows.shape[1], out.shape[1]
    near, far = (lax.broadcasted_iota(jnp.int32, (tiles, lanes), n) for n in (0, 1))
    down = lax.broadcasted_iota(jnp.int32, (tiles, 1), 0).astype(F32)
    across = lax.broadcasted_iota(jnp.int32, (1, lanes), 1).astype(F32)
    eye = near == far
    wide = lambda v: jnp.concatenate([v[...].astype(F32), jnp.zeros((1, lanes - tiles), F32)], axis=1)
    stand = lambda v: jnp.sum(jnp.where(eye, v, 0.0), axis=1, keepdims=True)
    lie = lambda v: jnp.sum(jnp.where(eye, v, 0.0), axis=0, keepdims=True)
    ones = lambda m: jnp.where(m, 1.0, 0.0)
    left = lambda m: jnp.sum(ones(m), axis=1, keepdims=True)
    up = lambda m: jnp.sum(ones(m), axis=0, keepdims=True)
    number = count[0].astype(F32)
    inside = across < float(tiles)

    def order(values):
        key = jnp.where(across < number, wide(values), float(tiles))
        key = jnp.where(inside, key, float(tiles + 1))
        code = key * float(lanes) + across
        key_d, code_d = stand(key), stand(code)
        same = key == key_d
        rank = left(code < code_d)
        last = left(key <= key_d) - 1.0
        keep = left(same & (code < code_d))
        later = left(same & (code > code_d))
        ends = jnp.where((later == 0.0) & (key_d < float(tiles)), 1.0, 0.0)
        return key_d, rank, last, keep, ends

    def sort(rank, values):
        return jnp.sum(jnp.where(rank == across, values, 0.0), axis=0, keepdims=True)

    row_d, rank_f, last_f, keep_f, ends_f = order(rows)
    col_d, rank_b, _, keep_b, _ = order(cols)
    found = up(col_d == across)
    until = up(col_d <= across) - 1.0
    last_b = jnp.where(found > 0.0, until, float(tiles))
    plan = [
        sort(rank_f, down), sort(rank_f, stand(wide(cols))), sort(rank_f, keep_f), sort(rank_f, ends_f),
        sort(rank_f, stand(wide(rows))), sort(rank_b, down), sort(rank_b, last_f), sort(rank_b, keep_b), last_b,
    ]
    wanted = stand(wide(touched))
    blocks = owner_map.shape[1]
    every = lax.broadcasted_iota(jnp.int32, (1, blocks), 1).astype(F32)
    position = jnp.sum(jnp.where(wanted == every, owner_map[...].astype(F32), 0.0), axis=1, keepdims=True)
    position = position.astype(jnp.int32)
    owner, tag = position >> 2, (position & 3).astype(F32)
    place = {"x": (owner >> 3) & 3, "y": owner >> 5, "z": owner & 3}
    core = (owner >> 2) & 1
    slots, marks, index = [], [], []
    for a, b, c in ORDERS:
        at = (place[a] * 32 + core * 16 + place[b] * 4 + place[c]).astype(F32)
        match = at == across
        slots.append(jnp.sum(jnp.where(match, down, 0.0), axis=0, keepdims=True))
        marks.append(jnp.sum(jnp.where(match, tag + 1.0, 0.0), axis=0, keepdims=True) - 1.0)
        index.append(lie(at))
    found = slots + marks + index + plan
    for n, row in enumerate(found):
        out[n:n + 1, :] = row.astype(jnp.int32)
    out[len(found):, :] = jnp.zeros((out.shape[0] - len(found), lanes), jnp.int32)


def tables(rows, cols, touched, owner_map, count):
    whole = pl.BlockSpec(memory_space=pltpu.VMEM)
    return pl.pallas_call(
        tables_kernel,
        out_shape=jax.ShapeDtypeStruct((24, 128), jnp.int32),
        in_specs=[whole] * 4 + [pl.BlockSpec(memory_space=pltpu.SMEM)],
        out_specs=whole,
        name="tables",
    )(rows, cols, touched, owner_map.reshape(1, -1), count)


def loop(count, step, body, *init):
    def group(g, carry):
        for n in range(step):
            carry = body(g * step + n, *carry)
        return carry

    return lax.fori_loop(0, count // step, group, init)


def near_device(me, axis, delta, to_core):
    at = dict(me)
    at[axis] = lax.rem(me[axis] + delta + SIDE, SIDE)
    return ((at["y"] * SIDE + at["x"]) * 2 + to_core, at["z"])


class Place:
    def __init__(self):
        dev, z = lax.axis_index("dev"), lax.axis_index("ka")
        self.core = lax.rem(dev, 2)
        self.me = {"x": lax.rem(dev // 2, SIDE), "y": dev // 8, "z": z}
        self.way = 1 - 2 * self.core
        self.partner = (dev + 1 - 2 * self.core, z)

    def near(self, axis, delta, to_core=None):
        return near_device(self.me, axis, delta, self.core if to_core is None else to_core)

    def ring(self, axis, delta):
        return lax.rem(self.me[axis] + delta + SIDE, SIDE)


def row_number(blk):
    return lax.broadcasted_iota(jnp.int32, (SUB, blk), 0)


def part_of(p, ref, slot):
    tile = lambda n: ref[slot, n * SUB:(n + 1) * SUB, :]
    pair = [tile(2 * p), tile(2 * p + 1)]
    if p == 0:
        return pair + [tile(6)]
    if p == 1:
        return pair + [pltpu.roll(tile(7), 6, 0)]
    edge = row_number(ref.shape[2]) < 2
    return pair + [jnp.where(edge, pltpu.roll(tile(6), 2, 0), pltpu.roll(tile(7), 2, 0))]


def from_parts(found):
    row = row_number(found[0].shape[1])
    shared = pltpu.roll(found[2][2 * SUB:], 6, 0)
    six = jnp.where(row < 6, found[0][2 * SUB:], shared)
    seven = jnp.where(row < 2, shared, pltpu.roll(found[1][2 * SUB:], 2, 0))
    return jnp.concatenate([f[:2 * SUB] for f in found] + [six, seven], axis=0)


class Exchange:
    def __init__(self, at, table, boxes, send_sem, recv_sem):
        self.at, self.table = at, table
        (self.mail, self.in1, self.fwd1, self.part2, self.fwd2, self.in2, self.part3, self.in3,
         self.zb2, self.inbox, self.sel, self.zrel, self.share) = boxes
        self.first = True
        self.send_sem, self.recv_sem = send_sem, recv_sem
        self.sends = []
        self.parts = range(len(ORDERS))

    def copy(self, p, src, dst, send, recv, device):
        return pltpu.make_async_remote_copy(
            src_ref=src, dst_ref=dst, send_sem=self.send_sem.at[p, send], recv_sem=self.recv_sem.at[p, recv],
            device_id=device, device_id_type=MESH)

    def go(self, p, src, dst, send, recv, device):
        moving = self.copy(p, src, dst, send, recv, device)
        moving.start()
        self.sends.append(moving)

    def arrive(self, p, dst, recv):
        self.copy(p, dst, dst, 0, recv, self.at.partner).wait_recv()

    def sent(self):
        for moving in self.sends:
            moving.wait_send()
        self.sends = []

    def pack(self, p, x, u):
        table, parts, mail = self.table, len(ORDERS), self.mail[p]

        def record(q, _):
            for i in range(16):
                slot = table[p, q * 16 + i]
                for n, (one, two) in enumerate(zip(part_of(p, x, slot), part_of(p, u, slot))):
                    mail[q, i, n * SUB:(n + 1) * SUB, :] = one + two
                tag = table[parts + p, q * 16 + i]
                mail[q, i, ROWS[p]:ROWS[p] + 1, :] = jnp.full((1, x.shape[2]), tag, jnp.int32).astype(F32)
            return (_,)

        loop(8, 1, record, 0)

    def marked(self, p):
        return pl.ds(0, ROWS[p] + (1 if self.first else 0))

    def scatter(self, p, box, into, relay, base, base_f):
        at, a, core = self.at, ORDERS[p][0], self.at.core
        self.go(p, box(at.ring(a, 2), None), relay, base_f, base_f, at.near(a, at.way))
        for delta in (1, 3):
            for c in (0, 1):
                self.go(p, box(at.ring(a, delta), c), into(delta), base + delta * 2 + c,
                        base + delta * 2 + core, at.near(a, delta, c))
        self.go(p, box(at.me[a], 1 - core), into(0), base, base + core, at.partner)

    def relay(self, p, relay, into, base, base_f):
        at, a = self.at, ORDERS[p][0]
        self.arrive(p, relay(None), base_f)
        for c in (0, 1):
            self.go(p, relay(c), into, base + 4 + c, base + 4 + at.core, at.near(a, at.way, c))

    def start(self, p, x, u):
        self.pack(p, x, u)

        rows = self.marked(p)

        def box(place, c):
            return self.mail[p].at[pl.ds(place * 2, 2) if c is None else place * 2 + c, :, rows]

        return lambda: self.scatter(
            p, box, lambda delta: self.in1[p].at[delta * 2 + self.at.core, :, rows], self.fwd1[p].at[:, :, rows],
            S1, S1F)

    def pass_on(self):
        for p in self.parts:
            fwd, rows = self.fwd1[p], self.marked(p)
            self.relay(p, lambda c: fwd.at[:, :, rows] if c is None else fwd.at[c, :, rows],
                       self.in1[p].at[4 + self.at.core, :, rows], S1, S1F)

    def sources(self, p):
        at, a = self.at, ORDERS[p][0]
        mail, in1 = self.mail[p], self.in1[p]
        found = [(0, at.core, lambda i, rows: mail[at.me[a] * 2 + at.core, i, rows, :])]
        for delta, c in ((0, 1 - at.core), (1, 0), (1, 1), (2, 0), (2, 1), (3, 0), (3, 1)):
            found.append((delta, c, lambda i, rows, n=delta * 2 + c: in1[n, i, rows, :]))
        return found

    def others(self):
        return ((1, 0), (1, 1), (3, 0), (3, 1), (0, 1 - self.at.core), (2, 0), (2, 1))

    def combine(self, p):
        found = self.sources(p)
        part2 = self.part2[p]
        blk = part2.shape[4]
        mark = ROWS[p] - 2 * SUB

        def some(a2, _):
            for a3 in range(SIDE):
                i = a2 * SIDE + a3
                tags = [jnp.broadcast_to(read(i, pl.ds(ROWS[p], 1)), (SUB, blk)) for _, _, read in found]
                hits = [[tag == float(k) for tag in tags] for k in range(PER)]
                for j in range(DEEP // SUB):
                    data = [read(i, pl.ds(j * SUB, SUB)) for _, _, read in found]
                    for k in range(PER):
                        value = fold([jnp.where(h, v, 0.0) for h, v in zip(hits[k], data)])
                        if self.first and j == 2:
                            count = fold([jnp.where(h, 1.0, 0.0) for h in hits[k]])
                            value = jnp.where(row_number(blk) == mark, count, value)
                        part2[a2, a3, k, j * SUB:(j + 1) * SUB, :] = value
            return (_,)

        loop(SIDE, 1, some, 0)

    def reduce_first(self):
        at = self.at
        for p in self.parts:
            b, d = ORDERS[p][1], ORDERS[p][2]
            rows = self.marked(p)
            for delta, c in self.others():
                self.arrive(p, self.in1[p].at[delta * 2 + c, :, rows], S1 + delta * 2 + c)
            self.combine(p)
            for n, delta in enumerate(THERE):
                piece = at.ring(d, delta)
                self.go(p, self.part2[p].at[at.ring(b, 2), piece, :, rows], self.fwd2[p].at[piece, :, rows],
                        S2F + n, S2F + n, at.near(b, at.way))
            for n, delta in enumerate(THERE):
                piece = at.ring(d, delta)
                self.go(p, self.part2[p].at[at.ring(b, -at.way), piece, :, rows], self.in2[p].at[1, piece, :, rows],
                        S2D + n, S2D + n, at.near(b, -at.way))

    def reduce_second(self):
        at = self.at
        for n, delta in enumerate(THERE):
            for p in self.parts:
                b, piece = ORDERS[p][1], at.ring(ORDERS[p][2], delta)
                rows = self.marked(p)
                self.arrive(p, self.fwd2[p].at[piece, :, rows], S2F + n)
                to = at.ring(b, at.way)
                self.part2[p][to, piece] = self.part2[p][to, piece] + self.fwd2[p][piece]
                self.go(p, self.part2[p].at[to, piece, :, rows], self.in2[p].at[0, piece, :, rows],
                        S2S + n, S2S + n, at.near(b, at.way))

    def reduce_third(self):
        at = self.at
        for n, delta in enumerate(THERE):
            for p in self.parts:
                b, d = ORDERS[p][1], ORDERS[p][2]
                piece = at.ring(d, delta)
                rows = self.marked(p)
                self.arrive(p, self.in2[p].at[1, piece, :, rows], S2D + n)
                self.arrive(p, self.in2[p].at[0, piece, :, rows], S2S + n)
                self.part3[p][piece] = (
                    self.part2[p][at.me[b], piece] + self.in2[p][0, piece] + self.in2[p][1, piece])
                if delta:
                    self.go(p, self.part3[p].at[piece, :, rows], self.in3[p].at[delta - 1, :, rows],
                            S3 + delta, S3 + delta, at.near(d, delta))

    def agree(self):
        at = self.at
        for p in self.parts:
            b, d = ORDERS[p][1], ORDERS[p][2]
            rows = self.marked(p)
            for delta in (1, 3, 2):
                self.arrive(p, self.in3[p].at[delta - 1, :, rows], S3 + delta)
            for k in range(PER):
                value = fold([self.part3[p][at.me[d], k]] + [self.in3[p][n, k] for n in range(3)])
                if self.first:
                    self.share[p][k:k + 1, :] = jnp.maximum(value[ROWS[p]:ROWS[p] + 1], 1.0)
                share = self.share[p][k:k + 1, :]
                value = value / share
                cut = jnp.broadcast_to(1.0 / share, value.shape)
                self.zb2[p][at.me[b], at.me[d], k] = value - jnp.minimum(jnp.maximum(value, -cut), cut)
            own = self.zb2[p].at[at.me[b], at.me[d], :, pl.ds(0, ROWS[p])]
            for delta in (2, 1, 3):
                self.go(p, own, own, T3 + delta, T3 + delta, at.near(d, delta))
            self.spread(p, 0)

    def keep(self, z_own):
        at = self.at
        for k in range(PER):
            z_own[k] = from_parts([self.zb2[p][at.me[ORDERS[p][1]], at.me[ORDERS[p][2]], k] for p in self.parts])

    def spread(self, p, n):
        at, b = self.at, ORDERS[p][1]
        own = self.zb2[p].at[at.me[b], at.ring(ORDERS[p][2], -BACK[n]), :, pl.ds(0, ROWS[p])]
        if n:
            self.arrive(p, own, T3 + BACK[n])
        self.go(p, own, own, T2O + n, T2O + n, at.near(b, at.way))
        self.go(p, own, own, T2D + n, T2D + n, at.near(b, -at.way))

    def spread_on(self, p, n):
        at, b = self.at, ORDERS[p][1]
        passing = self.zb2[p].at[at.ring(b, -at.way), at.ring(ORDERS[p][2], -BACK[n]), :, pl.ds(0, ROWS[p])]
        self.arrive(p, passing, T2O + n)
        self.go(p, passing, passing, T2F + n, T2F + n, at.near(b, at.way))

    def spread_all(self):
        for act, n in ((self.spread, 1), (self.spread, 2), (self.spread_on, 0), (self.spread, 3),
                       (self.spread_on, 1), (self.spread_on, 2), (self.spread_on, 3)):
            for p in self.parts:
                act(p, n)

    def select(self, p):
        at = self.at
        a = ORDERS[p][0]
        found = self.sources(p)
        zb2, inbox, sel = self.zb2[p], self.inbox[p], self.sel[p]
        tiles = [slice(j * SUB, (j + 1) * SUB) for j in range(DEEP // SUB)]

        def some(a2, _):
            for a3 in range(SIDE):
                i = a2 * SIDE + a3
                blocks = [[zb2[a2, a3, k, rows, :] for rows in tiles] for k in range(PER)]
                for number, (delta, c, read) in enumerate(found):
                    tag = jnp.broadcast_to(read(i, pl.ds(ROWS[p], 1)), blocks[0][0].shape)
                    hit = [tag == float(k) for k in range(PER - 1)]
                    for j, rows in enumerate(tiles):
                        value = blocks[PER - 1][j]
                        for k in range(PER - 1):
                            value = jnp.where(hit[k], blocks[k][j], value)
                        place = (at.ring(a, -delta) * 2 + c) * 16 + i
                        (sel if number else inbox)[place, rows, :] = value
            return (_,)

        loop(SIDE, 1, some, 0)

    def give_back(self):
        at = self.at
        self.sent()
        for p in self.parts:
            a, b = ORDERS[p][0], ORDERS[p][1]
            rows = pl.ds(0, ROWS[p])
            for n, delta in enumerate(BACK):
                piece = at.ring(ORDERS[p][2], -delta)
                self.arrive(p, self.zb2[p].at[at.ring(b, at.way), piece, :, rows], T2D + n)
                self.arrive(p, self.zb2[p].at[at.ring(b, 2), piece, :, rows], T2F + n)
            self.select(p)
            sel = self.sel[p]

            def box(place, c):
                return sel.at[pl.ds(place * 32, 32) if c is None else pl.ds((place * 2 + c) * 16, 16), rows]

            mine = self.inbox[p].at[pl.ds((at.me[a] * 2 + at.core) * 16, 16), rows]
            self.scatter(p, box, lambda delta: mine, self.zrel[p].at[:, rows], T1, T1F)

    def give_on(self):
        at = self.at
        for p in self.parts:
            zrel, a = self.zrel[p], ORDERS[p][0]
            rows = pl.ds(0, ROWS[p])
            self.relay(p, lambda c: zrel.at[:, rows] if c is None else zrel.at[pl.ds(c * 16, 16), rows],
                       self.inbox[p].at[pl.ds((at.ring(a, -at.way) * 2 + at.core) * 16, 16), rows], T1, T1F)

    def finish(self):
        at = self.at
        for p in self.parts:
            a, rows = ORDERS[p][0], pl.ds(0, ROWS[p])
            for delta, c in self.others():
                self.arrive(p, self.inbox[p].at[pl.ds((at.ring(a, -delta) * 2 + c) * 16, 16), rows],
                            T1 + delta * 2 + c)
        self.sent()

    def read(self, c):
        return from_parts([self.inbox[p][self.table[2 * len(ORDERS) + p, c]] for p in self.parts])


class Solver:
    def __init__(self, plan, tiles_hl, x, u, r, p, p_hl, image_hl, back, z_before):
        self.plan, self.tiles_hl = plan, tiles_hl
        self.x, self.u, self.r, self.p = x, u, r, p
        self.p_hl, self.image_hl, self.back, self.z_before = p_hl, image_hl, back, z_before
        self.slots, self.blk = p_hl.shape[0], p_hl.shape[2]
        self.targets = p_hl.shape[1] // 2
        self.zero = jnp.zeros((self.targets, self.blk), F32)

    def forward(self, observed=None):
        plan, targets, blk = self.plan, self.targets, self.blk

        def tile_step(k, acc, total):
            wide = lax.dot_general(
                self.p_hl[plan[9 + 1, k]], self.tiles_hl[plan[9 + 0, k]], (((1,), (1,)), ((), ())),
                preferred_element_type=F32)
            acc = jnp.where(plan[9 + 2, k] > 0, acc, 0.0) + join(wide, targets, blk)
            if observed is not None:
                split_store(self.image_hl, k, observed[plan[9 + 4, k]] - acc)
            else:
                split_store(self.image_hl, k, acc)
                total = total + jnp.where(plan[9 + 3, k] > 0, acc * acc, 0.0)
            return acc, total

        return loop(self.slots, GROUP, tile_step, self.zero, self.zero)[1]

    def backward(self):
        plan, targets, blk = self.plan, self.targets, self.blk

        def tile_step(k, acc):
            both = self.tiles_hl[plan[9 + 5, k]]
            weights = jnp.concatenate([both[:blk], both[blk:]], axis=1)
            wide = jnp.dot(self.image_hl[plan[9 + 6, k]], weights, preferred_element_type=F32)
            acc = jnp.where(plan[9 + 7, k] > 0, acc, 0.0) + join(wide, targets, blk)
            self.back[k] = acc
            return (acc,)

        loop(self.slots, GROUP, tile_step, self.zero)

    def load_x(self):
        def one(c, _):
            split_store(self.p_hl, c, self.x[c])
            return (_,)

        loop(self.slots, 4, one, 0)

    def begin(self, first, z_of):
        def one(c, rr, gap):
            z, x, u = z_of(c), self.x[c], self.u[c]
            diff = x - z
            u_new = u + diff
            self.u[c] = u_new
            if first:
                r = self.back[self.plan[9 + 8, c]] + (z - u_new) - x
                self.z_before[c] = z
            else:
                r = self.r[c] + ((z - u_new) - (self.z_before[c] - u))
            self.r[c] = r
            self.p[c] = r
            split_store(self.p_hl, c, r)
            return rr + r * r, gap + diff * diff

        rr, gap = loop(self.slots, 4, one, self.zero, self.zero)
        self.own = rr
        self.rr = total_of(rr)
        return gap

    def length(self):
        self.a = self.rr / total_of(self.forward() + self.own)

    def move_x(self):
        p, x, a = self.p, self.x, self.a

        def move(c, _):
            x[c] = x[c] + a * p[c]
            return (_,)

        loop(self.slots, 4, move, 0)

    def move_r(self):
        p, r, back, plan, a = self.p, self.r, self.back, self.plan, self.a
        self.backward()

        def move(c, nn):
            new = r[c] - a * (back[plan[9 + 8, c]] + p[c])
            r[c] = new
            return (nn + new * new,)

        return loop(self.slots, 4, move, self.zero)[0]

    def step(self):
        p, r, x = self.p, self.r, self.x
        self.length()
        a = self.a
        nn = total_of(self.move_r())
        ratio = nn / self.rr

        def turn(c, own):
            value = p[c]
            x[c] = x[c] + a * value
            value = r[c] + ratio * value
            p[c] = value
            split_store(self.p_hl, c, value)
            return (own + value * value,)

        self.own = loop(self.slots, 4, turn, self.zero)[0]
        self.rr = nn


def fused_kernel(table, tiles_in, observed_in, x_in, u_in, x, u_out, z_own, gap_out, *scratch):
    plan = table
    (u, tiles, observed, tiles_hl, r, p, p_hl, image_hl, back, z_before, gap_box, local_sem, gap_send, gap_recv,
     send_sem, recv_sem) = scratch[BOXES * len(ORDERS):]
    boxes = [scratch[n * len(ORDERS):(n + 1) * len(ORDERS)] for n in range(BOXES)]
    loads = [pltpu.make_async_copy(src, dst, local_sem.at[n]) for n, (src, dst) in enumerate(
        ((x_in, x), (u_in, u), (tiles_in, tiles), (observed_in, observed)))]
    for load in loads:
        load.start()
    at = Place()
    barrier = pltpu.get_barrier_semaphore()
    friends = [at.partner]
    for axis in ("x", "y", "z"):
        friends += [at.near(axis, 2)] + [at.near(axis, delta, c) for delta in (1, -1) for c in (0, 1)]
    for friend in friends:
        pl.semaphore_signal(barrier, inc=1, device_id=friend, device_id_type=MESH)
    exchange = Exchange(at, table, boxes, send_sem, recv_sem)
    solver = Solver(plan, tiles_hl, x, u, r, p, p_hl, image_hl, back, z_before)
    loads[0].wait()
    loads[1].wait()
    for part in exchange.parts:
        launch = exchange.start(part, x, u)
        if part == 0:
            pl.semaphore_wait(barrier, len(friends))
        launch()
    loads[2].wait()

    def one_tile(t, _):
        split_tile(tiles_hl, t, tiles[t])
        return (_,)

    loop(tiles.shape[0], 2, one_tile, 0)
    back[back.shape[0] - 1] = solver.zero
    loads[3].wait()
    solver.load_x()
    exchange.pass_on()
    solver.forward(observed=observed)
    solver.backward()

    def rest():
        exchange.reduce_first()
        exchange.reduce_second()
        exchange.reduce_third()
        exchange.agree()
        exchange.spread_all()
        exchange.give_back()
        exchange.give_on()
        if not exchange.first:
            exchange.keep(z_own)
        exchange.finish()

    rest()
    solver.begin(True, exchange.read)

    def advance(_, carry):
        solver.rr, solver.own = carry
        solver.step()
        return solver.rr, solver.own

    solver.rr, solver.own = lax.fori_loop(0, CG_STEPS - 1, advance, (solver.rr, solver.own))
    solver.length()
    solver.move_x()
    exchange.first = False
    for part in exchange.parts:
        exchange.start(part, x, u)()
    solver.move_r()
    exchange.pass_on()
    rest()
    gap = solver.begin(False, exchange.read)
    store = pltpu.make_async_copy(u, u_out, local_sem.at[4])
    store.start()

    gap_moves = []

    def gap_copy(n, device):
        return pltpu.make_async_remote_copy(
            src_ref=gap_box.at[10 + n // 3], dst_ref=gap_box.at[n], send_sem=gap_send.at[n],
            recv_sem=gap_recv.at[n], device_id=device, device_id_type=MESH)

    def gap_stage(stage, value):
        gap_box[10 + stage] = value
        peers = [at.near("xyz"[stage], delta) for delta in (1, 2, 3)] if stage < 3 else [at.partner]
        for n, peer in enumerate(peers):
            moving = gap_copy(3 * stage + n, peer)
            moving.start()
            gap_moves.append(moving)

    def gap_sum(stage):
        value = gap_box[10 + stage]
        for n in range(3 if stage < 3 else 1):
            gap_copy(3 * stage + n, at.partner).wait_recv()
            value = value + gap_box[3 * stage + n]
        return value

    gap_stage(0, gap)
    for number in range(CG_STEPS - 1):
        solver.step()
        gap_stage(number + 1, gap_sum(number))
    solver.length()
    solver.move_x()
    gap_out[...] = gap_sum(3)
    for moving in gap_moves:
        moving.wait_send()
    store.wait()


def fused(table, tiles, observed, x, u):
    slots, targets, blk = x.shape
    count = tiles.shape[0]
    shards = table.shape[1]
    each = lambda *shape: [pltpu.VMEM(shape + (DEEP, blk), F32) for _ in ORDERS]
    scratch = (
        each(8, 16) + each(8, 16) + each(2, 16) + each(SIDE, SIDE, PER) + each(SIDE, PER) + each(2, SIDE, PER)
        + each(SIDE, PER) + each(3, PER) + each(SIDE, SIDE, PER) + each(shards) + each(shards) + each(32)
        + [pltpu.VMEM((SUB, blk), F32) for _ in ORDERS]
        + [
            pltpu.VMEM(x.shape, F32), pltpu.VMEM(tiles.shape, F32), pltpu.VMEM(observed.shape, F32),
            pltpu.VMEM((count, 2 * blk, blk), BF16), pltpu.VMEM(x.shape, F32), pltpu.VMEM(x.shape, F32),
            pltpu.VMEM((slots, 2 * targets, blk), BF16), pltpu.VMEM((count, 2 * targets, blk), BF16),
            pltpu.VMEM((count + 1, targets, blk), F32), pltpu.VMEM(x.shape, F32),
            pltpu.VMEM((14, targets, blk), F32),
            pltpu.SemaphoreType.DMA((5,)), pltpu.SemaphoreType.DMA((10,)), pltpu.SemaphoreType.DMA((10,)),
            pltpu.SemaphoreType.DMA((len(ORDERS), SEMS)), pltpu.SemaphoreType.DMA((len(ORDERS), SEMS)),
        ]
    )
    whole = pl.BlockSpec(memory_space=pltpu.VMEM)
    scalars = pl.BlockSpec(memory_space=pltpu.SMEM)
    like = jax.ShapeDtypeStruct(x.shape, F32)
    return pl.pallas_call(
        fused_kernel,
        out_shape=(like, like, jax.ShapeDtypeStruct((PER, targets, blk), F32),
                   jax.ShapeDtypeStruct((targets, blk), F32)),
        in_specs=[scalars] + [pl.BlockSpec(memory_space=pl.ANY)] * 4,
        out_specs=(whole, pl.BlockSpec(memory_space=pl.ANY), whole, whole),
        scratch_shapes=scratch,
        compiler_params=pltpu.CompilerParams(
            collective_id=0, has_side_effects=True, vmem_limit_bytes=67043328),
        name="consensus",
    )(table, tiles, observed, x, u)


def on_device(tile_data, tile_row, tile_col, tile_count, touched, owner_map, observed, start_x, start_u):
    shards = lax.axis_size(AXES)
    local_cols = touched.shape[1]
    table = tables(tile_row, tile_col, touched, owner_map, tile_count)
    flip = lambda a: jnp.swapaxes(a, 1, 2)
    x, u, z, gap = fused(table, tile_data, flip(observed), flip(start_x), flip(start_u))
    primal_gap = jnp.sqrt(jnp.sum(gap, axis=1) / (shards * local_cols * start_x.shape[1]))
    return flip(x), flip(u), flip(z), primal_gap


def solution(mesh):
    split = P(AXES)
    return jax.shard_map(
        on_device, mesh=mesh,
        in_specs=(split, split, split, split, split, P(), split, split, split),
        out_specs=(split, split, split, P()),
        check_vma=False,
    )
```

```python
import functools

import jax
import jax.numpy as jnp
from jax import lax
from jax.experimental import pallas as pl
from jax.experimental.pallas import tpu as pltpu
from jax.sharding import PartitionSpec as P

ITERS = 2
CG_STEPS = 4
GROUP = 32
AXES = ("dev", "ka")
F32 = jnp.float32
BF16 = jnp.bfloat16
MESH = pl.DeviceIdType.MESH

SIDE = 4
SUB = 8
PER = 4
ORDERS = (("x", "y", "z"), ("y", "z", "x"), ("z", "x", "y"))
ROWS = (22, 22, 20)
DEEP = 24
S1, S1F, S2F, S2S, S2D, S3, T3, T2O, T2F, T2D, T1, T1F, SEMS = 0, 8, 9, 13, 17, 21, 25, 29, 33, 37, 41, 49, 50
THERE, BACK = (2, 1, 3, 0), (0, 1, 3, 2)
BOXES = 13


def fold(values):
    return functools.reduce(lambda s, n: s + n, values)


def split_tile(ref, index, value):
    rows = value.shape[0]
    high = value.astype(BF16)
    low = (value - high.astype(F32)).astype(BF16)
    ref[index, :rows, :] = high
    ref[index, rows:, :] = low


def split_store(ref, index, value):
    for n in range(0, value.shape[0], SUB):
        part = value[n:n + SUB]
        high = part.astype(BF16).astype(F32)
        ref[index, 2 * n:2 * n + 2 * SUB, :] = jnp.concatenate([high, part - high], axis=0).astype(BF16)


def join(wide, rows, cols):
    pieces = []
    for n in range(0, 2 * rows, 2 * SUB):
        high, low = wide[n:n + SUB], wide[n + SUB:n + 2 * SUB]
        pieces.append((high[:, :cols] + high[:, cols:]) + low[:, :cols])
    return jnp.concatenate(pieces, axis=0)


def total_of(value):
    return jnp.sum(value, axis=1, keepdims=True)


def tables_kernel(rows, cols, touched, owner_map, count, out):
    tiles, lanes = rows.shape[1], out.shape[1]
    near, far = (lax.broadcasted_iota(jnp.int32, (tiles, lanes), n) for n in (0, 1))
    down = lax.broadcasted_iota(jnp.int32, (tiles, 1), 0).astype(F32)
    across = lax.broadcasted_iota(jnp.int32, (1, lanes), 1).astype(F32)
    eye = near == far
    wide = lambda v: jnp.concatenate([v[...].astype(F32), jnp.zeros((1, lanes - tiles), F32)], axis=1)
    stand = lambda v: jnp.sum(jnp.where(eye, v, 0.0), axis=1, keepdims=True)
    lie = lambda v: jnp.sum(jnp.where(eye, v, 0.0), axis=0, keepdims=True)
    ones = lambda m: jnp.where(m, 1.0, 0.0)
    left = lambda m: jnp.sum(ones(m), axis=1, keepdims=True)
    up = lambda m: jnp.sum(ones(m), axis=0, keepdims=True)
    number = count[0].astype(F32)
    inside = across < float(tiles)

    def order(values):
        key = jnp.where(across < number, wide(values), float(tiles))
        key = jnp.where(inside, key, float(tiles + 1))
        code = key * float(lanes) + across
        key_d, code_d = stand(key), stand(code)
        same = key == key_d
        rank = left(code < code_d)
        last = left(key <= key_d) - 1.0
        keep = left(same & (code < code_d))
        later = left(same & (code > code_d))
        ends = jnp.where((later == 0.0) & (key_d < float(tiles)), 1.0, 0.0)
        return key_d, rank, last, keep, ends

    def sort(rank, values):
        return jnp.sum(jnp.where(rank == across, values, 0.0), axis=0, keepdims=True)

    row_d, rank_f, last_f, keep_f, ends_f = order(rows)
    col_d, rank_b, _, keep_b, _ = order(cols)
    found = up(col_d == across)
    until = up(col_d <= across) - 1.0
    last_b = jnp.where(found > 0.0, until, float(tiles))
    plan = [
        sort(rank_f, down), sort(rank_f, stand(wide(cols))), sort(rank_f, keep_f), sort(rank_f, ends_f),
        sort(rank_f, stand(wide(rows))), sort(rank_b, down), sort(rank_b, last_f), sort(rank_b, keep_b), last_b,
    ]
    wanted = stand(wide(touched))
    blocks = owner_map.shape[1]
    every = lax.broadcasted_iota(jnp.int32, (1, blocks), 1).astype(F32)
    position = jnp.sum(jnp.where(wanted == every, owner_map[...].astype(F32), 0.0), axis=1, keepdims=True)
    position = position.astype(jnp.int32)
    owner, tag = position >> 2, (position & 3).astype(F32)
    place = {"x": (owner >> 3) & 3, "y": owner >> 5, "z": owner & 3}
    core = (owner >> 2) & 1
    slots, marks, index = [], [], []
    for a, b, c in ORDERS:
        at = (place[a] * 32 + core * 16 + place[b] * 4 + place[c]).astype(F32)
        match = at == across
        slots.append(jnp.sum(jnp.where(match, down, 0.0), axis=0, keepdims=True))
        marks.append(jnp.sum(jnp.where(match, tag + 1.0, 0.0), axis=0, keepdims=True) - 1.0)
        index.append(lie(at))
    found = slots + marks + index + plan
    for n, row in enumerate(found):
        out[n:n + 1, :] = row.astype(jnp.int32)
    out[len(found):, :] = jnp.zeros((out.shape[0] - len(found), lanes), jnp.int32)


def tables(rows, cols, touched, owner_map, count):
    whole = pl.BlockSpec(memory_space=pltpu.VMEM)
    return pl.pallas_call(
        tables_kernel,
        out_shape=jax.ShapeDtypeStruct((24, 128), jnp.int32),
        in_specs=[whole] * 4 + [pl.BlockSpec(memory_space=pltpu.SMEM)],
        out_specs=whole,
        name="tables",
    )(rows, cols, touched, owner_map.reshape(1, -1), count)


def loop(count, step, body, *init):
    def group(g, carry):
        for n in range(step):
            carry = body(g * step + n, *carry)
        return carry

    return lax.fori_loop(0, count // step, group, init)


def near_device(me, axis, delta, to_core):
    at = dict(me)
    at[axis] = lax.rem(me[axis] + delta + SIDE, SIDE)
    return ((at["y"] * SIDE + at["x"]) * 2 + to_core, at["z"])


class Place:
    def __init__(self):
        dev, z = lax.axis_index("dev"), lax.axis_index("ka")
        self.core = lax.rem(dev, 2)
        self.me = {"x": lax.rem(dev // 2, SIDE), "y": dev // 8, "z": z}
        self.way = 1 - 2 * self.core
        self.partner = (dev + 1 - 2 * self.core, z)

    def near(self, axis, delta, to_core=None):
        return near_device(self.me, axis, delta, self.core if to_core is None else to_core)

    def ring(self, axis, delta):
        return lax.rem(self.me[axis] + delta + SIDE, SIDE)


def row_number(blk):
    return lax.broadcasted_iota(jnp.int32, (SUB, blk), 0)


def part_of(p, ref, slot):
    tile = lambda n: ref[slot, n * SUB:(n + 1) * SUB, :]
    pair = [tile(2 * p), tile(2 * p + 1)]
    if p == 0:
        return pair + [tile(6)]
    if p == 1:
        return pair + [pltpu.roll(tile(7), 6, 0)]
    edge = row_number(ref.shape[2]) < 2
    return pair + [jnp.where(edge, pltpu.roll(tile(6), 2, 0), pltpu.roll(tile(7), 2, 0))]


def from_parts(found):
    row = row_number(found[0].shape[1])
    shared = pltpu.roll(found[2][2 * SUB:], 6, 0)
    six = jnp.where(row < 6, found[0][2 * SUB:], shared)
    seven = jnp.where(row < 2, shared, pltpu.roll(found[1][2 * SUB:], 2, 0))
    return jnp.concatenate([f[:2 * SUB] for f in found] + [six, seven], axis=0)


class Exchange:
    def __init__(self, at, table, boxes, send_sem, recv_sem):
        self.at, self.table = at, table
        (self.mail, self.in1, self.fwd1, self.part2, self.fwd2, self.in2, self.part3, self.in3,
         self.zb2, self.inbox, self.sel, self.zrel, self.share) = boxes
        self.first = True
        self.send_sem, self.recv_sem = send_sem, recv_sem
        self.sends = []
        self.parts = range(len(ORDERS))

    def copy(self, p, src, dst, send, recv, device):
        return pltpu.make_async_remote_copy(
            src_ref=src, dst_ref=dst, send_sem=self.send_sem.at[p, send], recv_sem=self.recv_sem.at[p, recv],
            device_id=device, device_id_type=MESH)

    def go(self, p, src, dst, send, recv, device):
        moving = self.copy(p, src, dst, send, recv, device)
        moving.start()
        self.sends.append(moving)

    def arrive(self, p, dst, recv):
        self.copy(p, dst, dst, 0, recv, self.at.partner).wait_recv()

    def sent(self):
        for moving in self.sends:
            moving.wait_send()
        self.sends = []

    def pack(self, p, x, u, delta):
        table, parts, mail = self.table, len(ORDERS), self.mail[p]
        base = self.at.ring(ORDERS[p][0], delta) * 2

        def record(c, _):
            q = base + c
            for i in range(16):
                slot = table[p, q * 16 + i]
                for n, (one, two) in enumerate(zip(part_of(p, x, slot), part_of(p, u, slot))):
                    mail[q, i, n * SUB:(n + 1) * SUB, :] = one + two
                tag = table[parts + p, q * 16 + i]
                mail[q, i, ROWS[p]:ROWS[p] + 1, :] = jnp.full((1, x.shape[2]), tag, jnp.int32).astype(F32)
            return (_,)

        loop(2, 1, record, 0)

    def marked(self, p):
        return pl.ds(0, ROWS[p] + (1 if self.first else 0))

    def scatter_far(self, p, box, relay, base_f):
        at, a = self.at, ORDERS[p][0]
        self.go(p, box(at.ring(a, 2), None), relay, base_f, base_f, at.near(a, at.way))

    def scatter_near(self, p, delta, box, into, base):
        at, a, core = self.at, ORDERS[p][0], self.at.core
        if delta:
            for c in (0, 1):
                self.go(p, box(at.ring(a, delta), c), into(delta), base + delta * 2 + c,
                        base + delta * 2 + core, at.near(a, delta, c))
        else:
            self.go(p, box(at.me[a], 1 - core), into(0), base, base + core, at.partner)

    def relay(self, p, relay, into, base, base_f):
        at, a = self.at, ORDERS[p][0]
        self.arrive(p, relay(None), base_f)
        for c in (0, 1):
            self.go(p, relay(c), into, base + 4 + c, base + 4 + at.core, at.near(a, at.way, c))

    def start(self, x, u, ready=lambda: None):
        def box(p, place, c):
            return self.mail[p].at[pl.ds(place * 2, 2) if c is None else place * 2 + c, :, self.marked(p)]

        for p in self.parts:
            self.pack(p, x, u, 2)
            if p == 0:
                ready()
            self.scatter_far(p, functools.partial(box, p), self.fwd1[p].at[:, :, self.marked(p)], S1F)
        for delta in (1, 3, 0):
            for p in self.parts:
                self.pack(p, x, u, delta)
                self.scatter_near(
                    p, delta, functools.partial(box, p),
                    lambda delta: self.in1[p].at[delta * 2 + self.at.core, :, self.marked(p)], S1)

    def pass_on(self):
        for p in self.parts:
            fwd, rows = self.fwd1[p], self.marked(p)
            self.relay(p, lambda c: fwd.at[:, :, rows] if c is None else fwd.at[c, :, rows],
                       self.in1[p].at[4 + self.at.core, :, rows], S1, S1F)

    def sources(self, p):
        at, a = self.at, ORDERS[p][0]
        mail, in1 = self.mail[p], self.in1[p]
        found = [(0, at.core, lambda i, rows: mail[at.me[a] * 2 + at.core, i, rows, :])]
        for delta, c in ((0, 1 - at.core), (1, 0), (1, 1), (2, 0), (2, 1), (3, 0), (3, 1)):
            found.append((delta, c, lambda i, rows, n=delta * 2 + c: in1[n, i, rows, :]))
        return found

    def others(self):
        return ((1, 0), (1, 1), (3, 0), (3, 1), (0, 1 - self.at.core), (2, 0), (2, 1))

    def combine(self, p):
        found = self.sources(p)
        part2 = self.part2[p]
        blk = part2.shape[4]
        mark = ROWS[p] - 2 * SUB

        def some(a2, _):
            for a3 in range(SIDE):
                i = a2 * SIDE + a3
                tags = [jnp.broadcast_to(read(i, pl.ds(ROWS[p], 1)), (SUB, blk)) for _, _, read in found]
                hits = [[tag == float(k) for tag in tags] for k in range(PER)]
                for j in range(DEEP // SUB):
                    data = [read(i, pl.ds(j * SUB, SUB)) for _, _, read in found]
                    for k in range(PER):
                        value = fold([jnp.where(h, v, 0.0) for h, v in zip(hits[k], data)])
                        if self.first and j == 2:
                            count = fold([jnp.where(h, 1.0, 0.0) for h in hits[k]])
                            value = jnp.where(row_number(blk) == mark, count, value)
                        part2[a2, a3, k, j * SUB:(j + 1) * SUB, :] = value
            return (_,)

        loop(SIDE, 1, some, 0)

    def reduce_first(self):
        at = self.at
        for p in self.parts:
            b, d = ORDERS[p][1], ORDERS[p][2]
            rows = self.marked(p)
            for delta, c in self.others():
                self.arrive(p, self.in1[p].at[delta * 2 + c, :, rows], S1 + delta * 2 + c)
            self.combine(p)
            for n, delta in enumerate(THERE):
                piece = at.ring(d, delta)
                self.go(p, self.part2[p].at[at.ring(b, 2), piece, :, rows], self.fwd2[p].at[piece, :, rows],
                        S2F + n, S2F + n, at.near(b, at.way))
            for n, delta in enumerate(THERE):
                piece = at.ring(d, delta)
                self.go(p, self.part2[p].at[at.ring(b, -at.way), piece, :, rows], self.in2[p].at[1, piece, :, rows],
                        S2D + n, S2D + n, at.near(b, -at.way))

    def reduce_second(self):
        at = self.at
        for n, delta in enumerate(THERE):
            for p in self.parts:
                b, piece = ORDERS[p][1], at.ring(ORDERS[p][2], delta)
                rows = self.marked(p)
                self.arrive(p, self.fwd2[p].at[piece, :, rows], S2F + n)
                to = at.ring(b, at.way)
                self.part2[p][to, piece] = self.part2[p][to, piece] + self.fwd2[p][piece]
                self.go(p, self.part2[p].at[to, piece, :, rows], self.in2[p].at[0, piece, :, rows],
                        S2S + n, S2S + n, at.near(b, at.way))

    def reduce_third(self):
        at = self.at
        for n, delta in enumerate(THERE):
            for p in self.parts:
                b, d = ORDERS[p][1], ORDERS[p][2]
                piece = at.ring(d, delta)
                rows = self.marked(p)
                self.arrive(p, self.in2[p].at[1, piece, :, rows], S2D + n)
                self.arrive(p, self.in2[p].at[0, piece, :, rows], S2S + n)
                self.part3[p][piece] = (
                    self.part2[p][at.me[b], piece] + self.in2[p][0, piece] + self.in2[p][1, piece])
                if delta:
                    self.go(p, self.part3[p].at[piece, :, rows], self.in3[p].at[delta - 1, :, rows],
                            S3 + delta, S3 + delta, at.near(d, delta))

    def agree(self):
        at = self.at
        for p in self.parts:
            b, d = ORDERS[p][1], ORDERS[p][2]
            rows = self.marked(p)
            for delta in (1, 3, 2):
                self.arrive(p, self.in3[p].at[delta - 1, :, rows], S3 + delta)
            for k in range(PER):
                value = fold([self.part3[p][at.me[d], k]] + [self.in3[p][n, k] for n in range(3)])
                if self.first:
                    self.share[p][k:k + 1, :] = jnp.maximum(value[ROWS[p]:ROWS[p] + 1], 1.0)
                share = self.share[p][k:k + 1, :]
                value = value / share
                cut = jnp.broadcast_to(1.0 / share, value.shape)
                self.zb2[p][at.me[b], at.me[d], k] = value - jnp.minimum(jnp.maximum(value, -cut), cut)
            own = self.zb2[p].at[at.me[b], at.me[d], :, pl.ds(0, ROWS[p])]
            for delta in (2, 1, 3):
                self.go(p, own, own, T3 + delta, T3 + delta, at.near(d, delta))
            self.spread(p, 0)

    def keep(self, z_own):
        at = self.at
        for k in range(PER):
            z_own[k] = from_parts([self.zb2[p][at.me[ORDERS[p][1]], at.me[ORDERS[p][2]], k] for p in self.parts])

    def spread(self, p, n):
        at, b = self.at, ORDERS[p][1]
        own = self.zb2[p].at[at.me[b], at.ring(ORDERS[p][2], -BACK[n]), :, pl.ds(0, ROWS[p])]
        if n:
            self.arrive(p, own, T3 + BACK[n])
        self.go(p, own, own, T2O + n, T2O + n, at.near(b, at.way))
        self.go(p, own, own, T2D + n, T2D + n, at.near(b, -at.way))

    def spread_on(self, p, n):
        at, b = self.at, ORDERS[p][1]
        passing = self.zb2[p].at[at.ring(b, -at.way), at.ring(ORDERS[p][2], -BACK[n]), :, pl.ds(0, ROWS[p])]
        self.arrive(p, passing, T2O + n)
        self.go(p, passing, passing, T2F + n, T2F + n, at.near(b, at.way))

    def spread_all(self):
        for act, n in ((self.spread, 1), (self.spread, 2), (self.spread_on, 0), (self.spread, 3),
                       (self.spread_on, 1), (self.spread_on, 2), (self.spread_on, 3)):
            for p in self.parts:
                act(p, n)

    def select(self, p):
        at = self.at
        a = ORDERS[p][0]
        found = self.sources(p)
        zb2, inbox, sel = self.zb2[p], self.inbox[p], self.sel[p]
        tiles = [slice(j * SUB, (j + 1) * SUB) for j in range(DEEP // SUB)]

        def some(a2, _):
            for a3 in range(SIDE):
                i = a2 * SIDE + a3
                blocks = [[zb2[a2, a3, k, rows, :] for rows in tiles] for k in range(PER)]
                for number, (delta, c, read) in enumerate(found):
                    tag = jnp.broadcast_to(read(i, pl.ds(ROWS[p], 1)), blocks[0][0].shape)
                    hit = [tag == float(k) for k in range(PER - 1)]
                    for j, rows in enumerate(tiles):
                        value = blocks[PER - 1][j]
                        for k in range(PER - 1):
                            value = jnp.where(hit[k], blocks[k][j], value)
                        place = (at.ring(a, -delta) * 2 + c) * 16 + i
                        (sel if number else inbox)[place, rows, :] = value
            return (_,)

        loop(SIDE, 1, some, 0)

    def give_back(self):
        at = self.at
        self.sent()
        for p in self.parts:
            a, b = ORDERS[p][0], ORDERS[p][1]
            rows = pl.ds(0, ROWS[p])
            for n, delta in enumerate(BACK):
                piece = at.ring(ORDERS[p][2], -delta)
                self.arrive(p, self.zb2[p].at[at.ring(b, at.way), piece, :, rows], T2D + n)
                self.arrive(p, self.zb2[p].at[at.ring(b, 2), piece, :, rows], T2F + n)
            self.select(p)
            sel = self.sel[p]

            def box(place, c):
                return sel.at[pl.ds(place * 32, 32) if c is None else pl.ds((place * 2 + c) * 16, 16), rows]

            mine = self.inbox[p].at[pl.ds((at.me[a] * 2 + at.core) * 16, 16), rows]
            self.scatter_far(p, box, self.zrel[p].at[:, rows], T1F)
            for delta in (1, 3, 0):
                self.scatter_near(p, delta, box, lambda delta: mine, T1)

    def give_on(self):
        at = self.at
        for p in self.parts:
            zrel, a = self.zrel[p], ORDERS[p][0]
            rows = pl.ds(0, ROWS[p])
            self.relay(p, lambda c: zrel.at[:, rows] if c is None else zrel.at[pl.ds(c * 16, 16), rows],
                       self.inbox[p].at[pl.ds((at.ring(a, -at.way) * 2 + at.core) * 16, 16), rows], T1, T1F)

    def finish(self):
        at = self.at
        for p in self.parts:
            a, rows = ORDERS[p][0], pl.ds(0, ROWS[p])
            for delta, c in self.others():
                self.arrive(p, self.inbox[p].at[pl.ds((at.ring(a, -delta) * 2 + c) * 16, 16), rows],
                            T1 + delta * 2 + c)
        self.sent()

    def read(self, c):
        return from_parts([self.inbox[p][self.table[2 * len(ORDERS) + p, c]] for p in self.parts])


class Solver:
    def __init__(self, plan, tiles_hl, x, u, r, p, p_hl, image_hl, back, z_before):
        self.plan, self.tiles_hl = plan, tiles_hl
        self.x, self.u, self.r, self.p = x, u, r, p
        self.p_hl, self.image_hl, self.back, self.z_before = p_hl, image_hl, back, z_before
        self.slots, self.blk = p_hl.shape[0], p_hl.shape[2]
        self.targets = p_hl.shape[1] // 2
        self.zero = jnp.zeros((self.targets, self.blk), F32)

    def forward(self, observed=None):
        plan, targets, blk = self.plan, self.targets, self.blk

        def tile_step(k, acc, total):
            wide = lax.dot_general(
                self.p_hl[plan[9 + 1, k]], self.tiles_hl[plan[9 + 0, k]], (((1,), (1,)), ((), ())),
                preferred_element_type=F32)
            acc = jnp.where(plan[9 + 2, k] > 0, acc, 0.0) + join(wide, targets, blk)
            if observed is not None:
                split_store(self.image_hl, k, observed[plan[9 + 4, k]] - acc)
            else:
                split_store(self.image_hl, k, acc)
                total = total + jnp.where(plan[9 + 3, k] > 0, acc * acc, 0.0)
            return acc, total

        return loop(self.slots, GROUP, tile_step, self.zero, self.zero)[1]

    def backward(self):
        plan, targets, blk = self.plan, self.targets, self.blk

        def tile_step(k, acc):
            both = self.tiles_hl[plan[9 + 5, k]]
            weights = jnp.concatenate([both[:blk], both[blk:]], axis=1)
            wide = jnp.dot(self.image_hl[plan[9 + 6, k]], weights, preferred_element_type=F32)
            acc = jnp.where(plan[9 + 7, k] > 0, acc, 0.0) + join(wide, targets, blk)
            self.back[k] = acc
            return (acc,)

        loop(self.slots, GROUP, tile_step, self.zero)

    def load_x(self):
        def one(c, _):
            split_store(self.p_hl, c, self.x[c])
            return (_,)

        loop(self.slots, 4, one, 0)

    def begin(self, first, z_of):
        def one(c, rr, gap):
            z, x, u = z_of(c), self.x[c], self.u[c]
            diff = x - z
            u_new = u + diff
            self.u[c] = u_new
            if first:
                r = self.back[self.plan[9 + 8, c]] + (z - u_new) - x
                self.z_before[c] = z
            else:
                r = self.r[c] + ((z - u_new) - (self.z_before[c] - u))
            self.r[c] = r
            self.p[c] = r
            split_store(self.p_hl, c, r)
            return rr + r * r, gap + diff * diff

        rr, gap = loop(self.slots, 4, one, self.zero, self.zero)
        self.own = rr
        self.rr = total_of(rr)
        return gap

    def length(self):
        self.a = self.rr / total_of(self.forward() + self.own)

    def move_x(self):
        p, x, a = self.p, self.x, self.a

        def move(c, _):
            x[c] = x[c] + a * p[c]
            return (_,)

        loop(self.slots, 4, move, 0)

    def move_r(self):
        p, r, back, plan, a = self.p, self.r, self.back, self.plan, self.a
        self.backward()

        def move(c, nn):
            new = r[c] - a * (back[plan[9 + 8, c]] + p[c])
            r[c] = new
            return (nn + new * new,)

        return loop(self.slots, 4, move, self.zero)[0]

    def step(self):
        p, r, x = self.p, self.r, self.x
        self.length()
        a = self.a
        nn = total_of(self.move_r())
        ratio = nn / self.rr

        def turn(c, own):
            value = p[c]
            x[c] = x[c] + a * value
            value = r[c] + ratio * value
            p[c] = value
            split_store(self.p_hl, c, value)
            return (own + value * value,)

        self.own = loop(self.slots, 4, turn, self.zero)[0]
        self.rr = nn


def fused_kernel(table, tiles_in, observed_in, x_in, u_in, x, u_out, z_own, gap_out, *scratch):
    plan = table
    (u, tiles, observed, tiles_hl, r, p, p_hl, image_hl, back, z_before, gap_box, local_sem, gap_send, gap_recv,
     send_sem, recv_sem) = scratch[BOXES * len(ORDERS):]
    boxes = [scratch[n * len(ORDERS):(n + 1) * len(ORDERS)] for n in range(BOXES)]
    loads = [pltpu.make_async_copy(src, dst, local_sem.at[n]) for n, (src, dst) in enumerate(
        ((x_in, x), (u_in, u), (tiles_in, tiles), (observed_in, observed)))]
    for load in loads:
        load.start()
    at = Place()
    barrier = pltpu.get_barrier_semaphore()
    friends = [at.partner]
    for axis in ("x", "y", "z"):
        friends += [at.near(axis, 2)] + [at.near(axis, delta, c) for delta in (1, -1) for c in (0, 1)]
    for friend in friends:
        pl.semaphore_signal(barrier, inc=1, device_id=friend, device_id_type=MESH)
    exchange = Exchange(at, table, boxes, send_sem, recv_sem)
    solver = Solver(plan, tiles_hl, x, u, r, p, p_hl, image_hl, back, z_before)
    loads[0].wait()
    loads[1].wait()
    exchange.start(x, u, lambda: pl.semaphore_wait(barrier, len(friends)))
    loads[2].wait()

    def one_tile(t, _):
        split_tile(tiles_hl, t, tiles[t])
        return (_,)

    loop(tiles.shape[0], 2, one_tile, 0)
    back[back.shape[0] - 1] = solver.zero
    loads[3].wait()
    solver.load_x()
    exchange.pass_on()
    solver.forward(observed=observed)
    solver.backward()

    def rest():
        exchange.reduce_first()
        exchange.reduce_second()
        exchange.reduce_third()
        exchange.agree()
        exchange.spread_all()
        exchange.give_back()
        exchange.give_on()
        if not exchange.first:
            exchange.keep(z_own)
        exchange.finish()

    rest()
    solver.begin(True, exchange.read)

    def advance(_, carry):
        solver.rr, solver.own = carry
        solver.step()
        return solver.rr, solver.own

    solver.rr, solver.own = lax.fori_loop(0, CG_STEPS - 1, advance, (solver.rr, solver.own))
    solver.length()
    solver.move_x()
    exchange.first = False
    exchange.start(x, u)
    solver.move_r()
    exchange.pass_on()
    rest()
    gap = solver.begin(False, exchange.read)
    store = pltpu.make_async_copy(u, u_out, local_sem.at[4])
    store.start()

    def gap_copy(n, stage, device):
        return pltpu.make_async_remote_copy(
            src_ref=gap_box.at[10 + stage], dst_ref=gap_box.at[n], send_sem=gap_send.at[n],
            recv_sem=gap_recv.at[n], device_id=device, device_id_type=MESH)

    def gap_peer(stage, delta):
        along = {"x": (1 - stage) * (2 - stage) // 2, "y": stage * (2 - stage), "z": stage * (stage - 1) // 2}
        to = {a: lax.rem(at.me[a] + delta * along[a], SIDE) for a in along}
        return ((to["y"] * SIDE + to["x"]) * 2 + at.core, to["z"])

    def gap_step(stage, carry):
        solver.rr, solver.own = carry
        moves = [gap_copy(3 * stage + delta - 1, stage, gap_peer(stage, delta)) for delta in (1, 2, 3)]
        for moving in moves:
            moving.start()
        solver.step()
        value = gap_box[10 + stage]
        for n, moving in enumerate(moves):
            moving.wait()
            value = value + gap_box[3 * stage + n]
        gap_box[11 + stage] = value
        return solver.rr, solver.own

    gap_box[10] = gap
    solver.rr, solver.own = lax.fori_loop(0, CG_STEPS - 1, gap_step, (solver.rr, solver.own))
    moving = gap_copy(9, 3, at.partner)
    moving.start()
    solver.length()
    solver.move_x()
    moving.wait()
    gap_out[...] = gap_box[13] + gap_box[9]
    store.wait()


def hand_over_kernel(scale, x_in, u_in, z_in, gap, x, u, z, primal, x_box, u_box, z_box, sems):
    step = x_in.shape[0] // 4
    moves = [(z_in, z_box, z)]
    for n in range(4):
        rows = pl.ds(n * step, step)
        moves += [(a.at[rows], b.at[rows], c.at[rows]) for a, b, c in ((x_in, x_box, x), (u_in, u_box, u))]
    reads = [pltpu.make_async_copy(a, b, sems.at[0, n]) for n, (a, b, _) in enumerate(moves)]
    writes = [pltpu.make_async_copy(b, c, sems.at[1, n]) for n, (_, b, c) in enumerate(moves)]
    for read in reads:
        read.start()
    targets, blk = gap.shape
    down, across = (lax.broadcasted_iota(jnp.int32, (targets, blk), n) for n in (0, 1))
    total = jnp.sum(gap[...], axis=1, keepdims=True)
    total = jnp.sum(jnp.where(down == across, total, 0.0), axis=0, keepdims=True)
    primal[...] = jnp.sqrt(total / scale)
    for read, write in zip(reads, writes):
        read.wait()
        write.start()
    for write in writes:
        write.wait()


def hand_over(scale, x, u, z, gap):
    anywhere, whole = pl.BlockSpec(memory_space=pl.ANY), pl.BlockSpec(memory_space=pltpu.VMEM)
    like = [jax.ShapeDtypeStruct(a.shape, F32) for a in (x, u, z)]
    return pl.pallas_call(
        functools.partial(hand_over_kernel, float(scale)),
        out_shape=(*like, jax.ShapeDtypeStruct((1, gap.shape[1]), F32)),
        in_specs=[anywhere] * 3 + [whole],
        out_specs=(anywhere, anywhere, anywhere, whole),
        scratch_shapes=[pltpu.VMEM(a.shape, F32) for a in (x, u, z)] + [pltpu.SemaphoreType.DMA((2, 9))],
        compiler_params=pltpu.CompilerParams(vmem_limit_bytes=67043328),
        name="hand_over",
    )(x, u, z, gap)


def fused(table, tiles, observed, x, u):
    slots, targets, blk = x.shape
    count = tiles.shape[0]
    shards = table.shape[1]
    each = lambda *shape: [pltpu.VMEM(shape + (DEEP, blk), F32) for _ in ORDERS]
    scratch = (
        each(8, 16) + each(8, 16) + each(2, 16) + each(SIDE, SIDE, PER) + each(SIDE, PER) + each(2, SIDE, PER)
        + each(SIDE, PER) + each(3, PER) + each(SIDE, SIDE, PER) + each(shards) + each(shards) + each(32)
        + [pltpu.VMEM((SUB, blk), F32) for _ in ORDERS]
        + [
            pltpu.VMEM(x.shape, F32), pltpu.VMEM(tiles.shape, F32), pltpu.VMEM(observed.shape, F32),
            pltpu.VMEM((count, 2 * blk, blk), BF16), pltpu.VMEM(x.shape, F32), pltpu.VMEM(x.shape, F32),
            pltpu.VMEM((slots, 2 * targets, blk), BF16), pltpu.VMEM((count, 2 * targets, blk), BF16),
            pltpu.VMEM((count + 1, targets, blk), F32), pltpu.VMEM(x.shape, F32),
            pltpu.VMEM((14, targets, blk), F32),
            pltpu.SemaphoreType.DMA((5,)), pltpu.SemaphoreType.DMA((10,)), pltpu.SemaphoreType.DMA((10,)),
            pltpu.SemaphoreType.DMA((len(ORDERS), SEMS)), pltpu.SemaphoreType.DMA((len(ORDERS), SEMS)),
        ]
    )
    whole = pl.BlockSpec(memory_space=pltpu.VMEM)
    scalars = pl.BlockSpec(memory_space=pltpu.SMEM)
    like = jax.ShapeDtypeStruct(x.shape, F32)
    return pl.pallas_call(
        fused_kernel,
        out_shape=(like, like, jax.ShapeDtypeStruct((PER, targets, blk), F32),
                   jax.ShapeDtypeStruct((targets, blk), F32)),
        in_specs=[scalars] + [pl.BlockSpec(memory_space=pl.ANY)] * 4,
        out_specs=(whole, pl.BlockSpec(memory_space=pl.ANY), whole, whole),
        scratch_shapes=scratch,
        compiler_params=pltpu.CompilerParams(
            collective_id=0, has_side_effects=True, vmem_limit_bytes=67043328),
        name="consensus",
    )(table, tiles, observed, x, u)


def on_device(tile_data, tile_row, tile_col, tile_count, touched, owner_map, observed, start_x, start_u):
    shards = lax.axis_size(AXES)
    local_cols = touched.shape[1]
    table = tables(tile_row, tile_col, touched, owner_map, tile_count)
    flip = lambda a: jnp.swapaxes(a, 1, 2)
    x, u, z, gap = fused(table, tile_data, flip(observed), flip(start_x), flip(start_u))
    x, u, z, primal = hand_over(shards * local_cols * start_x.shape[1], x, u, z, gap)
    return flip(x), flip(u), flip(z), primal[0, :start_x.shape[2]]


def solution(mesh):
    split = P(AXES)
    return jax.shard_map(
        on_device, mesh=mesh,
        in_specs=(split, split, split, split, split, P(), split, split, split),
        out_specs=(split, split, split, P()),
        check_vma=False,
    )
```

```python
import functools

import jax
import jax.numpy as jnp
from jax import lax
from jax.experimental import pallas as pl
from jax.experimental.pallas import tpu as pltpu
from jax.sharding import PartitionSpec as P

ITERS = 2
CG_STEPS = 4
GROUP = 32
AXES = ("dev", "ka")
F32 = jnp.float32
BF16 = jnp.bfloat16
MESH = pl.DeviceIdType.MESH

SIDE = 4
SUB = 8
PER = 4
ORDERS = (("x", "y", "z"), ("y", "z", "x"), ("z", "x", "y"))
ROWS = (22, 22, 20)
DEEP = 24
S1, S1F, S2F, S2S, S2D, S3, T3, T2O, T2F, T2D, T1, T1F, SEMS = 0, 8, 9, 13, 17, 21, 25, 29, 33, 37, 41, 49, 50
THERE, BACK = (2, 1, 3, 0), (0, 1, 3, 2)
BOXES = 13


def fold(values):
    return functools.reduce(lambda s, n: s + n, values)


def split_tile(ref, index, value):
    rows = value.shape[0]
    high = value.astype(BF16)
    low = (value - high.astype(F32)).astype(BF16)
    ref[index, :rows, :] = high
    ref[index, rows:, :] = low


def split_store(ref, index, value):
    for n in range(0, value.shape[0], SUB):
        part = value[n:n + SUB]
        high = part.astype(BF16).astype(F32)
        ref[index, 2 * n:2 * n + 2 * SUB, :] = jnp.concatenate([high, part - high], axis=0).astype(BF16)


def join(wide, rows, cols):
    pieces = []
    for n in range(0, 2 * rows, 2 * SUB):
        high, low = wide[n:n + SUB], wide[n + SUB:n + 2 * SUB]
        pieces.append((high[:, :cols] + high[:, cols:]) + low[:, :cols])
    return jnp.concatenate(pieces, axis=0)


def total_of(value):
    return jnp.sum(value, axis=1, keepdims=True)


def tables_kernel(rows, cols, touched, owner_map, count, out):
    tiles, lanes = rows.shape[1], out.shape[1]
    near, far = (lax.broadcasted_iota(jnp.int32, (tiles, lanes), n) for n in (0, 1))
    down = lax.broadcasted_iota(jnp.int32, (tiles, 1), 0).astype(F32)
    across = lax.broadcasted_iota(jnp.int32, (1, lanes), 1).astype(F32)
    eye = near == far
    wide = lambda v: jnp.concatenate([v[...].astype(F32), jnp.zeros((1, lanes - tiles), F32)], axis=1)
    stand = lambda v: jnp.sum(jnp.where(eye, v, 0.0), axis=1, keepdims=True)
    lie = lambda v: jnp.sum(jnp.where(eye, v, 0.0), axis=0, keepdims=True)
    ones = lambda m: jnp.where(m, 1.0, 0.0)
    left = lambda m: jnp.sum(ones(m), axis=1, keepdims=True)
    up = lambda m: jnp.sum(ones(m), axis=0, keepdims=True)
    number = count[0].astype(F32)
    inside = across < float(tiles)

    def order(values):
        key = jnp.where(across < number, wide(values), float(tiles))
        key = jnp.where(inside, key, float(tiles + 1))
        code = key * float(lanes) + across
        key_d, code_d = stand(key), stand(code)
        same = key == key_d
        rank = left(code < code_d)
        last = left(key <= key_d) - 1.0
        keep = left(same & (code < code_d))
        later = left(same & (code > code_d))
        ends = jnp.where((later == 0.0) & (key_d < float(tiles)), 1.0, 0.0)
        return key_d, rank, last, keep, ends

    def sort(rank, values):
        return jnp.sum(jnp.where(rank == across, values, 0.0), axis=0, keepdims=True)

    row_d, rank_f, last_f, keep_f, ends_f = order(rows)
    col_d, rank_b, _, keep_b, _ = order(cols)
    found = up(col_d == across)
    until = up(col_d <= across) - 1.0
    last_b = jnp.where(found > 0.0, until, float(tiles))
    plan = [
        sort(rank_f, down), sort(rank_f, stand(wide(cols))), sort(rank_f, keep_f), sort(rank_f, ends_f),
        sort(rank_f, stand(wide(rows))), sort(rank_b, down), sort(rank_b, last_f), sort(rank_b, keep_b), last_b,
    ]
    wanted = stand(wide(touched))
    blocks = owner_map.shape[1]
    every = lax.broadcasted_iota(jnp.int32, (1, blocks), 1).astype(F32)
    position = jnp.sum(jnp.where(wanted == every, owner_map[...].astype(F32), 0.0), axis=1, keepdims=True)
    position = position.astype(jnp.int32)
    owner, tag = position >> 2, (position & 3).astype(F32)
    place = {"x": (owner >> 3) & 3, "y": owner >> 5, "z": owner & 3}
    core = (owner >> 2) & 1
    slots, marks, index = [], [], []
    for a, b, c in ORDERS:
        at = (place[a] * 32 + core * 16 + place[b] * 4 + place[c]).astype(F32)
        match = at == across
        slots.append(jnp.sum(jnp.where(match, down, 0.0), axis=0, keepdims=True))
        marks.append(jnp.sum(jnp.where(match, tag + 1.0, 0.0), axis=0, keepdims=True) - 1.0)
        index.append(lie(at))
    found = slots + marks + index + plan
    for n, row in enumerate(found):
        out[n:n + 1, :] = row.astype(jnp.int32)
    out[len(found):, :] = jnp.zeros((out.shape[0] - len(found), lanes), jnp.int32)


def tables(rows, cols, touched, owner_map, count):
    whole = pl.BlockSpec(memory_space=pltpu.VMEM)
    return pl.pallas_call(
        tables_kernel,
        out_shape=jax.ShapeDtypeStruct((24, 128), jnp.int32),
        in_specs=[whole] * 4 + [pl.BlockSpec(memory_space=pltpu.SMEM)],
        out_specs=whole,
        name="tables",
    )(rows, cols, touched, owner_map.reshape(1, -1), count)


def loop(count, step, body, *init):
    def group(g, carry):
        for n in range(step):
            carry = body(g * step + n, *carry)
        return carry

    return lax.fori_loop(0, count // step, group, init)


def near_device(me, axis, delta, to_core):
    at = dict(me)
    at[axis] = lax.rem(me[axis] + delta + SIDE, SIDE)
    return ((at["y"] * SIDE + at["x"]) * 2 + to_core, at["z"])


class Place:
    def __init__(self):
        dev, z = lax.axis_index("dev"), lax.axis_index("ka")
        self.core = lax.rem(dev, 2)
        self.me = {"x": lax.rem(dev // 2, SIDE), "y": dev // 8, "z": z}
        self.way = 1 - 2 * self.core
        self.partner = (dev + 1 - 2 * self.core, z)

    def near(self, axis, delta, to_core=None):
        return near_device(self.me, axis, delta, self.core if to_core is None else to_core)

    def ring(self, axis, delta):
        return lax.rem(self.me[axis] + delta + SIDE, SIDE)


def row_number(blk):
    return lax.broadcasted_iota(jnp.int32, (SUB, blk), 0)


def part_of(p, ref, slot):
    tile = lambda n: ref[slot, n * SUB:(n + 1) * SUB, :]
    pair = [tile(2 * p), tile(2 * p + 1)]
    if p == 0:
        return pair + [tile(6)]
    if p == 1:
        return pair + [pltpu.roll(tile(7), 6, 0)]
    edge = row_number(ref.shape[2]) < 2
    return pair + [jnp.where(edge, pltpu.roll(tile(6), 2, 0), pltpu.roll(tile(7), 2, 0))]


def from_parts(found):
    row = row_number(found[0].shape[1])
    shared = pltpu.roll(found[2][2 * SUB:], 6, 0)
    six = jnp.where(row < 6, found[0][2 * SUB:], shared)
    seven = jnp.where(row < 2, shared, pltpu.roll(found[1][2 * SUB:], 2, 0))
    return jnp.concatenate([f[:2 * SUB] for f in found] + [six, seven], axis=0)


class Exchange:
    def __init__(self, at, table, boxes, send_sem, recv_sem):
        self.at, self.table = at, table
        (self.mail, self.in1, self.fwd1, self.part2, self.fwd2, self.in2, self.part3, self.in3,
         self.zb2, self.inbox, self.sel, self.zrel, self.share) = boxes
        self.first = True
        self.send_sem, self.recv_sem = send_sem, recv_sem
        self.sends = []
        self.parts = range(len(ORDERS))

    def copy(self, p, src, dst, send, recv, device):
        return pltpu.make_async_remote_copy(
            src_ref=src, dst_ref=dst, send_sem=self.send_sem.at[p, send], recv_sem=self.recv_sem.at[p, recv],
            device_id=device, device_id_type=MESH)

    def go(self, p, src, dst, send, recv, device):
        moving = self.copy(p, src, dst, send, recv, device)
        moving.start()
        self.sends.append(moving)

    def arrive(self, p, dst, recv):
        self.copy(p, dst, dst, 0, recv, self.at.partner).wait_recv()

    def sent(self):
        for moving in self.sends:
            moving.wait_send()
        self.sends = []

    def pack(self, p, x, u, delta):
        table, parts, mail = self.table, len(ORDERS), self.mail[p]
        base = self.at.ring(ORDERS[p][0], delta) * 2

        def record(c, _):
            q = base + c
            for i in range(16):
                slot = table[p, q * 16 + i]
                for n, (one, two) in enumerate(zip(part_of(p, x, slot), part_of(p, u, slot))):
                    mail[q, i, n * SUB:(n + 1) * SUB, :] = one + two
                tag = table[parts + p, q * 16 + i]
                mail[q, i, ROWS[p]:ROWS[p] + 1, :] = jnp.full((1, x.shape[2]), tag, jnp.int32).astype(F32)
            return (_,)

        loop(2, 1, record, 0)

    def marked(self, p):
        return pl.ds(0, ROWS[p] + (1 if self.first else 0))

    def scatter_far(self, p, box, relay, base_f):
        at, a = self.at, ORDERS[p][0]
        self.go(p, box(at.ring(a, 2), None), relay, base_f, base_f, at.near(a, at.way))

    def scatter_near(self, p, delta, box, into, base):
        at, a, core = self.at, ORDERS[p][0], self.at.core
        if delta:
            for c in (0, 1):
                self.go(p, box(at.ring(a, delta), c), into(delta), base + delta * 2 + c,
                        base + delta * 2 + core, at.near(a, delta, c))
        else:
            self.go(p, box(at.me[a], 1 - core), into(0), base, base + core, at.partner)

    def relay(self, p, relay, into, base, base_f):
        at, a = self.at, ORDERS[p][0]
        self.arrive(p, relay(None), base_f)
        for c in (0, 1):
            self.go(p, relay(c), into, base + 4 + c, base + 4 + at.core, at.near(a, at.way, c))

    def start(self, x, u, ready=lambda: None):
        def box(p, place, c):
            return self.mail[p].at[pl.ds(place * 2, 2) if c is None else place * 2 + c, :, self.marked(p)]

        for p in self.parts:
            self.pack(p, x, u, 2)
            if p == 0:
                ready()
            self.scatter_far(p, functools.partial(box, p), self.fwd1[p].at[:, :, self.marked(p)], S1F)
        for delta in (1, 3, 0):
            for p in self.parts:
                self.pack(p, x, u, delta)
                self.scatter_near(
                    p, delta, functools.partial(box, p),
                    lambda delta: self.in1[p].at[delta * 2 + self.at.core, :, self.marked(p)], S1)

    def pass_on(self):
        for p in self.parts:
            fwd, rows = self.fwd1[p], self.marked(p)
            self.relay(p, lambda c: fwd.at[:, :, rows] if c is None else fwd.at[c, :, rows],
                       self.in1[p].at[4 + self.at.core, :, rows], S1, S1F)

    def sources(self, p):
        at, a = self.at, ORDERS[p][0]
        mail, in1 = self.mail[p], self.in1[p]
        found = [(0, at.core, lambda i, rows: mail[at.me[a] * 2 + at.core, i, rows, :])]
        for delta, c in ((0, 1 - at.core), (1, 0), (1, 1), (2, 0), (2, 1), (3, 0), (3, 1)):
            found.append((delta, c, lambda i, rows, n=delta * 2 + c: in1[n, i, rows, :]))
        return found

    def others(self):
        return ((1, 0), (1, 1), (3, 0), (3, 1), (0, 1 - self.at.core), (2, 0), (2, 1))

    def combine(self, p, far):
        at, b = self.at, ORDERS[p][1]
        found = self.sources(p)
        part2 = self.part2[p]
        blk = part2.shape[4]
        mark = ROWS[p] - 2 * SUB

        def some(n, _):
            a2 = at.ring(b, 2) if far else at.ring(b, at.way * (n - 1))
            for a3 in range(SIDE):
                i = a2 * SIDE + a3
                tags = [jnp.broadcast_to(read(i, pl.ds(ROWS[p], 1)), (SUB, blk)) for _, _, read in found]
                hits = [[tag == float(k) for tag in tags] for k in range(PER)]
                for j in range(DEEP // SUB):
                    data = [read(i, pl.ds(j * SUB, SUB)) for _, _, read in found]
                    for k in range(PER):
                        value = fold([jnp.where(h, v, 0.0) for h, v in zip(hits[k], data)])
                        if self.first and j == 2:
                            count = fold([jnp.where(h, 1.0, 0.0) for h in hits[k]])
                            value = jnp.where(row_number(blk) == mark, count, value)
                        part2[a2, a3, k, j * SUB:(j + 1) * SUB, :] = value
            return (_,)

        if far:
            some(0, 0)
        else:
            loop(SIDE - 1, 1, some, 0)

    def reduce_first(self):
        at = self.at
        for p in self.parts:
            b, d = ORDERS[p][1], ORDERS[p][2]
            rows = self.marked(p)
            for delta, c in self.others():
                self.arrive(p, self.in1[p].at[delta * 2 + c, :, rows], S1 + delta * 2 + c)
            self.combine(p, True)
            for n, delta in enumerate(THERE):
                piece = at.ring(d, delta)
                self.go(p, self.part2[p].at[at.ring(b, 2), piece, :, rows], self.fwd2[p].at[piece, :, rows],
                        S2F + n, S2F + n, at.near(b, at.way))
        for p in self.parts:
            b, d = ORDERS[p][1], ORDERS[p][2]
            rows = self.marked(p)
            self.combine(p, False)
            for n, delta in enumerate(THERE):
                piece = at.ring(d, delta)
                self.go(p, self.part2[p].at[at.ring(b, -at.way), piece, :, rows], self.in2[p].at[1, piece, :, rows],
                        S2D + n, S2D + n, at.near(b, -at.way))

    def reduce_second(self):
        at = self.at
        for n, delta in enumerate(THERE):
            for p in self.parts:
                b, piece = ORDERS[p][1], at.ring(ORDERS[p][2], delta)
                rows = self.marked(p)
                self.arrive(p, self.fwd2[p].at[piece, :, rows], S2F + n)
                to = at.ring(b, at.way)
                self.part2[p][to, piece] = self.part2[p][to, piece] + self.fwd2[p][piece]
                self.go(p, self.part2[p].at[to, piece, :, rows], self.in2[p].at[0, piece, :, rows],
                        S2S + n, S2S + n, at.near(b, at.way))

    def reduce_third(self):
        at = self.at
        for n, delta in enumerate(THERE):
            for p in self.parts:
                b, d = ORDERS[p][1], ORDERS[p][2]
                piece = at.ring(d, delta)
                rows = self.marked(p)
                self.arrive(p, self.in2[p].at[1, piece, :, rows], S2D + n)
                self.arrive(p, self.in2[p].at[0, piece, :, rows], S2S + n)
                self.part3[p][piece] = (
                    self.part2[p][at.me[b], piece] + self.in2[p][0, piece] + self.in2[p][1, piece])
                if delta:
                    self.go(p, self.part3[p].at[piece, :, rows], self.in3[p].at[delta - 1, :, rows],
                            S3 + delta, S3 + delta, at.near(d, delta))

    def agree(self):
        at = self.at
        for p in self.parts:
            b, d = ORDERS[p][1], ORDERS[p][2]
            rows = self.marked(p)
            for delta in (1, 3, 2):
                self.arrive(p, self.in3[p].at[delta - 1, :, rows], S3 + delta)
            for k in range(PER):
                value = fold([self.part3[p][at.me[d], k]] + [self.in3[p][n, k] for n in range(3)])
                if self.first:
                    self.share[p][k:k + 1, :] = jnp.maximum(value[ROWS[p]:ROWS[p] + 1], 1.0)
                share = self.share[p][k:k + 1, :]
                value = value / share
                cut = jnp.broadcast_to(1.0 / share, value.shape)
                self.zb2[p][at.me[b], at.me[d], k] = value - jnp.minimum(jnp.maximum(value, -cut), cut)
            own = self.zb2[p].at[at.me[b], at.me[d], :, pl.ds(0, ROWS[p])]
            for delta in (2, 1, 3):
                self.go(p, own, own, T3 + delta, T3 + delta, at.near(d, delta))
            self.spread(p, 0)

    def keep(self, z_own):
        at = self.at
        for k in range(PER):
            z_own[k] = from_parts([self.zb2[p][at.me[ORDERS[p][1]], at.me[ORDERS[p][2]], k] for p in self.parts])

    def spread(self, p, n):
        at, b = self.at, ORDERS[p][1]
        own = self.zb2[p].at[at.me[b], at.ring(ORDERS[p][2], -BACK[n]), :, pl.ds(0, ROWS[p])]
        if n:
            self.arrive(p, own, T3 + BACK[n])
        self.go(p, own, own, T2O + n, T2O + n, at.near(b, at.way))
        self.go(p, own, own, T2D + n, T2D + n, at.near(b, -at.way))

    def spread_on(self, p, n):
        at, b = self.at, ORDERS[p][1]
        passing = self.zb2[p].at[at.ring(b, -at.way), at.ring(ORDERS[p][2], -BACK[n]), :, pl.ds(0, ROWS[p])]
        self.arrive(p, passing, T2O + n)
        self.go(p, passing, passing, T2F + n, T2F + n, at.near(b, at.way))

    def spread_all(self):
        for act, n in ((self.spread, 1), (self.spread, 2), (self.spread_on, 0), (self.spread, 3),
                       (self.spread_on, 1), (self.spread_on, 2), (self.spread_on, 3)):
            for p in self.parts:
                act(p, n)

    def select(self, p, far):
        at = self.at
        a = ORDERS[p][0]
        found = self.sources(p)
        zb2, inbox, sel = self.zb2[p], self.inbox[p], self.sel[p]
        tiles = [slice(j * SUB, (j + 1) * SUB) for j in range(DEEP // SUB)]

        def some(a2, _):
            for a3 in range(SIDE):
                i = a2 * SIDE + a3
                blocks = [[zb2[a2, a3, k, rows, :] for rows in tiles] for k in range(PER)]
                for number, (delta, c, read) in enumerate(found):
                    if (delta == 2) != far:
                        continue
                    tag = jnp.broadcast_to(read(i, pl.ds(ROWS[p], 1)), blocks[0][0].shape)
                    hit = [tag == float(k) for k in range(PER - 1)]
                    for j, rows in enumerate(tiles):
                        value = blocks[PER - 1][j]
                        for k in range(PER - 1):
                            value = jnp.where(hit[k], blocks[k][j], value)
                        place = (at.ring(a, -delta) * 2 + c) * 16 + i
                        (sel if number else inbox)[place, rows, :] = value
            return (_,)

        loop(SIDE, 1, some, 0)

    def give_back(self):
        at = self.at
        self.sent()
        for p in self.parts:
            a, b = ORDERS[p][0], ORDERS[p][1]
            rows = pl.ds(0, ROWS[p])
            for n, delta in enumerate(BACK):
                piece = at.ring(ORDERS[p][2], -delta)
                self.arrive(p, self.zb2[p].at[at.ring(b, at.way), piece, :, rows], T2D + n)
                self.arrive(p, self.zb2[p].at[at.ring(b, 2), piece, :, rows], T2F + n)
            self.select(p, True)
            self.scatter_far(p, functools.partial(self.sel_box, p), self.zrel[p].at[:, rows], T1F)
        for p in self.parts:
            a, rows = ORDERS[p][0], pl.ds(0, ROWS[p])
            mine = self.inbox[p].at[pl.ds((at.me[a] * 2 + at.core) * 16, 16), rows]
            self.select(p, False)
            for delta in (1, 3, 0):
                self.scatter_near(p, delta, functools.partial(self.sel_box, p), lambda delta: mine, T1)

    def sel_box(self, p, place, c):
        records = pl.ds(place * 32, 32) if c is None else pl.ds((place * 2 + c) * 16, 16)
        return self.sel[p].at[records, pl.ds(0, ROWS[p])]

    def give_on(self):
        at = self.at
        for p in self.parts:
            zrel, a = self.zrel[p], ORDERS[p][0]
            rows = pl.ds(0, ROWS[p])
            self.relay(p, lambda c: zrel.at[:, rows] if c is None else zrel.at[pl.ds(c * 16, 16), rows],
                       self.inbox[p].at[pl.ds((at.ring(a, -at.way) * 2 + at.core) * 16, 16), rows], T1, T1F)

    def finish(self):
        at = self.at
        for p in self.parts:
            a, rows = ORDERS[p][0], pl.ds(0, ROWS[p])
            for delta, c in self.others():
                self.arrive(p, self.inbox[p].at[pl.ds((at.ring(a, -delta) * 2 + c) * 16, 16), rows],
                            T1 + delta * 2 + c)
        self.sent()

    def read(self, c):
        return from_parts([self.inbox[p][self.table[2 * len(ORDERS) + p, c]] for p in self.parts])


class Solver:
    def __init__(self, plan, tiles_hl, x, u, r, p, p_hl, image_hl, back, z_before):
        self.plan, self.tiles_hl = plan, tiles_hl
        self.x, self.u, self.r, self.p = x, u, r, p
        self.p_hl, self.image_hl, self.back, self.z_before = p_hl, image_hl, back, z_before
        self.slots, self.blk = p_hl.shape[0], p_hl.shape[2]
        self.targets = p_hl.shape[1] // 2
        self.zero = jnp.zeros((self.targets, self.blk), F32)

    def forward(self, observed=None):
        plan, targets, blk = self.plan, self.targets, self.blk

        def tile_step(k, acc, total):
            wide = lax.dot_general(
                self.p_hl[plan[9 + 1, k]], self.tiles_hl[plan[9 + 0, k]], (((1,), (1,)), ((), ())),
                preferred_element_type=F32)
            acc = jnp.where(plan[9 + 2, k] > 0, acc, 0.0) + join(wide, targets, blk)
            if observed is not None:
                split_store(self.image_hl, k, observed[plan[9 + 4, k]] - acc)
            else:
                split_store(self.image_hl, k, acc)
                total = total + jnp.where(plan[9 + 3, k] > 0, acc * acc, 0.0)
            return acc, total

        return loop(self.slots, GROUP, tile_step, self.zero, self.zero)[1]

    def backward(self):
        plan, targets, blk = self.plan, self.targets, self.blk

        def tile_step(k, acc):
            both = self.tiles_hl[plan[9 + 5, k]]
            weights = jnp.concatenate([both[:blk], both[blk:]], axis=1)
            wide = jnp.dot(self.image_hl[plan[9 + 6, k]], weights, preferred_element_type=F32)
            acc = jnp.where(plan[9 + 7, k] > 0, acc, 0.0) + join(wide, targets, blk)
            self.back[k] = acc
            return (acc,)

        loop(self.slots, GROUP, tile_step, self.zero)

    def load_x(self):
        def one(c, _):
            split_store(self.p_hl, c, self.x[c])
            return (_,)

        loop(self.slots, 8, one, 0)

    def begin(self, first, z_of):
        def one(c, rr, gap):
            z, x, u = z_of(c), self.x[c], self.u[c]
            diff = x - z
            u_new = u + diff
            self.u[c] = u_new
            if first:
                r = self.back[self.plan[9 + 8, c]] + (z - u_new) - x
                self.z_before[c] = z
            else:
                r = self.r[c] + ((z - u_new) - (self.z_before[c] - u))
            self.r[c] = r
            self.p[c] = r
            split_store(self.p_hl, c, r)
            return rr + r * r, gap + diff * diff

        rr, gap = loop(self.slots, 8, one, self.zero, self.zero)
        self.own = rr
        self.rr = total_of(rr)
        return gap

    def length(self):
        self.a = self.rr / total_of(self.forward() + self.own)

    def move_x(self):
        p, x, a = self.p, self.x, self.a

        def move(c, _):
            x[c] = x[c] + a * p[c]
            return (_,)

        loop(self.slots, 8, move, 0)

    def move_r(self):
        p, r, back, plan, a = self.p, self.r, self.back, self.plan, self.a
        self.backward()

        def move(c, nn):
            new = r[c] - a * (back[plan[9 + 8, c]] + p[c])
            r[c] = new
            return (nn + new * new,)

        return loop(self.slots, 8, move, self.zero)[0]

    def step(self):
        p, r, x = self.p, self.r, self.x
        self.length()
        a = self.a
        nn = total_of(self.move_r())
        ratio = nn / self.rr

        def turn(c, own):
            value = p[c]
            x[c] = x[c] + a * value
            value = r[c] + ratio * value
            p[c] = value
            split_store(self.p_hl, c, value)
            return (own + value * value,)

        self.own = loop(self.slots, 8, turn, self.zero)[0]
        self.rr = nn


def fused_kernel(table, tiles_in, observed_in, x_in, u_in, x, u_out, z_own, gap_out, *scratch):
    plan = table
    (u, tiles, observed, tiles_hl, r, p, p_hl, image_hl, back, z_before, gap_box, local_sem, gap_send, gap_recv,
     send_sem, recv_sem) = scratch[BOXES * len(ORDERS):]
    boxes = [scratch[n * len(ORDERS):(n + 1) * len(ORDERS)] for n in range(BOXES)]
    loads = [pltpu.make_async_copy(src, dst, local_sem.at[n]) for n, (src, dst) in enumerate(
        ((x_in, x), (u_in, u), (tiles_in, tiles), (observed_in, observed)))]
    for load in loads:
        load.start()
    at = Place()
    barrier = pltpu.get_barrier_semaphore()
    friends = [at.partner]
    for axis in ("x", "y", "z"):
        friends += [at.near(axis, 2)] + [at.near(axis, delta, c) for delta in (1, -1) for c in (0, 1)]
    for friend in friends:
        pl.semaphore_signal(barrier, inc=1, device_id=friend, device_id_type=MESH)
    exchange = Exchange(at, table, boxes, send_sem, recv_sem)
    solver = Solver(plan, tiles_hl, x, u, r, p, p_hl, image_hl, back, z_before)
    loads[0].wait()
    loads[1].wait()
    exchange.start(x, u, lambda: pl.semaphore_wait(barrier, len(friends)))
    loads[2].wait()

    def one_tile(t, _):
        split_tile(tiles_hl, t, tiles[t])
        return (_,)

    loop(tiles.shape[0], 2, one_tile, 0)
    back[back.shape[0] - 1] = solver.zero
    loads[3].wait()
    solver.load_x()
    exchange.pass_on()
    solver.forward(observed=observed)
    solver.backward()

    def rest():
        exchange.reduce_first()
        exchange.reduce_second()
        exchange.reduce_third()
        exchange.agree()
        exchange.spread_all()
        exchange.give_back()
        exchange.give_on()
        if not exchange.first:
            exchange.keep(z_own)
        exchange.finish()

    rest()
    solver.begin(True, exchange.read)

    def advance(_, carry):
        solver.rr, solver.own = carry
        solver.step()
        return solver.rr, solver.own

    solver.rr, solver.own = lax.fori_loop(0, CG_STEPS - 1, advance, (solver.rr, solver.own))
    solver.length()
    solver.move_x()
    exchange.first = False
    exchange.start(x, u)
    solver.move_r()
    exchange.pass_on()
    rest()
    gap = solver.begin(False, exchange.read)
    store = pltpu.make_async_copy(u, u_out, local_sem.at[4])
    store.start()

    def gap_copy(n, stage, device):
        return pltpu.make_async_remote_copy(
            src_ref=gap_box.at[10 + stage], dst_ref=gap_box.at[n], send_sem=gap_send.at[n],
            recv_sem=gap_recv.at[n], device_id=device, device_id_type=MESH)

    def gap_peer(stage, delta):
        along = {"x": (1 - stage) * (2 - stage) // 2, "y": stage * (2 - stage), "z": stage * (stage - 1) // 2}
        to = {a: lax.rem(at.me[a] + delta * along[a], SIDE) for a in along}
        return ((to["y"] * SIDE + to["x"]) * 2 + at.core, to["z"])

    def gap_step(stage, carry):
        solver.rr, solver.own = carry
        moves = [gap_copy(3 * stage + delta - 1, stage, gap_peer(stage, delta)) for delta in (1, 2, 3)]
        for moving in moves:
            moving.start()
        solver.step()
        value = gap_box[10 + stage]
        for n, moving in enumerate(moves):
            moving.wait()
            value = value + gap_box[3 * stage + n]
        gap_box[11 + stage] = value
        return solver.rr, solver.own

    gap_box[10] = gap
    solver.rr, solver.own = lax.fori_loop(0, CG_STEPS - 1, gap_step, (solver.rr, solver.own))
    moving = gap_copy(9, 3, at.partner)
    moving.start()
    solver.length()
    solver.move_x()
    moving.wait()
    gap_out[...] = gap_box[13] + gap_box[9]
    store.wait()


def hand_over_kernel(scale, x_in, u_in, z_in, gap, x, u, z, primal, x_box, u_box, z_box, sems):
    step = x_in.shape[0] // 4
    moves = [(z_in, z_box, z)]
    for n in range(4):
        rows = pl.ds(n * step, step)
        moves += [(a.at[rows], b.at[rows], c.at[rows]) for a, b, c in ((x_in, x_box, x), (u_in, u_box, u))]
    reads = [pltpu.make_async_copy(a, b, sems.at[0, n]) for n, (a, b, _) in enumerate(moves)]
    writes = [pltpu.make_async_copy(b, c, sems.at[1, n]) for n, (_, b, c) in enumerate(moves)]
    for read in reads:
        read.start()
    targets, blk = gap.shape
    down, across = (lax.broadcasted_iota(jnp.int32, (targets, blk), n) for n in (0, 1))
    total = jnp.sum(gap[...], axis=1, keepdims=True)
    total = jnp.sum(jnp.where(down == across, total, 0.0), axis=0, keepdims=True)
    primal[...] = jnp.sqrt(total / scale)[:, :targets]
    for read, write in zip(reads, writes):
        read.wait()
        write.start()
    for write in writes:
        write.wait()


def hand_over(scale, x, u, z, gap):
    anywhere, whole = pl.BlockSpec(memory_space=pl.ANY), pl.BlockSpec(memory_space=pltpu.VMEM)
    like = [jax.ShapeDtypeStruct(a.shape, F32) for a in (x, u, z)]
    return pl.pallas_call(
        functools.partial(hand_over_kernel, float(scale)),
        out_shape=(*like, jax.ShapeDtypeStruct((1, gap.shape[0]), F32)),
        in_specs=[anywhere] * 3 + [whole],
        out_specs=(anywhere, anywhere, anywhere, whole),
        scratch_shapes=[pltpu.VMEM(a.shape, F32) for a in (x, u, z)] + [pltpu.SemaphoreType.DMA((2, 9))],
        compiler_params=pltpu.CompilerParams(vmem_limit_bytes=67043328),
        name="hand_over",
    )(x, u, z, gap)


def fused(table, tiles, observed, x, u):
    slots, targets, blk = x.shape
    count = tiles.shape[0]
    shards = table.shape[1]
    each = lambda *shape: [pltpu.VMEM(shape + (DEEP, blk), F32) for _ in ORDERS]
    scratch = (
        each(8, 16) + each(8, 16) + each(2, 16) + each(SIDE, SIDE, PER) + each(SIDE, PER) + each(2, SIDE, PER)
        + each(SIDE, PER) + each(3, PER) + each(SIDE, SIDE, PER) + each(shards) + each(shards) + each(32)
        + [pltpu.VMEM((SUB, blk), F32) for _ in ORDERS]
        + [
            pltpu.VMEM(x.shape, F32), pltpu.VMEM(tiles.shape, F32), pltpu.VMEM(observed.shape, F32),
            pltpu.VMEM((count, 2 * blk, blk), BF16), pltpu.VMEM(x.shape, F32), pltpu.VMEM(x.shape, F32),
            pltpu.VMEM((slots, 2 * targets, blk), BF16), pltpu.VMEM((count, 2 * targets, blk), BF16),
            pltpu.VMEM((count + 1, targets, blk), F32), pltpu.VMEM(x.shape, F32),
            pltpu.VMEM((14, targets, blk), F32),
            pltpu.SemaphoreType.DMA((5,)), pltpu.SemaphoreType.DMA((10,)), pltpu.SemaphoreType.DMA((10,)),
            pltpu.SemaphoreType.DMA((len(ORDERS), SEMS)), pltpu.SemaphoreType.DMA((len(ORDERS), SEMS)),
        ]
    )
    whole = pl.BlockSpec(memory_space=pltpu.VMEM)
    scalars = pl.BlockSpec(memory_space=pltpu.SMEM)
    like = jax.ShapeDtypeStruct(x.shape, F32)
    return pl.pallas_call(
        fused_kernel,
        out_shape=(like, like, jax.ShapeDtypeStruct((PER, targets, blk), F32),
                   jax.ShapeDtypeStruct((targets, blk), F32)),
        in_specs=[scalars] + [pl.BlockSpec(memory_space=pl.ANY)] * 4,
        out_specs=(whole, pl.BlockSpec(memory_space=pl.ANY), whole, whole),
        scratch_shapes=scratch,
        compiler_params=pltpu.CompilerParams(
            collective_id=0, has_side_effects=True, vmem_limit_bytes=67043328),
        name="consensus",
    )(table, tiles, observed, x, u)


def on_device(tile_data, tile_row, tile_col, tile_count, touched, owner_map, observed, start_x, start_u):
    shards = lax.axis_size(AXES)
    local_cols = touched.shape[1]
    table = tables(tile_row, tile_col, touched, owner_map, tile_count)
    flip = lambda a: jnp.swapaxes(a, 1, 2)
    x, u, z, gap = fused(table, tile_data, flip(observed), flip(start_x), flip(start_u))
    x, u, z, primal = hand_over(shards * local_cols * start_x.shape[1], x, u, z, gap)
    return flip(x), flip(u), flip(z), primal[0]


def solution(mesh):
    split = P(AXES)
    return jax.shard_map(
        on_device, mesh=mesh,
        in_specs=(split, split, split, split, split, P(), split, split, split),
        out_specs=(split, split, split, P()),
        check_vma=False,
    )
```

```python
import functools

import jax
import jax.numpy as jnp
from jax import lax
from jax.experimental import pallas as pl
from jax.experimental.pallas import tpu as pltpu
from jax.sharding import PartitionSpec as P

ITERS = 2
CG_STEPS = 4
GROUP = 32
AXES = ("dev", "ka")
F32 = jnp.float32
BF16 = jnp.bfloat16
MESH = pl.DeviceIdType.MESH

SIDE = 4
SUB = 8
PER = 4
ORDERS = (("x", "y", "z"), ("y", "z", "x"), ("z", "x", "y"))
ROWS = (22, 22, 20)
DEEP = 24
S1, S1F, S2F, S2S, S2D, S3, T3, T2O, T2F, T2D, T1, T1F, SEMS = 0, 8, 9, 13, 17, 21, 25, 29, 33, 37, 41, 49, 50
THERE, BACK = (2, 1, 3, 0), (0, 1, 3, 2)
BOXES = 13


def fold(values):
    return functools.reduce(lambda s, n: s + n, values)


def split_tile(ref, index, value):
    rows = value.shape[0]
    high = value.astype(BF16)
    low = (value - high.astype(F32)).astype(BF16)
    ref[index, :rows, :] = high
    ref[index, rows:, :] = low


def split_store(ref, index, value):
    for n in range(0, value.shape[0], SUB):
        part = value[n:n + SUB]
        high = part.astype(BF16).astype(F32)
        ref[index, 2 * n:2 * n + 2 * SUB, :] = jnp.concatenate([high, part - high], axis=0).astype(BF16)


def join(wide, rows, cols):
    pieces = []
    for n in range(0, 2 * rows, 2 * SUB):
        high, low = wide[n:n + SUB], wide[n + SUB:n + 2 * SUB]
        pieces.append((high[:, :cols] + high[:, cols:]) + low[:, :cols])
    return jnp.concatenate(pieces, axis=0)


def total_of(value):
    return jnp.sum(value, axis=1, keepdims=True)


def tables_kernel(rows, cols, touched, owner_map, count, out):
    tiles, lanes = rows.shape[1], out.shape[1]
    near, far = (lax.broadcasted_iota(jnp.int32, (tiles, lanes), n) for n in (0, 1))
    down = lax.broadcasted_iota(jnp.int32, (tiles, 1), 0).astype(F32)
    across = lax.broadcasted_iota(jnp.int32, (1, lanes), 1).astype(F32)
    eye = near == far
    wide = lambda v: jnp.concatenate([v[...].astype(F32), jnp.zeros((1, lanes - tiles), F32)], axis=1)
    stand = lambda v: jnp.sum(jnp.where(eye, v, 0.0), axis=1, keepdims=True)
    lie = lambda v: jnp.sum(jnp.where(eye, v, 0.0), axis=0, keepdims=True)
    ones = lambda m: jnp.where(m, 1.0, 0.0)
    left = lambda m: jnp.sum(ones(m), axis=1, keepdims=True)
    up = lambda m: jnp.sum(ones(m), axis=0, keepdims=True)
    number = count[0].astype(F32)
    inside = across < float(tiles)

    def order(values):
        key = jnp.where(across < number, wide(values), float(tiles))
        key = jnp.where(inside, key, float(tiles + 1))
        code = key * float(lanes) + across
        key_d, code_d = stand(key), stand(code)
        same = key == key_d
        rank = left(code < code_d)
        last = left(key <= key_d) - 1.0
        keep = left(same & (code < code_d))
        later = left(same & (code > code_d))
        ends = jnp.where((later == 0.0) & (key_d < float(tiles)), 1.0, 0.0)
        return key_d, rank, last, keep, ends

    def sort(rank, values):
        return jnp.sum(jnp.where(rank == across, values, 0.0), axis=0, keepdims=True)

    row_d, rank_f, last_f, keep_f, ends_f = order(rows)
    col_d, rank_b, _, keep_b, _ = order(cols)
    found = up(col_d == across)
    until = up(col_d <= across) - 1.0
    last_b = jnp.where(found > 0.0, until, float(tiles))
    plan = [
        sort(rank_f, down), sort(rank_f, stand(wide(cols))), sort(rank_f, keep_f), sort(rank_f, ends_f),
        sort(rank_f, stand(wide(rows))), sort(rank_b, down), sort(rank_b, last_f), sort(rank_b, keep_b), last_b,
    ]
    wanted = stand(wide(touched))
    blocks = owner_map.shape[1]
    every = lax.broadcasted_iota(jnp.int32, (1, blocks), 1).astype(F32)
    position = jnp.sum(jnp.where(wanted == every, owner_map[...].astype(F32), 0.0), axis=1, keepdims=True)
    position = position.astype(jnp.int32)
    owner, tag = position >> 2, (position & 3).astype(F32)
    place = {"x": (owner >> 3) & 3, "y": owner >> 5, "z": owner & 3}
    core = (owner >> 2) & 1
    slots, marks, index = [], [], []
    for a, b, c in ORDERS:
        at = (place[a] * 32 + core * 16 + place[b] * 4 + place[c]).astype(F32)
        match = at == across
        slots.append(jnp.sum(jnp.where(match, down, 0.0), axis=0, keepdims=True))
        marks.append(jnp.sum(jnp.where(match, tag + 1.0, 0.0), axis=0, keepdims=True) - 1.0)
        index.append(lie(at))
    found = slots + marks + index + plan
    for n, row in enumerate(found):
        out[n:n + 1, :] = row.astype(jnp.int32)
    out[len(found):, :] = jnp.zeros((out.shape[0] - len(found), lanes), jnp.int32)


def tables(rows, cols, touched, owner_map, count):
    whole = pl.BlockSpec(memory_space=pltpu.VMEM)
    return pl.pallas_call(
        tables_kernel,
        out_shape=jax.ShapeDtypeStruct((24, 128), jnp.int32),
        in_specs=[whole] * 4 + [pl.BlockSpec(memory_space=pltpu.SMEM)],
        out_specs=whole,
        name="tables",
    )(rows, cols, touched, owner_map.reshape(1, -1), count)


def loop(count, step, body, *init):
    def group(g, carry):
        for n in range(step):
            carry = body(g * step + n, *carry)
        return carry

    return lax.fori_loop(0, count // step, group, init)


def near_device(me, axis, delta, to_core):
    at = dict(me)
    at[axis] = lax.rem(me[axis] + delta + SIDE, SIDE)
    return ((at["y"] * SIDE + at["x"]) * 2 + to_core, at["z"])


class Place:
    def __init__(self):
        dev, z = lax.axis_index("dev"), lax.axis_index("ka")
        self.core = lax.rem(dev, 2)
        self.me = {"x": lax.rem(dev // 2, SIDE), "y": dev // 8, "z": z}
        self.way = 1 - 2 * self.core
        self.partner = (dev + 1 - 2 * self.core, z)

    def near(self, axis, delta, to_core=None):
        return near_device(self.me, axis, delta, self.core if to_core is None else to_core)

    def ring(self, axis, delta):
        return lax.rem(self.me[axis] + delta + SIDE, SIDE)


def row_number(blk):
    return lax.broadcasted_iota(jnp.int32, (SUB, blk), 0)


def part_of(p, ref, slot):
    tile = lambda n: ref[slot, n * SUB:(n + 1) * SUB, :]
    pair = [tile(2 * p), tile(2 * p + 1)]
    if p == 0:
        return pair + [tile(6)]
    if p == 1:
        return pair + [pltpu.roll(tile(7), 6, 0)]
    edge = row_number(ref.shape[2]) < 2
    return pair + [jnp.where(edge, pltpu.roll(tile(6), 2, 0), pltpu.roll(tile(7), 2, 0))]


def from_parts(found):
    row = row_number(found[0].shape[1])
    shared = pltpu.roll(found[2][2 * SUB:], 6, 0)
    six = jnp.where(row < 6, found[0][2 * SUB:], shared)
    seven = jnp.where(row < 2, shared, pltpu.roll(found[1][2 * SUB:], 2, 0))
    return jnp.concatenate([f[:2 * SUB] for f in found] + [six, seven], axis=0)


class Exchange:
    def __init__(self, at, table, boxes, send_sem, recv_sem):
        self.at, self.table = at, table
        (self.mail, self.in1, self.fwd1, self.part2, self.fwd2, self.in2, self.part3, self.in3,
         self.zb2, self.inbox, self.sel, self.zrel, self.share) = boxes
        self.first = True
        self.send_sem, self.recv_sem = send_sem, recv_sem
        self.sends = []
        self.parts = range(len(ORDERS))

    def copy(self, p, src, dst, send, recv, device):
        return pltpu.make_async_remote_copy(
            src_ref=src, dst_ref=dst, send_sem=self.send_sem.at[p, send], recv_sem=self.recv_sem.at[p, recv],
            device_id=device, device_id_type=MESH)

    def go(self, p, src, dst, send, recv, device):
        moving = self.copy(p, src, dst, send, recv, device)
        moving.start()
        self.sends.append(moving)

    def arrive(self, p, dst, recv):
        self.copy(p, dst, dst, 0, recv, self.at.partner).wait_recv()

    def sent(self):
        for moving in self.sends:
            moving.wait_send()
        self.sends = []

    def pack(self, p, x, u, delta):
        table, parts, mail = self.table, len(ORDERS), self.mail[p]
        base = self.at.ring(ORDERS[p][0], delta) * 2

        def record(c, _):
            q = base + c
            for i in range(16):
                slot = table[p, q * 16 + i]
                for n, (one, two) in enumerate(zip(part_of(p, x, slot), part_of(p, u, slot))):
                    mail[q, i, n * SUB:(n + 1) * SUB, :] = one + two
                tag = table[parts + p, q * 16 + i]
                mail[q, i, ROWS[p]:ROWS[p] + 1, :] = jnp.full((1, x.shape[2]), tag, jnp.int32).astype(F32)
            return (_,)

        loop(2, 1, record, 0)

    def marked(self, p):
        return pl.ds(0, ROWS[p] + (1 if self.first else 0))

    def scatter_far(self, p, box, relay, base_f):
        at, a = self.at, ORDERS[p][0]
        self.go(p, box(at.ring(a, 2), None), relay, base_f, base_f, at.near(a, at.way))

    def scatter_near(self, p, delta, box, into, base):
        at, a, core = self.at, ORDERS[p][0], self.at.core
        if delta:
            for c in (0, 1):
                self.go(p, box(at.ring(a, delta), c), into(delta), base + delta * 2 + c,
                        base + delta * 2 + core, at.near(a, delta, c))
        else:
            self.go(p, box(at.me[a], 1 - core), into(0), base, base + core, at.partner)

    def relay(self, p, relay, into, base, base_f):
        at, a = self.at, ORDERS[p][0]
        self.arrive(p, relay(None), base_f)
        for c in (0, 1):
            self.go(p, relay(c), into, base + 4 + c, base + 4 + at.core, at.near(a, at.way, c))

    def start(self, x, u, ready=lambda: None):
        def box(p, place, c):
            return self.mail[p].at[pl.ds(place * 2, 2) if c is None else place * 2 + c, :, self.marked(p)]

        for p in self.parts:
            self.pack(p, x, u, 2)
            if p == 0:
                ready()
            self.scatter_far(p, functools.partial(box, p), self.fwd1[p].at[:, :, self.marked(p)], S1F)
        for delta in (1, 3, 0):
            for p in self.parts:
                self.pack(p, x, u, delta)
                self.scatter_near(
                    p, delta, functools.partial(box, p),
                    lambda delta: self.in1[p].at[delta * 2 + self.at.core, :, self.marked(p)], S1)

    def pass_on(self):
        for p in self.parts:
            fwd, rows = self.fwd1[p], self.marked(p)
            self.relay(p, lambda c: fwd.at[:, :, rows] if c is None else fwd.at[c, :, rows],
                       self.in1[p].at[4 + self.at.core, :, rows], S1, S1F)

    def sources(self, p):
        at, a = self.at, ORDERS[p][0]
        mail, in1 = self.mail[p], self.in1[p]
        found = [(0, at.core, lambda i, rows: mail[at.me[a] * 2 + at.core, i, rows, :])]
        for delta, c in ((0, 1 - at.core), (1, 0), (1, 1), (2, 0), (2, 1), (3, 0), (3, 1)):
            found.append((delta, c, lambda i, rows, n=delta * 2 + c: in1[n, i, rows, :]))
        return found

    def others(self):
        return ((1, 0), (1, 1), (3, 0), (3, 1), (0, 1 - self.at.core), (2, 0), (2, 1))

    def combine(self, p, far):
        at, b = self.at, ORDERS[p][1]
        found = self.sources(p)
        part2 = self.part2[p]
        blk = part2.shape[4]
        mark = ROWS[p] - 2 * SUB

        def some(n, _):
            a2 = at.ring(b, 2) if far else at.ring(b, at.way * (n - 1))
            for a3 in range(SIDE):
                i = a2 * SIDE + a3
                tags = [jnp.broadcast_to(read(i, pl.ds(ROWS[p], 1)), (SUB, blk)) for _, _, read in found]
                hits = [[tag == float(k) for tag in tags] for k in range(PER)]
                for j in range(DEEP // SUB):
                    data = [read(i, pl.ds(j * SUB, SUB)) for _, _, read in found]
                    for k in range(PER):
                        value = fold([jnp.where(h, v, 0.0) for h, v in zip(hits[k], data)])
                        if self.first and j == 2:
                            count = fold([jnp.where(h, 1.0, 0.0) for h in hits[k]])
                            value = jnp.where(row_number(blk) == mark, count, value)
                        part2[a2, a3, k, j * SUB:(j + 1) * SUB, :] = value
            return (_,)

        if far:
            some(0, 0)
        else:
            loop(SIDE - 1, 1, some, 0)

    def reduce_first(self):
        at = self.at
        for p in self.parts:
            b, d = ORDERS[p][1], ORDERS[p][2]
            rows = self.marked(p)
            for delta, c in self.others():
                self.arrive(p, self.in1[p].at[delta * 2 + c, :, rows], S1 + delta * 2 + c)
            self.combine(p, True)
            for n, delta in enumerate(THERE):
                piece = at.ring(d, delta)
                self.go(p, self.part2[p].at[at.ring(b, 2), piece, :, rows], self.fwd2[p].at[piece, :, rows],
                        S2F + n, S2F + n, at.near(b, at.way))
        for p in self.parts:
            b, d = ORDERS[p][1], ORDERS[p][2]
            rows = self.marked(p)
            self.combine(p, False)
            for n, delta in enumerate(THERE):
                piece = at.ring(d, delta)
                self.go(p, self.part2[p].at[at.ring(b, -at.way), piece, :, rows], self.in2[p].at[1, piece, :, rows],
                        S2D + n, S2D + n, at.near(b, -at.way))

    def reduce_second(self):
        at = self.at
        for n, delta in enumerate(THERE):
            for p in self.parts:
                b, piece = ORDERS[p][1], at.ring(ORDERS[p][2], delta)
                rows = self.marked(p)
                self.arrive(p, self.fwd2[p].at[piece, :, rows], S2F + n)
                to = at.ring(b, at.way)
                self.part2[p][to, piece] = self.part2[p][to, piece] + self.fwd2[p][piece]
                self.go(p, self.part2[p].at[to, piece, :, rows], self.in2[p].at[0, piece, :, rows],
                        S2S + n, S2S + n, at.near(b, at.way))

    def reduce_third(self):
        at = self.at
        for n, delta in enumerate(THERE):
            for p in self.parts:
                b, d = ORDERS[p][1], ORDERS[p][2]
                piece = at.ring(d, delta)
                rows = self.marked(p)
                self.arrive(p, self.in2[p].at[1, piece, :, rows], S2D + n)
                self.arrive(p, self.in2[p].at[0, piece, :, rows], S2S + n)
                self.part3[p][piece] = (
                    self.part2[p][at.me[b], piece] + self.in2[p][0, piece] + self.in2[p][1, piece])
                if delta:
                    self.go(p, self.part3[p].at[piece, :, rows], self.in3[p].at[delta - 1, :, rows],
                            S3 + delta, S3 + delta, at.near(d, delta))

    def agree(self):
        at = self.at
        for p in self.parts:
            b, d = ORDERS[p][1], ORDERS[p][2]
            rows = self.marked(p)
            for delta in (1, 3, 2):
                self.arrive(p, self.in3[p].at[delta - 1, :, rows], S3 + delta)
            for k in range(PER):
                value = fold([self.part3[p][at.me[d], k]] + [self.in3[p][n, k] for n in range(3)])
                if self.first:
                    self.share[p][k:k + 1, :] = jnp.maximum(value[ROWS[p]:ROWS[p] + 1], 1.0)
                share = self.share[p][k:k + 1, :]
                value = value / share
                cut = jnp.broadcast_to(1.0 / share, value.shape)
                self.zb2[p][at.me[b], at.me[d], k] = value - jnp.minimum(jnp.maximum(value, -cut), cut)
            own = self.zb2[p].at[at.me[b], at.me[d], :, pl.ds(0, ROWS[p])]
            for delta in (2, 1, 3):
                self.go(p, own, own, T3 + delta, T3 + delta, at.near(d, delta))
            self.spread(p, 0)

    def keep(self, z_own):
        at = self.at
        for k in range(PER):
            z_own[k] = from_parts([self.zb2[p][at.me[ORDERS[p][1]], at.me[ORDERS[p][2]], k] for p in self.parts])

    def spread(self, p, n):
        at, b = self.at, ORDERS[p][1]
        own = self.zb2[p].at[at.me[b], at.ring(ORDERS[p][2], -BACK[n]), :, pl.ds(0, ROWS[p])]
        if n:
            self.arrive(p, own, T3 + BACK[n])
        self.go(p, own, own, T2O + n, T2O + n, at.near(b, at.way))
        self.go(p, own, own, T2D + n, T2D + n, at.near(b, -at.way))

    def spread_on(self, p, n):
        at, b = self.at, ORDERS[p][1]
        passing = self.zb2[p].at[at.ring(b, -at.way), at.ring(ORDERS[p][2], -BACK[n]), :, pl.ds(0, ROWS[p])]
        self.arrive(p, passing, T2O + n)
        self.go(p, passing, passing, T2F + n, T2F + n, at.near(b, at.way))

    def spread_all(self):
        for act, n in ((self.spread, 1), (self.spread, 2), (self.spread_on, 0), (self.spread, 3),
                       (self.spread_on, 1), (self.spread_on, 2), (self.spread_on, 3)):
            for p in self.parts:
                act(p, n)

    def select(self, p, far):
        at = self.at
        a = ORDERS[p][0]
        found = self.sources(p)
        zb2, inbox, sel = self.zb2[p], self.inbox[p], self.sel[p]
        tiles = [slice(j * SUB, (j + 1) * SUB) for j in range(DEEP // SUB)]

        def some(a2, _):
            for a3 in range(SIDE):
                i = a2 * SIDE + a3
                blocks = [[zb2[a2, a3, k, rows, :] for rows in tiles] for k in range(PER)]
                for number, (delta, c, read) in enumerate(found):
                    if (delta == 2) != far:
                        continue
                    tag = jnp.broadcast_to(read(i, pl.ds(ROWS[p], 1)), blocks[0][0].shape)
                    hit = [tag == float(k) for k in range(PER - 1)]
                    for j, rows in enumerate(tiles):
                        value = blocks[PER - 1][j]
                        for k in range(PER - 1):
                            value = jnp.where(hit[k], blocks[k][j], value)
                        place = (at.ring(a, -delta) * 2 + c) * 16 + i
                        (sel if number else inbox)[place, rows, :] = value
            return (_,)

        loop(SIDE, 1, some, 0)

    def give_back(self):
        at = self.at
        self.sent()
        for p in self.parts:
            a, b = ORDERS[p][0], ORDERS[p][1]
            rows = pl.ds(0, ROWS[p])
            for n, delta in enumerate(BACK):
                piece = at.ring(ORDERS[p][2], -delta)
                self.arrive(p, self.zb2[p].at[at.ring(b, at.way), piece, :, rows], T2D + n)
                self.arrive(p, self.zb2[p].at[at.ring(b, 2), piece, :, rows], T2F + n)
            self.select(p, True)
            self.scatter_far(p, functools.partial(self.sel_box, p), self.zrel[p].at[:, rows], T1F)
        for p in self.parts:
            a, rows = ORDERS[p][0], pl.ds(0, ROWS[p])
            mine = self.inbox[p].at[pl.ds((at.me[a] * 2 + at.core) * 16, 16), rows]
            self.select(p, False)
            for delta in (1, 3, 0):
                self.scatter_near(p, delta, functools.partial(self.sel_box, p), lambda delta: mine, T1)

    def sel_box(self, p, place, c):
        records = pl.ds(place * 32, 32) if c is None else pl.ds((place * 2 + c) * 16, 16)
        return self.sel[p].at[records, pl.ds(0, ROWS[p])]

    def give_on(self):
        at = self.at
        for p in self.parts:
            zrel, a = self.zrel[p], ORDERS[p][0]
            rows = pl.ds(0, ROWS[p])
            self.relay(p, lambda c: zrel.at[:, rows] if c is None else zrel.at[pl.ds(c * 16, 16), rows],
                       self.inbox[p].at[pl.ds((at.ring(a, -at.way) * 2 + at.core) * 16, 16), rows], T1, T1F)

    def finish(self):
        at = self.at
        for p in self.parts:
            a, rows = ORDERS[p][0], pl.ds(0, ROWS[p])
            for delta, c in self.others():
                self.arrive(p, self.inbox[p].at[pl.ds((at.ring(a, -delta) * 2 + c) * 16, 16), rows],
                            T1 + delta * 2 + c)
        self.sent()

    def read(self, c):
        return from_parts([self.inbox[p][self.table[2 * len(ORDERS) + p, c]] for p in self.parts])


class Solver:
    def __init__(self, plan, tiles_hl, x, u, r, p, p_hl, image_hl, back, z_before):
        self.plan, self.tiles_hl = plan, tiles_hl
        self.x, self.u, self.r, self.p = x, u, r, p
        self.p_hl, self.image_hl, self.back, self.z_before = p_hl, image_hl, back, z_before
        self.slots, self.blk = p_hl.shape[0], p_hl.shape[2]
        self.targets = p_hl.shape[1] // 2
        self.zero = jnp.zeros((self.targets, self.blk), F32)

    def forward(self, observed=None):
        plan, targets, blk = self.plan, self.targets, self.blk

        def tile_step(k, acc, total):
            wide = lax.dot_general(
                self.p_hl[plan[9 + 1, k]], self.tiles_hl[plan[9 + 0, k]], (((1,), (1,)), ((), ())),
                preferred_element_type=F32)
            acc = jnp.where(plan[9 + 2, k] > 0, acc, 0.0) + join(wide, targets, blk)
            if observed is not None:
                split_store(self.image_hl, k, observed[plan[9 + 4, k]] - acc)
            else:
                split_store(self.image_hl, k, acc)
                total = total + jnp.where(plan[9 + 3, k] > 0, acc * acc, 0.0)
            return acc, total

        return loop(self.slots, GROUP, tile_step, self.zero, self.zero)[1]

    def backward(self):
        plan, targets, blk = self.plan, self.targets, self.blk

        def tile_step(k, acc):
            both = self.tiles_hl[plan[9 + 5, k]]
            weights = jnp.concatenate([both[:blk], both[blk:]], axis=1)
            wide = jnp.dot(self.image_hl[plan[9 + 6, k]], weights, preferred_element_type=F32)
            acc = jnp.where(plan[9 + 7, k] > 0, acc, 0.0) + join(wide, targets, blk)
            self.back[k] = acc
            return (acc,)

        loop(self.slots, GROUP, tile_step, self.zero)

    def load_x(self):
        def one(c, _):
            split_store(self.p_hl, c, self.x[c])
            return (_,)

        loop(self.slots, 16, one, 0)

    def begin(self, first, z_of):
        def one(c, rr, gap):
            z, x, u = z_of(c), self.x[c], self.u[c]
            diff = x - z
            u_new = u + diff
            self.u[c] = u_new
            if first:
                r = self.back[self.plan[9 + 8, c]] + (z - u_new) - x
                self.z_before[c] = z
            else:
                r = self.r[c] + ((z - u_new) - (self.z_before[c] - u))
            self.r[c] = r
            self.p[c] = r
            split_store(self.p_hl, c, r)
            return rr + r * r, gap + diff * diff

        rr, gap = loop(self.slots, 16, one, self.zero, self.zero)
        self.own = rr
        self.rr = total_of(rr)
        return gap

    def length(self):
        self.a = self.rr / total_of(self.forward() + self.own)

    def move_x(self):
        p, x, a = self.p, self.x, self.a

        def move(c, _):
            x[c] = x[c] + a * p[c]
            return (_,)

        loop(self.slots, 16, move, 0)

    def move_r(self):
        p, r, back, plan, a = self.p, self.r, self.back, self.plan, self.a
        self.backward()

        def move(c, nn):
            new = r[c] - a * (back[plan[9 + 8, c]] + p[c])
            r[c] = new
            return (nn + new * new,)

        return loop(self.slots, 16, move, self.zero)[0]

    def step(self):
        p, r, x = self.p, self.r, self.x
        self.length()
        a = self.a
        nn = total_of(self.move_r())
        ratio = nn / self.rr

        def turn(c, own):
            value = p[c]
            x[c] = x[c] + a * value
            value = r[c] + ratio * value
            p[c] = value
            split_store(self.p_hl, c, value)
            return (own + value * value,)

        self.own = loop(self.slots, 16, turn, self.zero)[0]
        self.rr = nn


def fused_kernel(table, tiles_in, observed_in, x_in, u_in, x, u_out, z_own, gap_out, *scratch):
    plan = table
    (u, tiles, observed, tiles_hl, r, p, p_hl, image_hl, back, z_before, gap_box, local_sem, gap_send, gap_recv,
     send_sem, recv_sem) = scratch[BOXES * len(ORDERS):]
    boxes = [scratch[n * len(ORDERS):(n + 1) * len(ORDERS)] for n in range(BOXES)]
    loads = [pltpu.make_async_copy(src, dst, local_sem.at[n]) for n, (src, dst) in enumerate(
        ((x_in, x), (u_in, u), (tiles_in, tiles), (observed_in, observed)))]
    for load in loads:
        load.start()
    at = Place()
    barrier = pltpu.get_barrier_semaphore()
    friends = [at.partner]
    for axis in ("x", "y", "z"):
        friends += [at.near(axis, 2)] + [at.near(axis, delta, c) for delta in (1, -1) for c in (0, 1)]
    for friend in friends:
        pl.semaphore_signal(barrier, inc=1, device_id=friend, device_id_type=MESH)
    exchange = Exchange(at, table, boxes, send_sem, recv_sem)
    solver = Solver(plan, tiles_hl, x, u, r, p, p_hl, image_hl, back, z_before)
    loads[0].wait()
    loads[1].wait()
    exchange.start(x, u, lambda: pl.semaphore_wait(barrier, len(friends)))
    loads[2].wait()

    def one_tile(t, _):
        split_tile(tiles_hl, t, tiles[t])
        return (_,)

    loop(tiles.shape[0], 2, one_tile, 0)
    back[back.shape[0] - 1] = solver.zero
    loads[3].wait()
    solver.load_x()
    exchange.pass_on()
    solver.forward(observed=observed)
    solver.backward()

    def rest():
        exchange.reduce_first()
        exchange.reduce_second()
        exchange.reduce_third()
        exchange.agree()
        exchange.spread_all()
        exchange.give_back()
        exchange.give_on()
        if not exchange.first:
            exchange.keep(z_own)
        exchange.finish()

    rest()
    solver.begin(True, exchange.read)

    def advance(_, carry):
        solver.rr, solver.own = carry
        solver.step()
        return solver.rr, solver.own

    solver.rr, solver.own = lax.fori_loop(0, CG_STEPS - 1, advance, (solver.rr, solver.own))
    solver.length()
    solver.move_x()
    exchange.first = False
    exchange.start(x, u)
    solver.move_r()
    exchange.pass_on()
    rest()
    gap = solver.begin(False, exchange.read)
    store = pltpu.make_async_copy(u, u_out, local_sem.at[4])
    store.start()

    def gap_copy(n, stage, device):
        return pltpu.make_async_remote_copy(
            src_ref=gap_box.at[10 + stage], dst_ref=gap_box.at[n], send_sem=gap_send.at[n],
            recv_sem=gap_recv.at[n], device_id=device, device_id_type=MESH)

    def gap_peer(stage, delta):
        along = {"x": (1 - stage) * (2 - stage) // 2, "y": stage * (2 - stage), "z": stage * (stage - 1) // 2}
        to = {a: lax.rem(at.me[a] + delta * along[a], SIDE) for a in along}
        return ((to["y"] * SIDE + to["x"]) * 2 + at.core, to["z"])

    def gap_step(stage, carry):
        solver.rr, solver.own = carry
        moves = [gap_copy(3 * stage + delta - 1, stage, gap_peer(stage, delta)) for delta in (1, 2, 3)]
        for moving in moves:
            moving.start()
        solver.step()
        value = gap_box[10 + stage]
        for n, moving in enumerate(moves):
            moving.wait()
            value = value + gap_box[3 * stage + n]
        gap_box[11 + stage] = value
        return solver.rr, solver.own

    gap_box[10] = gap
    solver.rr, solver.own = lax.fori_loop(0, CG_STEPS - 1, gap_step, (solver.rr, solver.own))
    moving = gap_copy(9, 3, at.partner)
    moving.start()
    solver.length()
    solver.move_x()
    moving.wait()
    gap_out[...] = gap_box[13] + gap_box[9]
    store.wait()


def hand_over_kernel(scale, x_in, u_in, z_in, gap, x, u, z, primal, x_box, u_box, z_box, sems):
    step = x_in.shape[0] // 4
    moves = [(z_in, z_box, z)]
    for n in range(4):
        rows = pl.ds(n * step, step)
        moves += [(a.at[rows], b.at[rows], c.at[rows]) for a, b, c in ((x_in, x_box, x), (u_in, u_box, u))]
    reads = [pltpu.make_async_copy(a, b, sems.at[0, n]) for n, (a, b, _) in enumerate(moves)]
    writes = [pltpu.make_async_copy(b, c, sems.at[1, n]) for n, (_, b, c) in enumerate(moves)]
    for read in reads:
        read.start()
    targets, blk = gap.shape
    down, across = (lax.broadcasted_iota(jnp.int32, (targets, blk), n) for n in (0, 1))
    total = jnp.sum(gap[...], axis=1, keepdims=True)
    total = jnp.sum(jnp.where(down == across, total, 0.0), axis=0, keepdims=True)
    primal[...] = jnp.sqrt(total / scale)[:, :targets]
    for read, write in zip(reads, writes):
        read.wait()
        write.start()
    for write in writes:
        write.wait()


def hand_over(scale, x, u, z, gap):
    anywhere, whole = pl.BlockSpec(memory_space=pl.ANY), pl.BlockSpec(memory_space=pltpu.VMEM)
    like = [jax.ShapeDtypeStruct(a.shape, F32) for a in (x, u, z)]
    return pl.pallas_call(
        functools.partial(hand_over_kernel, float(scale)),
        out_shape=(*like, jax.ShapeDtypeStruct((1, gap.shape[0]), F32)),
        in_specs=[anywhere] * 3 + [whole],
        out_specs=(anywhere, anywhere, anywhere, whole),
        scratch_shapes=[pltpu.VMEM(a.shape, F32) for a in (x, u, z)] + [pltpu.SemaphoreType.DMA((2, 9))],
        compiler_params=pltpu.CompilerParams(vmem_limit_bytes=67043328),
        name="hand_over",
    )(x, u, z, gap)


def fused(table, tiles, observed, x, u):
    slots, targets, blk = x.shape
    count = tiles.shape[0]
    shards = table.shape[1]
    each = lambda *shape: [pltpu.VMEM(shape + (DEEP, blk), F32) for _ in ORDERS]
    scratch = (
        each(8, 16) + each(8, 16) + each(2, 16) + each(SIDE, SIDE, PER) + each(SIDE, PER) + each(2, SIDE, PER)
        + each(SIDE, PER) + each(3, PER) + each(SIDE, SIDE, PER) + each(shards) + each(shards) + each(32)
        + [pltpu.VMEM((SUB, blk), F32) for _ in ORDERS]
        + [
            pltpu.VMEM(x.shape, F32), pltpu.VMEM(tiles.shape, F32), pltpu.VMEM(observed.shape, F32),
            pltpu.VMEM((count, 2 * blk, blk), BF16), pltpu.VMEM(x.shape, F32), pltpu.VMEM(x.shape, F32),
            pltpu.VMEM((slots, 2 * targets, blk), BF16), pltpu.VMEM((count, 2 * targets, blk), BF16),
            pltpu.VMEM((count + 1, targets, blk), F32), pltpu.VMEM(x.shape, F32),
            pltpu.VMEM((14, targets, blk), F32),
            pltpu.SemaphoreType.DMA((5,)), pltpu.SemaphoreType.DMA((10,)), pltpu.SemaphoreType.DMA((10,)),
            pltpu.SemaphoreType.DMA((len(ORDERS), SEMS)), pltpu.SemaphoreType.DMA((len(ORDERS), SEMS)),
        ]
    )
    whole = pl.BlockSpec(memory_space=pltpu.VMEM)
    scalars = pl.BlockSpec(memory_space=pltpu.SMEM)
    like = jax.ShapeDtypeStruct(x.shape, F32)
    return pl.pallas_call(
        fused_kernel,
        out_shape=(like, like, jax.ShapeDtypeStruct((PER, targets, blk), F32),
                   jax.ShapeDtypeStruct((targets, blk), F32)),
        in_specs=[scalars] + [pl.BlockSpec(memory_space=pl.ANY)] * 4,
        out_specs=(whole, pl.BlockSpec(memory_space=pl.ANY), whole, whole),
        scratch_shapes=scratch,
        compiler_params=pltpu.CompilerParams(
            collective_id=0, has_side_effects=True, vmem_limit_bytes=67043328),
        name="consensus",
    )(table, tiles, observed, x, u)


def on_device(tile_data, tile_row, tile_col, tile_count, touched, owner_map, observed, start_x, start_u):
    shards = lax.axis_size(AXES)
    local_cols = touched.shape[1]
    table = tables(tile_row, tile_col, touched, owner_map, tile_count)
    flip = lambda a: jnp.swapaxes(a, 1, 2)
    x, u, z, gap = fused(table, tile_data, flip(observed), flip(start_x), flip(start_u))
    x, u, z, primal = hand_over(shards * local_cols * start_x.shape[1], x, u, z, gap)
    return flip(x), flip(u), flip(z), primal[0]


def solution(mesh):
    split = P(AXES)
    return jax.shard_map(
        on_device, mesh=mesh,
        in_specs=(split, split, split, split, split, P(), split, split, split),
        out_specs=(split, split, split, P()),
        check_vma=False,
    )
```
